8 devices in a mesh: dp: 2 (over z, y), tp: 4 (over x, core).
Axes of the slice: x: 2, y: 2, z: 1, core: 2. Of those that a mesh axis runs over, the one named last changes fastest.
Arguments:
- x_tokens: bfloat16 [12, 64, 4096], P('dp', 'tp'), parts along dimension 0
- start_pos: int32 [12], P('dp'), parts along dimension 0
- k_cache: bfloat16 [2, 12, 8, 3136, 128], P(None, 'dp', 'tp'), parts along dimension 1
- v_cache: bfloat16 [2, 12, 8, 3136, 128], P(None, 'dp', 'tp'), parts along dimension 1
- w_q: bfloat16 [2, 4096, 6144], P(None, None, 'tp')
- w_k: bfloat16 [2, 4096, 1024], P(None, None, 'tp')
- w_v: bfloat16 [2, 4096, 1024], P(None, None, 'tp')
- w_o: bfloat16 [2, 6144, 4096], P(None, 'tp')
- w_up: bfloat16 [2, 4096, 16384], P(None, None, 'tp')
- w_down: bfloat16 [2, 16384, 4096], P(None, 'tp')
- ln_gain: bfloat16 [2, 2, 4096], replicated
- ln_bias: bfloat16 [2, 2, 4096], replicated
Outputs:
- output 1: bfloat16 [12, 64, 4096], P('dp', 'tp'), parts along dimension 0
- output 2: bfloat16 [2, 12, 8, 3136, 128], P(None, 'dp', 'tp'), parts along dimension 1
- output 3: bfloat16 [2, 12, 8, 3136, 128], P(None, 'dp', 'tp'), parts along dimension 1
There are 2 independent parts. The reference program is written for one: setup_inputs(seed, part) draws one part's arguments, and reference() takes and returns one part's arrays. A program takes and returns all parts, laid end to end along the dimension named above; an argument that names none is the same for every part.
All inputs are finite; a program needn't handle non-finite values.
Results may differ from the reference program's by a relative error of at most 0.0189325.
Values are sent between devices in bfloat16 or wider.
A program may use at most 1.25 GiB of HBM per device.

```python
import jax
import jax.numpy as jnp
from jax import lax

LAYERS = 2
BATCH_SEQS = 6
NEW_TOKENS = 64
PREFIX_MAX = 3072
D_MODEL = 4096
N_HEADS = 48
KV_HEADS = 8
HEAD_DIM = 128
FF_DIM = 16384

CACHE_LEN = PREFIX_MAX + NEW_TOKENS
Q_WIDTH = N_HEADS * HEAD_DIM
KV_WIDTH = KV_HEADS * HEAD_DIM
GROUP_SIZE = N_HEADS // KV_HEADS
ROT_DIM = HEAD_DIM // 2
LN_EPS = 1e-5
ROPE_BASE = 10000.0
SOFTMAX_SCALE = HEAD_DIM ** -0.5
NEG_BIG = -1e30


def draw_weight(key_w, shape, fan_in, gain):
    return (jax.random.normal(key_w, shape, jnp.float32) * (gain * fan_in ** -0.5)).astype(jnp.bfloat16)


def draw_starts(key_s):
    key_low, key_pick = jax.random.split(key_s)
    low_bound = PREFIX_MAX // 4
    drawn = jax.random.randint(key_low, (BATCH_SEQS,), low_bound, PREFIX_MAX + 1, jnp.int32)
    chosen = jax.random.randint(key_pick, (), 0, BATCH_SEQS, jnp.int32)
    return jnp.where(jnp.arange(BATCH_SEQS, dtype=jnp.int32) == chosen, PREFIX_MAX, drawn).astype(jnp.int32)


def setup_inputs(seed: int = 0, part: int = 0) -> dict:
    part_key = jax.random.fold_in(jax.random.key(seed), part)
    part_keys = jax.random.split(part_key, 4)
    weight_keys = jax.random.split(jax.random.key(seed + 1), 8)
    cache_shape = (LAYERS, BATCH_SEQS, KV_HEADS, CACHE_LEN, HEAD_DIM)
    return {
        'x_tokens': jax.random.normal(part_keys[0], (BATCH_SEQS, NEW_TOKENS, D_MODEL), jnp.float32).astype(jnp.bfloat16),
        'start_pos': draw_starts(part_keys[1]),
        'k_cache': jax.random.normal(part_keys[2], cache_shape, jnp.float32).astype(jnp.bfloat16),
        'v_cache': jax.random.normal(part_keys[3], cache_shape, jnp.float32).astype(jnp.bfloat16),
        'w_q': draw_weight(weight_keys[0], (LAYERS, D_MODEL, Q_WIDTH), D_MODEL, 1.5),
        'w_k': draw_weight(weight_keys[1], (LAYERS, D_MODEL, KV_WIDTH), D_MODEL, 1.0),
        'w_v': draw_weight(weight_keys[2], (LAYERS, D_MODEL, KV_WIDTH), D_MODEL, 1.0),
        'w_o': draw_weight(weight_keys[3], (LAYERS, Q_WIDTH, D_MODEL), Q_WIDTH, 3.0),
        'w_up': draw_weight(weight_keys[4], (LAYERS, D_MODEL, FF_DIM), D_MODEL, 1.0),
        'w_down': draw_weight(weight_keys[5], (LAYERS, FF_DIM, D_MODEL), FF_DIM, 1.0),
        'ln_gain': (0.3 * jax.random.normal(weight_keys[6], (LAYERS, 2, D_MODEL), jnp.float32)).astype(jnp.bfloat16),
        'ln_bias': (0.3 * jax.random.normal(weight_keys[7], (LAYERS, 2, D_MODEL), jnp.float32)).astype(jnp.bfloat16),
    }


def layer_norm1p(values_in, gain, bias):
    x_float = values_in.astype(jnp.float32)
    row_mean = jnp.mean(x_float, axis=-1, keepdims=True)
    centered = x_float - row_mean
    variance = jnp.mean(centered * centered, axis=-1, keepdims=True)
    normed = centered * lax.rsqrt(variance + LN_EPS)
    return (normed * (1.0 + gain.astype(jnp.float32)) + bias.astype(jnp.float32)).astype(jnp.bfloat16)


def rotate_half(values_in, positions):
    half_rot = ROT_DIM // 2
    inv_freq = ROPE_BASE ** (-(jnp.arange(half_rot, dtype=jnp.float32) * (2.0 / ROT_DIM)))
    angles = positions.astype(jnp.float32)[..., None] * inv_freq
    cos_a = jnp.cos(angles)
    sin_a = jnp.sin(angles)
    first = values_in[..., :half_rot]
    second = values_in[..., half_rot:ROT_DIM]
    return jnp.concatenate([first * cos_a - second * sin_a, second * cos_a + first * sin_a, values_in[..., ROT_DIM:]], axis=-1)


def write_rows(cache_seq, new_rows, start_row):
    zero_idx = jnp.zeros_like(start_row)
    return lax.dynamic_update_slice(cache_seq, new_rows, (zero_idx, start_row, zero_idx))


def attend_one(item):
    q_seq, k_seq, v_seq, pos_seq = item
    key_ok = jnp.arange(CACHE_LEN, dtype=jnp.int32)[None, :] <= pos_seq[:, None]
    q_heads = jnp.transpose(q_seq, (1, 2, 0, 3))

    def one_head(head_item):
        q_head, k_head, v_head = head_item
        scores = jnp.einsum('gch,sh->gcs', q_head.astype(jnp.float32), k_head.astype(jnp.float32)) * SOFTMAX_SCALE
        scores = jnp.where(key_ok[None], scores, NEG_BIG)
        peak = jnp.max(scores, axis=-1, keepdims=True)
        weights = jnp.exp(scores - peak)
        row_sum = jnp.sum(weights, axis=-1, keepdims=True)
        context = jnp.einsum('gcs,sh->gch', weights.astype(jnp.bfloat16).astype(jnp.float32), v_head.astype(jnp.float32)) / row_sum
        return context.astype(jnp.bfloat16)

    ctx_heads = lax.map(one_head, (q_heads, k_seq, v_seq))
    return jnp.transpose(ctx_heads, (2, 0, 1, 3))


def reference(x_tokens, start_pos, k_cache, v_cache, w_q, w_k, w_v, w_o, w_up, w_down, ln_gain, ln_bias):
    positions = start_pos[:, None] + jnp.arange(NEW_TOKENS, dtype=jnp.int32)[None, :]
    rows_all = BATCH_SEQS * NEW_TOKENS

    def layer_step(hidden, layer_args):
        q_weight, k_weight, v_weight, o_weight, up_weight, down_weight, k_old, v_old, gain_pair, bias_pair = layer_args
        normed = layer_norm1p(hidden, gain_pair[0], bias_pair[0]).reshape(rows_all, D_MODEL)
        q_proj = jnp.dot(normed, q_weight, preferred_element_type=jnp.float32).reshape(BATCH_SEQS, NEW_TOKENS, N_HEADS, HEAD_DIM)
        k_proj = jnp.dot(normed, k_weight, preferred_element_type=jnp.float32).reshape(BATCH_SEQS, NEW_TOKENS, KV_HEADS, HEAD_DIM)
        v_proj = jnp.dot(normed, v_weight, preferred_element_type=jnp.float32).astype(jnp.bfloat16).reshape(BATCH_SEQS, NEW_TOKENS, KV_HEADS, HEAD_DIM)
        q_rot = rotate_half(q_proj, positions[:, :, None]).astype(jnp.bfloat16)
        k_rot = rotate_half(k_proj, positions[:, :, None]).astype(jnp.bfloat16)
        k_new = jax.vmap(write_rows)(k_old, jnp.transpose(k_rot, (0, 2, 1, 3)), start_pos)
        v_new = jax.vmap(write_rows)(v_old, jnp.transpose(v_proj, (0, 2, 1, 3)), start_pos)
        q_grouped = q_rot.reshape(BATCH_SEQS, NEW_TOKENS, KV_HEADS, GROUP_SIZE, HEAD_DIM)
        context = lax.map(attend_one, (q_grouped, k_new, v_new, positions)).reshape(rows_all, Q_WIDTH)
        attn_out = jnp.dot(context, o_weight, preferred_element_type=jnp.float32).astype(jnp.bfloat16).reshape(BATCH_SEQS, NEW_TOKENS, D_MODEL)
        after_attn = (hidden.astype(jnp.float32) + attn_out.astype(jnp.float32)).astype(jnp.bfloat16)
        normed_mlp = layer_norm1p(after_attn, gain_pair[1], bias_pair[1]).reshape(rows_all, D_MODEL)
        up_val = jnp.dot(normed_mlp, up_weight, preferred_element_type=jnp.float32)
        act_sq = jnp.square(jnp.maximum(up_val, 0.0)).astype(jnp.bfloat16)
        mlp_out = jnp.dot(act_sq, down_weight, preferred_element_type=jnp.float32).astype(jnp.bfloat16).reshape(BATCH_SEQS, NEW_TOKENS, D_MODEL)
        new_hidden = (after_attn.astype(jnp.float32) + mlp_out.astype(jnp.float32)).astype(jnp.bfloat16)
        return new_hidden, (k_new, v_new)

    hidden_out, caches_out = lax.scan(layer_step, x_tokens, (w_q, w_k, w_v, w_o, w_up, w_down, k_cache, v_cache, ln_gain, ln_bias))
    return (hidden_out, caches_out[0], caches_out[1])
```

```python
import functools
import math

import jax
import jax.numpy as jnp
from jax import lax
from jax.experimental import pallas as pl
from jax.experimental.pallas import tpu as pltpu
from jax.sharding import PartitionSpec as P

LN_EPS = 1e-5
ROPE_BASE = 10000.0
NEG_BIG = -1e30
BF = jnp.bfloat16
F32 = jnp.float32


def layer_norm1p(values_in, gain, bias):
    x_float = values_in.astype(F32)
    row_mean = jnp.mean(x_float, axis=-1, keepdims=True)
    centered = x_float - row_mean
    variance = jnp.mean(centered * centered, axis=-1, keepdims=True)
    normed = centered * lax.rsqrt(variance + LN_EPS)
    return (normed * (1.0 + gain.astype(F32)) + bias.astype(F32)).astype(BF)


def rope_tables(positions, head_dim):
    rot = head_dim // 2
    half = rot // 2
    inv_freq = ROPE_BASE ** (-(jnp.arange(half, dtype=F32) * (2.0 / rot)))
    angles = positions.astype(F32)[:, None] * inv_freq
    cos_a, sin_a = jnp.cos(angles), jnp.sin(angles)
    zero = jnp.zeros_like(sin_a)
    rest = jnp.zeros((positions.shape[0], head_dim - rot), F32)
    c_tab = jnp.concatenate([cos_a, cos_a, rest + 1.0], axis=-1)
    s_up = jnp.concatenate([zero, sin_a, rest], axis=-1)
    s_dn = jnp.concatenate([-sin_a, zero, rest], axis=-1)
    return jnp.stack([c_tab, s_up, s_dn])


def attn_kernel(layer, dims, start_ref, q_ref, k_ref, v_ref, tab_ref, kc_hbm, vc_hbm, *rest):
    kv, group, toks, hd, s_len, ch, n_ch = dims
    if layer > 0:
        rest = rest[2:]
    ctx_ref, ko_hbm, vo_hbm, kbuf, vbuf, sbuf, qbuf, mbuf, lbuf, abuf, in_sem, out_sem = rest
    b = pl.program_id(0)
    nb = pl.num_programs(0)
    slot = lax.rem(b, 2)
    other = 1 - slot
    s_pad = kbuf.shape[2]
    win = toks + 16
    rows = group * toks
    coef = (hd ** -0.5) * math.log2(math.e)

    def load(bb, sl, go):
        for i, (src, dst) in enumerate(((kc_hbm, kbuf), (vc_hbm, vbuf))):
            copy = pltpu.make_async_copy(src.at[layer, bb], dst.at[sl, :, pl.ds(0, s_len), :], in_sem.at[sl, i])
            copy.start() if go else copy.wait()

    def save(bb, sl, go):
        for i, (src, dst) in enumerate(((kbuf, ko_hbm), (vbuf, vo_hbm))):
            copy = pltpu.make_async_copy(src.at[sl, :, pl.ds(0, s_len), :], dst.at[layer, bb], out_sem.at[sl, i])
            copy.start() if go else copy.wait()

    @pl.when(b == 0)
    def _():
        load(b, slot, True)
        if s_pad > s_len:
            for sl in range(2):
                kbuf[sl, :, s_len:, :] = jnp.zeros((kv, s_pad - s_len, hd), BF)
                vbuf[sl, :, s_len:, :] = jnp.zeros((kv, s_pad - s_len, hd), BF)

    @pl.when(b > 0)
    def _():
        save(b - 1, other, False)

    @pl.when(b + 1 < nb)
    def _():
        load(b + 1, other, True)

    c_tab, s_up, s_dn = tab_ref[0], tab_ref[1], tab_ref[2]
    half = hd // 4

    def rope(x):
        return x * c_tab + pltpu.roll(x, half, 1) * s_up + pltpu.roll(x, hd - half, 1) * s_dn

    for h in range(kv):
        for g in range(group):
            j = h * group + g
            qbuf[h, g * toks:(g + 1) * toks, :] = rope(q_ref[:, j * hd:(j + 1) * hd]).astype(BF)

    start = start_ref[b]
    base = jnp.minimum((start // 16) * 16, s_len - win)
    shift = start - base
    base = pl.multiple_of(base, 16)
    row_id = lax.broadcasted_iota(jnp.int32, (win, hd), 0)
    is_new = jnp.logical_and(row_id >= shift, row_id < shift + toks)

    load(b, slot, False)
    for h in range(kv):
        cols = slice(h * hd, (h + 1) * hd)
        for buf, fresh in ((kbuf, rope(k_ref[:, cols])), (vbuf, v_ref[:, cols])):
            fresh = fresh.astype(BF).astype(F32)
            fresh = jnp.concatenate([fresh, jnp.zeros((16, hd), F32)], axis=0)
            fresh = pltpu.roll(fresh, shift, 0)
            old = buf[slot, h, pl.ds(base, win), :].astype(F32)
            buf[slot, h, pl.ds(base, win), :] = jnp.where(is_new, fresh, old).astype(BF)
    save(b, slot, True)

    mbuf[...] = jnp.full(mbuf.shape, NEG_BIG, F32)
    lbuf[...] = jnp.zeros(lbuf.shape, F32)
    abuf[...] = jnp.zeros(abuf.shape, F32)
    n_full = start // ch
    n_used = (start + toks + ch - 1) // ch

    def score_step(masked, j, carry):
        if masked:
            lane = lax.broadcasted_iota(jnp.int32, (rows, ch), 1)
            tok = lax.rem(lax.broadcasted_iota(jnp.int32, (rows, ch), 0), toks)
            ok = lane - tok <= start - j * ch
        for h in range(kv):
            keys = kbuf[slot, h, pl.ds(pl.multiple_of(j * ch, ch), ch), :]
            s = lax.dot_general(qbuf[h], keys, (((1,), (1,)), ((), ())), preferred_element_type=F32)
            if masked:
                s = jnp.where(ok, s, NEG_BIG)
            sbuf[h, j] = s
            peak = mbuf[h]
            for t in range(ch // 128):
                peak = jnp.maximum(peak, s[:, t * 128:(t + 1) * 128])
            mbuf[h] = peak
        return carry

    lax.fori_loop(0, n_full, functools.partial(score_step, False), 0)
    lax.fori_loop(n_full, n_used, functools.partial(score_step, True), 0)
    for h in range(kv):
        mbuf[h] = jnp.broadcast_to(jnp.max(mbuf[h], axis=-1, keepdims=True), (rows, 128))

    def value_step(j, carry):
        for h in range(kv):
            peak = mbuf[h]
            total = lbuf[h]
            parts = []
            for t in range(ch // 128):
                e = jnp.exp2((sbuf[h, j, :, t * 128:(t + 1) * 128] - peak) * coef)
                total = total + e
                parts.append(e.astype(BF))
            lbuf[h] = total
            vals = vbuf[slot, h, pl.ds(pl.multiple_of(j * ch, ch), ch), :]
            abuf[h] += jnp.dot(jnp.concatenate(parts, axis=1), vals, preferred_element_type=F32)
        return carry

    lax.fori_loop(0, n_used, value_step, 0)
    for h in range(kv):
        ctx = (abuf[h] / jnp.sum(lbuf[h], axis=-1, keepdims=True)).astype(BF)
        for g in range(group):
            j = h * group + g
            ctx_ref[:, j * hd:(j + 1) * hd] = ctx[g * toks:(g + 1) * toks, :]

    @pl.when(b == nb - 1)
    def _():
        save(b, slot, False)


def attend(layer, q, k, v, tabs, start_pos, k_cache, v_cache, prev):
    n_seq = start_pos.shape[0]
    _, _, kv, s_len, hd = k_cache.shape
    toks = q.shape[0] // n_seq
    group = q.shape[1] // (kv * hd)
    n_ch = -(-s_len // 640)
    ch = 128 * -(-s_len // (128 * n_ch))
    rows = group * toks
    dims = (kv, group, toks, hd, s_len, ch, n_ch)
    any_spec = pl.BlockSpec(memory_space=pl.ANY)
    row_map = lambda b, *_: (b, 0)
    cache_shape = jax.ShapeDtypeStruct(k_cache.shape, BF)
    args = [start_pos, q, k, v, tabs, k_cache, v_cache] + list(prev)
    return pl.pallas_call(
        functools.partial(attn_kernel, layer, dims),
        grid_spec=pltpu.PrefetchScalarGridSpec(
            num_scalar_prefetch=1,
            grid=(n_seq,),
            in_specs=[
                pl.BlockSpec((toks, q.shape[1]), row_map),
                pl.BlockSpec((toks, kv * hd), row_map),
                pl.BlockSpec((toks, kv * hd), row_map),
                pl.BlockSpec((3, toks, hd), lambda b, *_: (0, b, 0)),
            ] + [any_spec] * (2 + len(prev)),
            out_specs=[pl.BlockSpec((toks, q.shape[1]), row_map), any_spec, any_spec],
            scratch_shapes=[
                pltpu.VMEM((2, kv, ch * n_ch, hd), BF),
                pltpu.VMEM((2, kv, ch * n_ch, hd), BF),
                pltpu.VMEM((kv, n_ch, rows, ch), F32),
                pltpu.VMEM((kv, rows, hd), BF),
                pltpu.VMEM((kv, rows, 128), F32),
                pltpu.VMEM((kv, rows, 128), F32),
                pltpu.VMEM((kv, rows, hd), F32),
                pltpu.SemaphoreType.DMA((2, 2)),
                pltpu.SemaphoreType.DMA((2, 2)),
            ],
        ),
        out_shape=[jax.ShapeDtypeStruct(q.shape, BF), cache_shape, cache_shape],
        input_output_aliases={7: 1, 8: 2} if prev else {},
        compiler_params=pltpu.CompilerParams(vmem_limit_bytes=60 * 1024 * 1024, dimension_semantics=("arbitrary",)),
        cost_estimate=pl.CostEstimate(flops=8_000_000_000, bytes_accessed=80_000_000, transcendentals=15_000_000),
        name="attend",
    )(*args)


def solution(mesh):
    tp_size = mesh.shape['tp']
    tok_spec = P('dp', 'tp', None)
    cache_spec = P(None, 'dp', 'tp', None, None)
    col_spec = P(None, None, 'tp')
    row_spec = P(None, 'tp', None)

    def device_fn(x_loc, start_pos, k_cache, v_cache, w_q, w_k, w_v, w_o, w_up, w_down, ln_gain, ln_bias):
        n_layers = w_q.shape[0]
        n_seq, tok_loc, d_model = x_loc.shape
        new_len = tok_loc * tp_size
        rows = n_seq * new_len
        positions = (start_pos[:, None] + jnp.arange(new_len, dtype=jnp.int32)[None, :]).reshape(rows)
        tabs = rope_tables(positions, k_cache.shape[4])
        hidden = x_loc
        prev = ()
        for layer in range(n_layers):
            normed = layer_norm1p(hidden, ln_gain[layer, 0], ln_bias[layer, 0])
            normed_all = lax.all_gather(normed, 'tp', axis=1, tiled=True).reshape(rows, d_model)
            q_proj = jnp.dot(normed_all, w_q[layer], preferred_element_type=F32)
            k_proj = jnp.dot(normed_all, w_k[layer], preferred_element_type=F32)
            v_proj = jnp.dot(normed_all, w_v[layer], preferred_element_type=F32)
            context, k_out, v_out = attend(layer, q_proj, k_proj, v_proj, tabs, start_pos, k_cache, v_cache, prev)
            prev = (k_out, v_out)
            attn_part = jnp.dot(context, w_o[layer], preferred_element_type=F32).astype(BF)
            attn_part = attn_part.reshape(n_seq, new_len, d_model)
            attn_loc = lax.psum_scatter(attn_part, 'tp', scatter_dimension=1, tiled=True)
            after_attn = (hidden.astype(F32) + attn_loc.astype(F32)).astype(BF)
            normed_mlp = layer_norm1p(after_attn, ln_gain[layer, 1], ln_bias[layer, 1])
            normed_mlp_all = lax.all_gather(normed_mlp, 'tp', axis=1, tiled=True).reshape(rows, d_model)
            up_val = jnp.dot(normed_mlp_all, w_up[layer], preferred_element_type=F32)
            act_sq = jnp.square(jnp.maximum(up_val, 0.0)).astype(BF)
            mlp_part = jnp.dot(act_sq, w_down[layer], preferred_element_type=F32).astype(BF)
            mlp_part = mlp_part.reshape(n_seq, new_len, d_model)
            mlp_loc = lax.psum_scatter(mlp_part, 'tp', scatter_dimension=1, tiled=True)
            hidden = (after_attn.astype(F32) + mlp_loc.astype(F32)).astype(BF)
        return hidden, prev[0], prev[1]

    return jax.shard_map(device_fn, mesh=mesh, in_specs=(tok_spec, P('dp'), cache_spec, cache_spec, col_spec, col_spec, col_spec, row_spec, col_spec, row_spec, P(), P()), out_specs=(tok_spec, cache_spec, cache_spec), check_vma=False)
```

```python
import functools
import math

import jax
import jax.numpy as jnp
from jax import lax
from jax.experimental import pallas as pl
from jax.experimental.pallas import tpu as pltpu
from jax.sharding import PartitionSpec as P

LN_EPS = 1e-5
ROPE_BASE = 10000.0
NEG_BIG = -1e30
BF = jnp.bfloat16
F32 = jnp.float32


def rope_tables(positions, head_dim):
    rot = head_dim // 2
    half = rot // 2
    inv_freq = ROPE_BASE ** (-(jnp.arange(half, dtype=F32) * (2.0 / rot)))
    angles = positions.astype(F32)[:, None] * inv_freq
    cos_a, sin_a = jnp.cos(angles), jnp.sin(angles)
    zero = jnp.zeros_like(sin_a)
    rest = jnp.zeros((positions.shape[0], head_dim - rot), F32)
    c_tab = jnp.concatenate([cos_a, cos_a, rest + 1.0], axis=-1)
    s_up = jnp.concatenate([zero, sin_a, rest], axis=-1)
    s_dn = jnp.concatenate([-sin_a, zero, rest], axis=-1)
    return jnp.stack([c_tab, s_up, s_dn])


def attn_kernel(layer, dims, start_ref, q_ref, k_ref, v_ref, tab_ref, kc_hbm, vc_hbm, *rest):
    kv, group, toks, hd, s_len, ch, n_ch = dims
    if layer > 0:
        rest = rest[2:]
    ctx_ref, ko_hbm, vo_hbm, kbuf, vbuf, sbuf, qbuf, mbuf, lbuf, abuf, in_sem, out_sem = rest
    b = pl.program_id(0)
    nb = pl.num_programs(0)
    slot = lax.rem(b, 2)
    other = 1 - slot
    s_pad = kbuf.shape[2]
    win = toks + 16
    rows = group * toks
    coef = (hd ** -0.5) * math.log2(math.e)

    def load(bb, sl, go):
        for i, (src, dst) in enumerate(((kc_hbm, kbuf), (vc_hbm, vbuf))):
            copy = pltpu.make_async_copy(src.at[layer, bb], dst.at[sl, :, pl.ds(0, s_len), :], in_sem.at[sl, i])
            copy.start() if go else copy.wait()

    def save(bb, sl, go):
        for i, (src, dst) in enumerate(((kbuf, ko_hbm), (vbuf, vo_hbm))):
            copy = pltpu.make_async_copy(src.at[sl, :, pl.ds(0, s_len), :], dst.at[layer, bb], out_sem.at[sl, i])
            copy.start() if go else copy.wait()

    @pl.when(b == 0)
    def _():
        load(b, slot, True)
        if s_pad > s_len:
            for sl in range(2):
                kbuf[sl, :, s_len:, :] = jnp.zeros((kv, s_pad - s_len, hd), BF)
                vbuf[sl, :, s_len:, :] = jnp.zeros((kv, s_pad - s_len, hd), BF)

    @pl.when(b > 0)
    def _():
        save(b - 1, other, False)

    @pl.when(b + 1 < nb)
    def _():
        load(b + 1, other, True)

    c_tab, s_up, s_dn = tab_ref[0], tab_ref[1], tab_ref[2]
    half = hd // 4

    def rope(x):
        return x * c_tab + pltpu.roll(x, half, 1) * s_up + pltpu.roll(x, hd - half, 1) * s_dn

    for h in range(kv):
        for g in range(group):
            j = h * group + g
            qbuf[h, g * toks:(g + 1) * toks, :] = rope(q_ref[:, j * hd:(j + 1) * hd]).astype(BF)

    start = start_ref[b]
    base = jnp.minimum((start // 16) * 16, s_len - win)
    shift = start - base
    base = pl.multiple_of(base, 16)
    row_id = lax.broadcasted_iota(jnp.int32, (win, hd), 0)
    is_new = jnp.logical_and(row_id >= shift, row_id < shift + toks)

    load(b, slot, False)
    for h in range(kv):
        cols = slice(h * hd, (h + 1) * hd)
        for buf, fresh in ((kbuf, rope(k_ref[:, cols])), (vbuf, v_ref[:, cols])):
            fresh = fresh.astype(BF).astype(F32)
            fresh = jnp.concatenate([fresh, jnp.zeros((16, hd), F32)], axis=0)
            fresh = pltpu.roll(fresh, shift, 0)
            old = buf[slot, h, pl.ds(base, win), :].astype(F32)
            buf[slot, h, pl.ds(base, win), :] = jnp.where(is_new, fresh, old).astype(BF)
    save(b, slot, True)

    mbuf[...] = jnp.full(mbuf.shape, NEG_BIG, F32)
    lbuf[...] = jnp.zeros(lbuf.shape, F32)
    abuf[...] = jnp.zeros(abuf.shape, F32)
    n_full = start // ch
    n_used = (start + toks + ch - 1) // ch

    def score_step(masked, j, carry):
        if masked:
            lane = lax.broadcasted_iota(jnp.int32, (rows, ch), 1)
            tok = lax.rem(lax.broadcasted_iota(jnp.int32, (rows, ch), 0), toks)
            ok = lane - tok <= start - j * ch
        for h in range(kv):
            keys = kbuf[slot, h, pl.ds(pl.multiple_of(j * ch, ch), ch), :]
            s = lax.dot_general(qbuf[h], keys, (((1,), (1,)), ((), ())), preferred_element_type=F32)
            if masked:
                s = jnp.where(ok, s, NEG_BIG)
            sbuf[h, j] = s
            peak = mbuf[h]
            for t in range(ch // 128):
                peak = jnp.maximum(peak, s[:, t * 128:(t + 1) * 128])
            mbuf[h] = peak
        return carry

    lax.fori_loop(0, n_full, functools.partial(score_step, False), 0)
    lax.fori_loop(n_full, n_used, functools.partial(score_step, True), 0)
    for h in range(kv):
        mbuf[h] = jnp.broadcast_to(jnp.max(mbuf[h], axis=-1, keepdims=True), (rows, 128))

    def value_step(j, carry):
        for h in range(kv):
            peak = mbuf[h]
            total = lbuf[h]
            parts = []
            for t in range(ch // 128):
                e = jnp.exp2((sbuf[h, j, :, t * 128:(t + 1) * 128] - peak) * coef)
                total = total + e
                parts.append(e.astype(BF))
            lbuf[h] = total
            vals = vbuf[slot, h, pl.ds(pl.multiple_of(j * ch, ch), ch), :]
            abuf[h] += jnp.dot(jnp.concatenate(parts, axis=1), vals, preferred_element_type=F32)
        return carry

    lax.fori_loop(0, n_used, value_step, 0)
    for h in range(kv):
        ctx = (abuf[h] / jnp.sum(lbuf[h], axis=-1, keepdims=True)).astype(BF)
        for g in range(group):
            j = h * group + g
            ctx_ref[:, j * hd:(j + 1) * hd] = ctx[g * toks:(g + 1) * toks, :]

    @pl.when(b == nb - 1)
    def _():
        save(b, slot, False)


def attend(layer, qkv, tabs, start_pos, k_cache, v_cache, prev):
    n_seq = start_pos.shape[0]
    _, _, kv, s_len, hd = k_cache.shape
    toks = qkv.shape[0] // n_seq
    kv_width = kv * hd
    q_width = qkv.shape[1] - 2 * kv_width
    group = q_width // kv_width
    n_ch = -(-s_len // 640)
    ch = 128 * -(-s_len // (128 * n_ch))
    rows = group * toks
    dims = (kv, group, toks, hd, s_len, ch, n_ch)
    any_spec = pl.BlockSpec(memory_space=pl.ANY)
    row_map = lambda b, *_: (b, 0)
    cache_shape = jax.ShapeDtypeStruct(k_cache.shape, BF)
    args = [start_pos, qkv, qkv, qkv, tabs, k_cache, v_cache] + list(prev)
    return pl.pallas_call(
        functools.partial(attn_kernel, layer, dims),
        grid_spec=pltpu.PrefetchScalarGridSpec(
            num_scalar_prefetch=1,
            grid=(n_seq,),
            in_specs=[
                pl.BlockSpec((toks, q_width), row_map),
                pl.BlockSpec((toks, kv_width), lambda b, *_: (b, group)),
                pl.BlockSpec((toks, kv_width), lambda b, *_: (b, group + 1)),
                pl.BlockSpec((3, toks, hd), lambda b, *_: (0, b, 0)),
            ] + [any_spec] * (2 + len(prev)),
            out_specs=[pl.BlockSpec((toks, q_width), row_map), any_spec, any_spec],
            scratch_shapes=[
                pltpu.VMEM((2, kv, ch * n_ch, hd), BF),
                pltpu.VMEM((2, kv, ch * n_ch, hd), BF),
                pltpu.VMEM((kv, n_ch, rows, ch), F32),
                pltpu.VMEM((kv, rows, hd), BF),
                pltpu.VMEM((kv, rows, 128), F32),
                pltpu.VMEM((kv, rows, 128), F32),
                pltpu.VMEM((kv, rows, hd), F32),
                pltpu.SemaphoreType.DMA((2, 2)),
                pltpu.SemaphoreType.DMA((2, 2)),
            ],
        ),
        out_shape=[jax.ShapeDtypeStruct((n_seq * toks, q_width), BF), cache_shape, cache_shape],
        input_output_aliases={7: 1, 8: 2} if prev else {},
        compiler_params=pltpu.CompilerParams(vmem_limit_bytes=60 * 1024 * 1024, dimension_semantics=("arbitrary",)),
        cost_estimate=pl.CostEstimate(flops=8_000_000_000, bytes_accessed=80_000_000, transcendentals=15_000_000),
        name="attend",
    )(*args)


STEPS = 8


def exchange_kernel(cfg, *args):
    refs = dict(zip(cfg['names'], args))
    layer, g_layer, ln_row = cfg['layer'], cfg['g_layer'], cfg['ln_row']
    scatter, gather = cfg['scatter'], cfg['gather']
    n_seq, toks, d_model = cfg['n_seq'], cfg['toks'], cfg['d_model']
    rows = n_seq * toks
    blk = d_model // STEPS
    me = lax.axis_index('tp')
    core = lax.rem(me, 2)
    partner = me + 1 - 2 * core
    counter = lax.rem(me + 2, 4)
    diag = lax.rem(partner + 2, 4)
    order = (me, partner, counter, diag)
    wbuf, xbuf = refs['wbuf'], refs['xbuf']

    barrier = pltpu.get_barrier_semaphore()
    for peer in (partner, counter):
        pl.semaphore_signal(barrier, inc=1, device_id={'tp': peer}, device_id_type=pl.DeviceIdType.MESH)

    def col(n, width=blk):
        return pl.ds(pl.multiple_of(n * width, width), width)

    x_copy = pltpu.make_async_copy(refs['x_hbm'], xbuf, refs['x_sem'])

    if scatter:
        depth = cfg['depth']
        abuf, w_s = refs['abuf'], refs['w_s']
        a_copies = [pltpu.make_async_copy(refs['a_hbm'].at[:, order[g]], abuf.at[g], refs['a_sem'].at[g]) for g in range(4)]

        def w_copy(n):
            return pltpu.make_async_copy(w_s.at[layer, :, col(n)], wbuf.at[pl.ds(0, depth), col(n)], refs['sw_sem'].at[n])

        for g in (2, 3):
            a_copies[g].start()
        w_copy(0).start()
        for g in (0, 1):
            a_copies[g].start()
        for n in range(1, STEPS):
            w_copy(n).start()
    x_copy.start()

    g_copies = []
    if gather:
        if cfg['kind'] == 'up':
            cut = depth
            for i, (lo, hi) in enumerate(((cut, d_model), (0, cut))):
                span = pl.ds(lo, hi - lo)
                g_copies.append(pltpu.make_async_copy(refs['w_up'].at[g_layer, span, :], wbuf.at[span, :], refs['gw_sem'].at[i]))
        else:
            at = 0
            for i, name in enumerate(('w_q', 'w_k', 'w_v')):
                width = refs[name].shape[2]
                g_copies.append(pltpu.make_async_copy(refs[name].at[g_layer], wbuf.at[:, pl.ds(at, width)], refs['gw_sem'].at[i]))
                at += width
        if not scatter:
            for copy in g_copies:
                copy.start()
        elif cfg['kind'] == 'up':
            g_copies[0].start()

    def remote(src, dst, send, recv, peer):
        return pltpu.make_async_remote_copy(src_ref=src, dst_ref=dst, send_sem=send, recv_sem=recv, device_id={'tp': peer}, device_id_type=pl.DeviceIdType.MESH)

    pl.semaphore_wait(barrier, 2)

    if scatter:
        dsend, drecv, qsend, qrecv, own = refs['dsend'], refs['drecv'], refs['qsend'], refs['qrecv'], refs['own']
        part = refs['part']

        def d_copy(n, i):
            return remote(dsend.at[n, i], drecv.at[n, i], refs['ds_sem'].at[n, i], refs['dr_sem'].at[n, i], partner)

        def q_copy(n):
            return remote(qsend.at[n], qrecv.at[n], refs['qs_sem'].at[n], refs['qr_sem'].at[n], counter)

        for copy in a_copies:
            copy.wait()

        def s_step(n, carry):
            w_copy(n).wait()
            far = jnp.dot(abuf[2:4].reshape(2 * rows, depth), wbuf[0:depth, col(n)], preferred_element_type=F32)
            dsend[n, 0] = far[rows:].astype(BF)
            d_copy(n, 0).start()
            part[...] = far[:rows]
            near = jnp.dot(abuf[0:2].reshape(2 * rows, depth), wbuf[0:depth, col(n)], preferred_element_type=F32)
            dsend[n, 1] = near[rows:].astype(BF)
            d_copy(n, 1).start()
            own[n] = near[:rows]
            d_copy(n, 0).wait_recv()
            qsend[n] = (part[...] + drecv[n, 0].astype(F32)).astype(BF)
            q_copy(n).start()
            return carry

        half = STEPS // 2
        lax.fori_loop(0, half, s_step, 0)
        if gather and cfg['kind'] == 'qkv':
            for copy in g_copies:
                copy.start()
        lax.fori_loop(half, STEPS, s_step, 0)
        if gather and cfg['kind'] == 'up':
            g_copies[1].start()

    x_copy.wait()
    total = jnp.zeros((rows, 128), F32)
    for n in range(STEPS):
        cols = slice(n * blk, (n + 1) * blk)
        if scatter:
            d_copy(n, 1).wait_recv()
            q_copy(n).wait_recv()
            summed = own[n] + drecv[n, 1].astype(F32) + qrecv[n].astype(F32)
            fresh = (xbuf[:, cols].astype(F32) + summed.astype(BF).astype(F32)).astype(BF)
            xbuf[:, cols] = fresh
        else:
            fresh = xbuf[:, cols]
        fresh = fresh.astype(F32)
        for j in range(blk // 128):
            total = total + fresh[:, j * 128:(j + 1) * 128]
    if scatter:
        out_copy = pltpu.make_async_copy(xbuf, refs['x_out'], refs['x_sem'])
        out_copy.start()

    if gather:
        near_h, far_h, acc, stage, y_out = refs['near_h'], refs['far_h'], refs['acc'], refs['stage'], refs['y_out']
        n_out = acc.shape[1]
        mean = jnp.sum(total, axis=-1, keepdims=True) / d_model
        total = jnp.zeros((rows, 128), F32)
        for n in range(STEPS):
            diff = xbuf[:, n * blk:(n + 1) * blk].astype(F32) - mean
            diff = diff * diff
            for j in range(blk // 128):
                total = total + diff[:, j * 128:(j + 1) * 128]
        inv = lax.rsqrt(jnp.sum(total, axis=-1, keepdims=True) / d_model + LN_EPS)

        def c_copy(k):
            return remote(near_h.at[pl.ds(0, rows), col(k)], far_h.at[pl.ds(0, rows), col(k)], refs['cs_sem'].at[k], refs['cr_sem'].at[k], counter)

        def f_copy(k):
            return remote(far_h.at[pl.ds(0, rows), col(k)], far_h.at[pl.ds(rows, rows), col(k)], refs['fs_sem'].at[k], refs['fr_sem'].at[k], partner)

        def p_copy(k):
            return remote(near_h.at[pl.ds(0, rows), col(k)], near_h.at[pl.ds(rows, rows), col(k)], refs['ps_sem'].at[k], refs['pr_sem'].at[k], partner)

        for k in range(STEPS):
            cols = slice(k * blk, (k + 1) * blk)
            gain = refs['ln_gain'][ln_row:ln_row + 1, cols].astype(F32)
            bias = refs['ln_bias'][ln_row:ln_row + 1, cols].astype(F32)
            normed = (xbuf[:, cols].astype(F32) - mean) * inv
            near_h[0:rows, cols] = (normed * (1.0 + gain) + bias).astype(BF)
            if k:
                c_copy(k - 1).start()
                p_copy(k - 1).start()
        acc[...] = jnp.zeros(acc.shape, F32)
        c_copy(STEPS - 1).start()
        p_copy(STEPS - 1).start()

        for copy in g_copies:
            copy.wait()
        for k in range(STEPS):
            p_copy(k).wait_recv()

        def finish(value):
            if cfg['kind'] == 'up':
                value = jnp.square(jnp.maximum(value, 0.0)).astype(BF)
            return value.reshape(2, n_seq, toks, value.shape[-1])

        n_blk = n_out // STEPS

        def y_copy(g, n):
            return pltpu.make_async_copy(stage.at[g, :, :, col(n, n_blk)], y_out.at[:, order[g], :, col(n, n_blk)], refs['y_sem'].at[g, n])

        piece = min(1024, n_out)

        def far_dot(k, cols):
            return jnp.dot(far_h[:, col(k)], wbuf[col(k), cols], preferred_element_type=F32)

        def near_step(i):
            near = jnp.dot(near_h[...], wbuf[:, col(i, n_blk)], preferred_element_type=F32)
            stage[0:2, :, :, col(i, n_blk)] = finish(near)
            y_copy(0, i).start()
            y_copy(1, i).start()
            c_copy(i).wait_recv()
            f_copy(i).start()

        def g_step(i, carry):
            near_step(i)
            f_copy(i - 1).wait_recv()
            for n in range(n_out // piece):
                cols = slice(n * piece, (n + 1) * piece)
                acc[:, cols] += far_dot(i - 1, cols)
            return carry

        near_step(0)
        lax.fori_loop(1, STEPS, g_step, 0)
        f_copy(STEPS - 1).wait_recv()
        for n in range(n_out // piece):
            cols = slice(n * piece, (n + 1) * piece)
            stage[2:4, :, :, cols] = finish(acc[:, cols] + far_dot(STEPS - 1, cols))
            for m in range(n * piece // n_blk, (n + 1) * piece // n_blk):
                y_copy(2, m).start()
                y_copy(3, m).start()
        for k in range(STEPS):
            c_copy(k).wait_send()
            p_copy(k).wait_send()
            f_copy(k).wait_send()
            for g in range(4):
                y_copy(g, k).wait()

    if scatter:
        for n in range(STEPS):
            d_copy(n, 0).wait_send()
            d_copy(n, 1).wait_send()
            q_copy(n).wait_send()
        out_copy.wait()


def exchange(cid, x, ln_gain, ln_bias, *, n_seq, layer=0, a=None, w_s=None, g_layer=0, ln_row=0, kind=None, weights=()):
    rows, d_model = x.shape
    toks = rows // n_seq
    blk = d_model // STEPS
    scatter, gather = a is not None, kind is not None
    any_spec, vmem = pl.BlockSpec(memory_space=pl.ANY), pl.BlockSpec(memory_space=pltpu.VMEM)
    dma = pltpu.SemaphoreType.DMA
    ins, outs, scr = [('x_hbm', x, any_spec)], [], []
    flops, moved = 0, 4_000_000
    scr += [('wbuf', None), ('xbuf', pltpu.VMEM((rows, d_model), BF)), ('x_sem', dma)]
    width = 0
    if scatter:
        depth = a.shape[3]
        ins += [('a_hbm', a, any_spec), ('w_s', w_s, any_spec)]
        outs += [('x_out', jax.ShapeDtypeStruct(x.shape, BF))]
        scr += [
            ('abuf', pltpu.VMEM((4, n_seq, toks, depth), BF)), ('a_sem', dma((4,))), ('sw_sem', dma((STEPS,))),
            ('dsend', pltpu.VMEM((STEPS, 2, rows, blk), BF)), ('drecv', pltpu.VMEM((STEPS, 2, rows, blk), BF)),
            ('qsend', pltpu.VMEM((STEPS, rows, blk), BF)), ('qrecv', pltpu.VMEM((STEPS, rows, blk), BF)),
            ('own', pltpu.VMEM((STEPS, rows, blk), F32)), ('part', pltpu.VMEM((rows, blk), F32)),
            ('ds_sem', dma((STEPS, 2))), ('dr_sem', dma((STEPS, 2))), ('qs_sem', dma((STEPS,))), ('qr_sem', dma((STEPS,))),
        ]
        width = d_model
        w_rows = depth
        flops += 2 * 4 * rows * depth * d_model
        moved += depth * d_model * 2
    if gather:
        names = ('w_up',) if kind == 'up' else ('w_q', 'w_k', 'w_v')
        ins += list(zip(names, weights, [any_spec] * len(names)))
        ins += [('ln_gain', ln_gain, vmem), ('ln_bias', ln_bias, vmem)]
        n_out = sum(w.shape[2] for w in weights)
        y_type = BF if kind == 'up' else F32
        outs += [('y_out', jax.ShapeDtypeStruct((n_seq, 4, toks, n_out), y_type))]
        scr += [
            ('near_h', pltpu.VMEM((2 * rows, d_model), BF)), ('far_h', pltpu.VMEM((2 * rows, d_model), BF)),
            ('acc', pltpu.VMEM((2 * rows, n_out), F32)), ('stage', pltpu.VMEM((4, n_seq, toks, n_out), y_type)),
            ('gw_sem', dma((3,))), ('y_sem', dma((4, STEPS))),
        ] + [(s, dma((STEPS,))) for s in ('cs_sem', 'cr_sem', 'fs_sem', 'fr_sem', 'ps_sem', 'pr_sem')]
        width = max(width, n_out)
        w_rows = d_model
        flops += 2 * 4 * rows * n_out * d_model
        moved += n_out * d_model * 2
    scr[0] = ('wbuf', pltpu.VMEM((w_rows, width), BF))
    cfg = dict(
        names=[i[0] for i in ins] + [o[0] for o in outs] + [s[0] for s in scr], layer=layer, g_layer=g_layer, ln_row=ln_row,
        scatter=scatter, gather=gather, n_seq=n_seq, toks=toks, d_model=d_model, kind=kind, depth=depth if scatter else 0,
    )
    return pl.pallas_call(
        functools.partial(exchange_kernel, cfg),
        in_specs=[i[2] for i in ins],
        out_specs=[any_spec] * len(outs),
        out_shape=[o[1] for o in outs],
        scratch_shapes=[s[1] for s in scr],
        compiler_params=pltpu.CompilerParams(collective_id=cid, has_side_effects=True, vmem_limit_bytes=66_000_000),
        cost_estimate=pl.CostEstimate(flops=flops, bytes_accessed=moved, transcendentals=0),
        name=('scatter_' if scatter else '') + ('gather_' + kind if gather else 'end'),
    )(*[i[1] for i in ins])


def solution(mesh):
    tok_spec = P('dp', 'tp', None)
    cache_spec = P(None, 'dp', 'tp', None, None)
    col_spec = P(None, None, 'tp')
    row_spec = P(None, 'tp', None)

    def device_fn(x_loc, start_pos, k_cache, v_cache, w_q, w_k, w_v, w_o, w_up, w_down, ln_gain, ln_bias):
        n_layers = w_q.shape[0]
        n_seq, tok_loc, d_model = x_loc.shape
        new_len = tok_loc * 4
        rows = n_seq * new_len
        positions = (start_pos[:, None] + jnp.arange(new_len, dtype=jnp.int32)[None, :]).reshape(rows)
        tabs = rope_tables(positions, k_cache.shape[4])
        gain, bias = ln_gain.reshape(2 * n_layers, d_model), ln_bias.reshape(2 * n_layers, d_model)
        hidden = x_loc.reshape(n_seq * tok_loc, d_model)
        prev = ()
        qkv, = exchange(0, hidden, gain, bias, n_seq=n_seq, kind='qkv', weights=(w_q, w_k, w_v))
        for layer in range(n_layers):
            context, *prev = attend(layer, qkv.reshape(rows, -1), tabs, start_pos, k_cache, v_cache, prev)
            context = context.reshape(n_seq, 4, tok_loc, -1)
            hidden, act = exchange(2 * layer + 1, hidden, gain, bias, n_seq=n_seq, layer=layer, a=context, w_s=w_o, g_layer=layer, ln_row=2 * layer + 1, kind='up', weights=(w_up,))
            if layer + 1 < n_layers:
                hidden, qkv = exchange(2 * layer + 2, hidden, gain, bias, n_seq=n_seq, layer=layer, a=act, w_s=w_down, g_layer=layer + 1, ln_row=2 * layer + 2, kind='qkv', weights=(w_q, w_k, w_v))
            else:
                hidden, = exchange(2 * layer + 2, hidden, gain, bias, n_seq=n_seq, layer=layer, a=act, w_s=w_down)
        return hidden.reshape(x_loc.shape), prev[0], prev[1]

    return jax.shard_map(device_fn, mesh=mesh, in_specs=(tok_spec, P('dp'), cache_spec, cache_spec, col_spec, col_spec, col_spec, row_spec, col_spec, row_spec, P(), P()), out_specs=(tok_spec, cache_spec, cache_spec), check_vma=False)
```

```python
import functools
import math

import jax
import jax.numpy as jnp
from jax import lax
from jax.experimental import pallas as pl
from jax.experimental.pallas import tpu as pltpu
from jax.sharding import PartitionSpec as P

LN_EPS = 1e-5
ROPE_BASE = 10000.0
NEG_BIG = -1e30
BF = jnp.bfloat16
F32 = jnp.float32


def rope_tables(positions, head_dim):
    rot = head_dim // 2
    half = rot // 2
    lane = jnp.arange(head_dim, dtype=jnp.int32)
    freq = ROPE_BASE ** (-((lane % half).astype(F32) * (2.0 / rot)))
    angles = positions.astype(F32)[:, None] * freq
    cos_a, sin_a = jnp.cos(angles), jnp.sin(angles)
    c_tab = jnp.where(lane < rot, cos_a, 1.0)
    s_up = jnp.where((lane >= half) & (lane < rot), sin_a, 0.0)
    s_dn = jnp.where(lane < half, -sin_a, 0.0)
    return jnp.stack([c_tab, s_up, s_dn])


def attn_kernel(layer, dims, start_ref, q_ref, k_ref, v_ref, tab_ref, kc_hbm, vc_hbm, *rest):
    kv, group, toks, hd, s_len, ch, n_ch = dims
    if layer > 0:
        rest = rest[2:]
    ctx_ref, ko_hbm, vo_hbm, kbuf, vbuf, sbuf, qbuf, mbuf, pbuf, lbuf, abuf, in_sem, out_sem = rest
    b = pl.program_id(0)
    nb = pl.num_programs(0)
    slot = lax.rem(b, 2)
    other = 1 - slot
    s_pad = kbuf.shape[2]
    win = toks + 16
    rows = group * toks
    coef = (hd ** -0.5) * math.log2(math.e)

    def load(bb, sl, go):
        for i, (src, dst) in enumerate(((kc_hbm, kbuf), (vc_hbm, vbuf))):
            copy = pltpu.make_async_copy(src.at[layer, bb], dst.at[sl, :, pl.ds(0, s_len), :], in_sem.at[sl, i])
            copy.start() if go else copy.wait()

    def save(bb, sl, go):
        for i, (src, dst) in enumerate(((kbuf, ko_hbm), (vbuf, vo_hbm))):
            copy = pltpu.make_async_copy(src.at[sl, :, pl.ds(0, s_len), :], dst.at[layer, bb], out_sem.at[sl, i])
            copy.start() if go else copy.wait()

    @pl.when(b == 0)
    def _():
        load(b, slot, True)
        if s_pad > s_len:
            for sl in range(2):
                kbuf[sl, :, s_len:, :] = jnp.zeros((kv, s_pad - s_len, hd), BF)
                vbuf[sl, :, s_len:, :] = jnp.zeros((kv, s_pad - s_len, hd), BF)

    @pl.when(b > 0)
    def _():
        save(b - 1, other, False)

    @pl.when(b + 1 < nb)
    def _():
        load(b + 1, other, True)

    c_tab, s_up, s_dn = tab_ref[0], tab_ref[1], tab_ref[2]
    half = hd // 4

    def rope(x):
        return x * c_tab + pltpu.roll(x, half, 1) * s_up + pltpu.roll(x, hd - half, 1) * s_dn

    for h in range(kv):
        for g in range(group):
            j = h * group + g
            qbuf[h, g * toks:(g + 1) * toks, :] = rope(q_ref[:, j * hd:(j + 1) * hd]).astype(BF)

    start = start_ref[b]
    base = jnp.minimum((start // 16) * 16, s_len - win)
    shift = start - base
    base = pl.multiple_of(base, 16)
    row_id = lax.broadcasted_iota(jnp.int32, (win, hd), 0)
    is_new = jnp.logical_and(row_id >= shift, row_id < shift + toks)

    load(b, slot, False)
    for h in range(kv):
        cols = slice(h * hd, (h + 1) * hd)
        for buf, fresh in ((kbuf, rope(k_ref[:, cols])), (vbuf, v_ref[:, cols])):
            fresh = fresh.astype(BF).astype(F32)
            fresh = jnp.concatenate([fresh, jnp.zeros((16, hd), F32)], axis=0)
            fresh = pltpu.roll(fresh, shift, 0)
            old = buf[slot, h, pl.ds(base, win), :].astype(F32)
            buf[slot, h, pl.ds(base, win), :] = jnp.where(is_new, fresh, old).astype(BF)
    save(b, slot, True)

    mbuf[...] = jnp.full(mbuf.shape, NEG_BIG, F32)
    lbuf[...] = jnp.zeros(lbuf.shape, F32)
    abuf[...] = jnp.zeros(abuf.shape, F32)
    n_full = jnp.maximum(start // ch, 1)
    n_used = (start + toks + ch - 1) // ch
    lanes = [slice(t * 128, (t + 1) * 128) for t in range(ch // 128)]

    def scores(h, j, masked):
        into = lax.rem(j, 2)
        keys = kbuf[slot, h, pl.ds(pl.multiple_of(j * ch, ch), ch), :]
        s = lax.dot_general(qbuf[h], keys, (((1,), (1,)), ((), ())), preferred_element_type=F32)
        if masked:
            lane = lax.broadcasted_iota(jnp.int32, (rows, ch), 1)
            tok = lax.rem(lax.broadcasted_iota(jnp.int32, (rows, ch), 0), toks)
            s = jnp.where(lane - tok <= start - j * ch, s, NEG_BIG)
        sbuf[h, into] = s
        top = s[:, lanes[0]]
        for t in lanes[1:]:
            top = jnp.maximum(top, s[:, t])
        return jnp.broadcast_to(jnp.max(top, axis=-1, keepdims=True), (rows, 128))

    def values(h, j, last):
        here = lax.rem(j, 2)
        old, peak = mbuf[h], pbuf[h]
        alpha = jnp.exp2((old - peak) * coef)
        total = lbuf[h] * alpha
        parts = []
        for t in lanes:
            e = jnp.exp2((sbuf[h, here, :, t] - peak) * coef)
            total = total + e
            parts.append(e.astype(BF))
        vals = vbuf[slot, h, pl.ds(pl.multiple_of(j * ch, ch), ch), :]
        mixed = abuf[h] * alpha + jnp.dot(jnp.concatenate(parts, axis=1), vals, preferred_element_type=F32)
        lbuf[h] = total
        abuf[h] = mixed
        if not last:
            mbuf[h] = peak

    def step(masked, j, carry):
        tops = [scores(h, j + 1, masked) for h in range(kv)]
        for h in range(kv):
            values(h, j, False)
        for h in range(kv):
            pbuf[h] = jnp.maximum(pbuf[h], tops[h])
        return carry

    for h in range(kv):
        pbuf[h] = scores(h, 0, True)
    lax.fori_loop(0, n_full - 1, functools.partial(step, False), 0)
    lax.fori_loop(n_full - 1, n_used - 1, functools.partial(step, True), 0)
    for h in range(kv):
        values(h, n_used - 1, True)
    for h in range(kv):
        ctx = (abuf[h] / jnp.sum(lbuf[h], axis=-1, keepdims=True)).astype(BF)
        for g in range(group):
            j = h * group + g
            ctx_ref[:, j * hd:(j + 1) * hd] = ctx[g * toks:(g + 1) * toks, :]

    @pl.when(b == nb - 1)
    def _():
        save(b, slot, False)


def attend(layer, qkv, tabs, start_pos, k_cache, v_cache, prev):
    n_seq = start_pos.shape[0]
    _, _, kv, s_len, hd = k_cache.shape
    toks = qkv.shape[0] // n_seq
    kv_width = kv * hd
    q_width = qkv.shape[1] - 2 * kv_width
    group = q_width // kv_width
    n_ch = -(-s_len // 640)
    ch = 128 * -(-s_len // (128 * n_ch))
    rows = group * toks
    dims = (kv, group, toks, hd, s_len, ch, n_ch)
    any_spec = pl.BlockSpec(memory_space=pl.ANY)
    row_map = lambda b, *_: (b, 0)
    cache_shape = jax.ShapeDtypeStruct(k_cache.shape, BF)
    args = [start_pos, qkv, qkv, qkv, tabs, k_cache, v_cache] + list(prev)
    return pl.pallas_call(
        functools.partial(attn_kernel, layer, dims),
        grid_spec=pltpu.PrefetchScalarGridSpec(
            num_scalar_prefetch=1,
            grid=(n_seq,),
            in_specs=[
                pl.BlockSpec((toks, q_width), row_map),
                pl.BlockSpec((toks, kv_width), lambda b, *_: (b, group)),
                pl.BlockSpec((toks, kv_width), lambda b, *_: (b, group + 1)),
                pl.BlockSpec((3, toks, hd), lambda b, *_: (0, b, 0)),
            ] + [any_spec] * (2 + len(prev)),
            out_specs=[pl.BlockSpec((toks, q_width), row_map), any_spec, any_spec],
            scratch_shapes=[
                pltpu.VMEM((2, kv, ch * n_ch, hd), BF),
                pltpu.VMEM((2, kv, ch * n_ch, hd), BF),
                pltpu.VMEM((kv, 2, rows, ch), F32),
                pltpu.VMEM((kv, rows, hd), BF),
                pltpu.VMEM((kv, rows, 128), F32),
                pltpu.VMEM((kv, rows, 128), F32),
                pltpu.VMEM((kv, rows, 128), F32),
                pltpu.VMEM((kv, rows, hd), F32),
                pltpu.SemaphoreType.DMA((2, 2)),
                pltpu.SemaphoreType.DMA((2, 2)),
            ],
        ),
        out_shape=[jax.ShapeDtypeStruct((n_seq * toks, q_width), BF), cache_shape, cache_shape],
        input_output_aliases={7: 1, 8: 2} if prev else {},
        compiler_params=pltpu.CompilerParams(vmem_limit_bytes=60 * 1024 * 1024, dimension_semantics=("arbitrary",)),
        cost_estimate=pl.CostEstimate(flops=8_000_000_000, bytes_accessed=80_000_000, transcendentals=15_000_000),
        name="attend",
    )(*args)


STEPS = 8
AHEAD = 3


def exchange_kernel(cfg, *args):
    refs = dict(zip(cfg['names'], args))
    layer, g_layer, ln_row = cfg['layer'], cfg['g_layer'], cfg['ln_row']
    scatter, gather = cfg['scatter'], cfg['gather']
    n_seq, toks, d_model = cfg['n_seq'], cfg['toks'], cfg['d_model']
    rows = n_seq * toks
    blk = d_model // STEPS
    me = lax.axis_index('tp')
    core = lax.rem(me, 2)
    partner = me + 1 - 2 * core
    counter = lax.rem(me + 2, 4)
    diag = lax.rem(partner + 2, 4)
    order = (me, partner, counter, diag)
    wbuf, xbuf = refs['wbuf'], refs['xbuf']

    barrier = pltpu.get_barrier_semaphore()
    for peer in (partner, counter):
        pl.semaphore_signal(barrier, inc=1, device_id={'tp': peer}, device_id_type=pl.DeviceIdType.MESH)

    def col(n, width=blk):
        return pl.ds(pl.multiple_of(n * width, width), width)

    x_copy = pltpu.make_async_copy(refs['x_hbm'], xbuf, refs['x_sem'])

    if scatter:
        depth = cfg['depth']
        abuf, w_s = refs['abuf'], refs['w_s']
        a_copies = [pltpu.make_async_copy(refs['a_hbm'].at[:, order[g]], abuf.at[g], refs['a_sem'].at[g]) for g in range(4)]

        def w_copy(n):
            return pltpu.make_async_copy(w_s.at[layer, :, col(n)], wbuf.at[pl.ds(0, depth), col(n)], refs['sw_sem'].at[n])

        for g in (2, 3):
            a_copies[g].start()
        w_copy(0).start()
        for g in (0, 1):
            a_copies[g].start()
        for n in range(1, AHEAD):
            w_copy(n).start()
    x_copy.start()

    g_copies = []
    if gather:
        if cfg['kind'] == 'up':
            cut = depth
            for i, (lo, hi) in enumerate(((cut, d_model), (0, cut))):
                span = pl.ds(lo, hi - lo)
                g_copies.append(pltpu.make_async_copy(refs['w_up'].at[g_layer, span, :], wbuf.at[span, :], refs['gw_sem'].at[i]))
        else:
            at = 0
            for i, name in enumerate(('w_q', 'w_k', 'w_v')):
                width = refs[name].shape[2]
                g_copies.append(pltpu.make_async_copy(refs[name].at[g_layer], wbuf.at[:, pl.ds(at, width)], refs['gw_sem'].at[i]))
                at += width

    def remote(src, dst, send, recv, peer):
        return pltpu.make_async_remote_copy(src_ref=src, dst_ref=dst, send_sem=send, recv_sem=recv, device_id={'tp': peer}, device_id_type=pl.DeviceIdType.MESH)

    if not scatter:
        x_copy.wait()
        for copy in g_copies:
            copy.start()
    pl.semaphore_wait(barrier, 2)

    if scatter:
        dsend, drecv, qsend, qrecv, own = refs['dsend'], refs['drecv'], refs['qsend'], refs['qrecv'], refs['own']
        part = refs['part']

        def d_copy(n, i):
            return remote(dsend.at[n, i], drecv.at[n, i], refs['ds_sem'].at[n, i], refs['dr_sem'].at[n, i], partner)

        def q_copy(n):
            return remote(qsend.at[n], qrecv.at[n], refs['qs_sem'].at[n], refs['qr_sem'].at[n], counter)

        for copy in a_copies:
            copy.wait()

        def s_step(n, carry):
            @pl.when(n + AHEAD < STEPS)
            def _():
                w_copy(n + AHEAD).start()

            w_copy(n).wait()
            far = jnp.dot(abuf[2:4].reshape(2 * rows, depth), wbuf[0:depth, col(n)], preferred_element_type=F32)
            dsend[n, 0] = far[rows:].astype(BF)
            d_copy(n, 0).start()
            part[...] = far[:rows]
            near = jnp.dot(abuf[0:2].reshape(2 * rows, depth), wbuf[0:depth, col(n)], preferred_element_type=F32)
            dsend[n, 1] = near[rows:].astype(BF)
            d_copy(n, 1).start()
            own[n] = near[:rows]
            d_copy(n, 0).wait_recv()
            qsend[n] = (part[...] + drecv[n, 0].astype(F32)).astype(BF)
            q_copy(n).start()
            return carry

        half = STEPS - AHEAD
        lax.fori_loop(0, half, s_step, 0)
        if gather:
            for copy in g_copies[:1] if cfg['kind'] == 'up' else g_copies:
                copy.start()
        lax.fori_loop(half, STEPS, s_step, 0)
        if gather and cfg['kind'] == 'up':
            g_copies[1].start()
        x_copy.wait()

    total = jnp.zeros((rows, 128), F32)
    for n in range(STEPS):
        cols = slice(n * blk, (n + 1) * blk)
        if scatter:
            d_copy(n, 1).wait_recv()
            q_copy(n).wait_recv()
            summed = own[n] + drecv[n, 1].astype(F32) + qrecv[n].astype(F32)
            fresh = (xbuf[:, cols].astype(F32) + summed.astype(BF).astype(F32)).astype(BF)
            xbuf[:, cols] = fresh
        else:
            fresh = xbuf[:, cols]
        fresh = fresh.astype(F32)
        for j in range(blk // 128):
            total = total + fresh[:, j * 128:(j + 1) * 128]
    if scatter:
        out_copy = pltpu.make_async_copy(xbuf, refs['x_out'], refs['x_sem'])
        out_copy.start()

    if gather:
        near_h, far_h, acc, stage, y_out = refs['near_h'], refs['far_h'], refs['acc'], refs['stage'], refs['y_out']
        n_out = acc.shape[1]
        mean = jnp.sum(total, axis=-1, keepdims=True) / d_model
        total = jnp.zeros((rows, 128), F32)
        for n in range(STEPS):
            diff = xbuf[:, n * blk:(n + 1) * blk].astype(F32) - mean
            diff = diff * diff
            for j in range(blk // 128):
                total = total + diff[:, j * 128:(j + 1) * 128]
        inv = lax.rsqrt(jnp.sum(total, axis=-1, keepdims=True) / d_model + LN_EPS)

        def c_copy(k):
            return remote(near_h.at[pl.ds(0, rows), col(k)], far_h.at[pl.ds(0, rows), col(k)], refs['cs_sem'].at[k], refs['cr_sem'].at[k], counter)

        def f_copy(k):
            return remote(far_h.at[pl.ds(0, rows), col(k)], far_h.at[pl.ds(rows, rows), col(k)], refs['fs_sem'].at[k], refs['fr_sem'].at[k], partner)

        def p_copy(k):
            return remote(near_h.at[pl.ds(0, rows), col(k)], near_h.at[pl.ds(rows, rows), col(k)], refs['ps_sem'].at[k], refs['pr_sem'].at[k], partner)

        for k in range(STEPS):
            cols = slice(k * blk, (k + 1) * blk)
            gain = refs['ln_gain'][ln_row // 2, ln_row % 2:ln_row % 2 + 1, cols].astype(F32)
            bias = refs['ln_bias'][ln_row // 2, ln_row % 2:ln_row % 2 + 1, cols].astype(F32)
            normed = (xbuf[:, cols].astype(F32) - mean) * inv
            near_h[0:rows, cols] = (normed * (1.0 + gain) + bias).astype(BF)
            if k:
                c_copy(k - 1).start()
                p_copy(k - 1).start()
        acc[...] = jnp.zeros(acc.shape, F32)
        c_copy(STEPS - 1).start()
        p_copy(STEPS - 1).start()

        for copy in g_copies:
            copy.wait()
        for k in range(STEPS):
            p_copy(k).wait_recv()

        def finish(value):
            if cfg['kind'] == 'up':
                value = jnp.square(jnp.maximum(value, 0.0)).astype(BF)
            return value.reshape(2, n_seq, toks, value.shape[-1])

        n_blk = n_out // STEPS

        def y_copy(g, n):
            return pltpu.make_async_copy(stage.at[g, :, :, col(n, n_blk)], y_out.at[:, order[g], :, col(n, n_blk)], refs['y_sem'].at[g, n])

        piece = min(1024, n_out)

        def far_dot(k, cols):
            return jnp.dot(far_h[:, col(k)], wbuf[col(k), cols], preferred_element_type=F32)

        def near_step(i):
            near = jnp.dot(near_h[...], wbuf[:, col(i, n_blk)], preferred_element_type=F32)
            stage[0:2, :, :, col(i, n_blk)] = finish(near)
            y_copy(0, i).start()
            y_copy(1, i).start()
            c_copy(i).wait_recv()
            f_copy(i).start()

        def g_step(i, carry):
            near_step(i)
            f_copy(i - 1).wait_recv()
            for n in range(n_out // piece):
                cols = slice(n * piece, (n + 1) * piece)
                acc[:, cols] += far_dot(i - 1, cols)
            return carry

        near_step(0)
        lax.fori_loop(1, STEPS, g_step, 0)
        f_copy(STEPS - 1).wait_recv()
        for n in range(n_out // piece):
            cols = slice(n * piece, (n + 1) * piece)
            stage[2:4, :, :, cols] = finish(acc[:, cols] + far_dot(STEPS - 1, cols))
            for m in range(n * piece // n_blk, (n + 1) * piece // n_blk):
                y_copy(2, m).start()
                y_copy(3, m).start()
        for k in range(STEPS):
            c_copy(k).wait_send()
            p_copy(k).wait_send()
            f_copy(k).wait_send()
            for g in range(4):
                y_copy(g, k).wait()

    if scatter:
        for n in range(STEPS):
            d_copy(n, 0).wait_send()
            d_copy(n, 1).wait_send()
            q_copy(n).wait_send()
        out_copy.wait()


def exchange(cid, x, ln_gain, ln_bias, *, n_seq, layer=0, a=None, w_s=None, g_layer=0, ln_row=0, kind=None, weights=()):
    rows, d_model = x.shape
    toks = rows // n_seq
    blk = d_model // STEPS
    scatter, gather = a is not None, kind is not None
    any_spec, vmem = pl.BlockSpec(memory_space=pl.ANY), pl.BlockSpec(memory_space=pltpu.VMEM)
    dma = pltpu.SemaphoreType.DMA
    ins, outs, scr = [('x_hbm', x, any_spec)], [], []
    flops, moved = 0, 4_000_000
    scr += [('wbuf', None), ('xbuf', pltpu.VMEM((rows, d_model), BF)), ('x_sem', dma)]
    width = 0
    if scatter:
        depth = a.shape[3]
        ins += [('a_hbm', a, any_spec), ('w_s', w_s, any_spec)]
        outs += [('x_out', jax.ShapeDtypeStruct(x.shape, BF))]
        scr += [
            ('abuf', pltpu.VMEM((4, n_seq, toks, depth), BF)), ('a_sem', dma((4,))), ('sw_sem', dma((STEPS,))),
            ('dsend', pltpu.VMEM((STEPS, 2, rows, blk), BF)), ('drecv', pltpu.VMEM((STEPS, 2, rows, blk), BF)),
            ('qsend', pltpu.VMEM((STEPS, rows, blk), BF)), ('qrecv', pltpu.VMEM((STEPS, rows, blk), BF)),
            ('own', pltpu.VMEM((STEPS, rows, blk), F32)), ('part', pltpu.VMEM((rows, blk), F32)),
            ('ds_sem', dma((STEPS, 2))), ('dr_sem', dma((STEPS, 2))), ('qs_sem', dma((STEPS,))), ('qr_sem', dma((STEPS,))),
        ]
        width = d_model
        w_rows = depth
        flops += 2 * 4 * rows * depth * d_model
        moved += depth * d_model * 2
    if gather:
        names = ('w_up',) if kind == 'up' else ('w_q', 'w_k', 'w_v')
        ins += list(zip(names, weights, [any_spec] * len(names)))
        ins += [('ln_gain', ln_gain, vmem), ('ln_bias', ln_bias, vmem)]
        n_out = sum(w.shape[2] for w in weights)
        y_type = BF if kind == 'up' else F32
        outs += [('y_out', jax.ShapeDtypeStruct((n_seq, 4, toks, n_out), y_type))]
        scr += [
            ('near_h', pltpu.VMEM((2 * rows, d_model), BF)), ('far_h', pltpu.VMEM((2 * rows, d_model), BF)),
            ('acc', pltpu.VMEM((2 * rows, n_out), F32)), ('stage', pltpu.VMEM((4, n_seq, toks, n_out), y_type)),
            ('gw_sem', dma((3,))), ('y_sem', dma((4, STEPS))),
        ] + [(s, dma((STEPS,))) for s in ('cs_sem', 'cr_sem', 'fs_sem', 'fr_sem', 'ps_sem', 'pr_sem')]
        width = max(width, n_out)
        w_rows = d_model
        flops += 2 * 4 * rows * n_out * d_model
        moved += n_out * d_model * 2
    scr[0] = ('wbuf', pltpu.VMEM((w_rows, width), BF))
    cfg = dict(
        names=[i[0] for i in ins] + [o[0] for o in outs] + [s[0] for s in scr], layer=layer, g_layer=g_layer, ln_row=ln_row,
        scatter=scatter, gather=gather, n_seq=n_seq, toks=toks, d_model=d_model, kind=kind, depth=depth if scatter else 0,
    )
    return pl.pallas_call(
        functools.partial(exchange_kernel, cfg),
        in_specs=[i[2] for i in ins],
        out_specs=[any_spec] * len(outs),
        out_shape=[o[1] for o in outs],
        scratch_shapes=[s[1] for s in scr],
        compiler_params=pltpu.CompilerParams(collective_id=cid, has_side_effects=True, vmem_limit_bytes=66_000_000),
        cost_estimate=pl.CostEstimate(flops=flops, bytes_accessed=moved, transcendentals=0),
        name=('scatter_' if scatter else '') + ('gather_' + kind if gather else 'end'),
    )(*[i[1] for i in ins])


def solution(mesh):
    tok_spec = P('dp', 'tp', None)
    cache_spec = P(None, 'dp', 'tp', None, None)
    col_spec = P(None, None, 'tp')
    row_spec = P(None, 'tp', None)

    def device_fn(x_loc, start_pos, k_cache, v_cache, w_q, w_k, w_v, w_o, w_up, w_down, ln_gain, ln_bias):
        n_layers = w_q.shape[0]
        n_seq, tok_loc, d_model = x_loc.shape
        new_len = tok_loc * 4
        rows = n_seq * new_len
        positions = (start_pos[:, None] + jnp.arange(new_len, dtype=jnp.int32)[None, :]).reshape(rows)
        tabs = rope_tables(positions, k_cache.shape[4])
        gain, bias = ln_gain, ln_bias
        hidden = x_loc.reshape(n_seq * tok_loc, d_model)
        prev = ()
        qkv, = exchange(0, hidden, gain, bias, n_seq=n_seq, kind='qkv', weights=(w_q, w_k, w_v))
        for layer in range(n_layers):
            context, *prev = attend(layer, qkv.reshape(rows, -1), tabs, start_pos, k_cache, v_cache, prev)
            context = context.reshape(n_seq, 4, tok_loc, -1)
            hidden, act = exchange(2 * layer + 1, hidden, gain, bias, n_seq=n_seq, layer=layer, a=context, w_s=w_o, g_layer=layer, ln_row=2 * layer + 1, kind='up', weights=(w_up,))
            if layer + 1 < n_layers:
                hidden, qkv = exchange(2 * layer + 2, hidden, gain, bias, n_seq=n_seq, layer=layer, a=act, w_s=w_down, g_layer=layer + 1, ln_row=2 * layer + 2, kind='qkv', weights=(w_q, w_k, w_v))
            else:
                hidden, = exchange(2 * layer + 2, hidden, gain, bias, n_seq=n_seq, layer=layer, a=act, w_s=w_down)
        return hidden.reshape(x_loc.shape), prev[0], prev[1]

    return jax.shard_map(device_fn, mesh=mesh, in_specs=(tok_spec, P('dp'), cache_spec, cache_spec, col_spec, col_spec, col_spec, row_spec, col_spec, row_spec, P(), P()), out_specs=(tok_spec, cache_spec, cache_spec), check_vma=False)
```

```python
import functools
import math

import jax
import jax.numpy as jnp
from jax import lax
from jax.experimental import pallas as pl
from jax.experimental.pallas import tpu as pltpu
from jax.sharding import PartitionSpec as P

LN_EPS = 1e-5
ROPE_BASE = 10000.0
NEG_BIG = -1e30
MIN_START = 768
BF = jnp.bfloat16
F32 = jnp.float32


def rope_tables(positions, head_dim):
    rot = head_dim // 2
    half = rot // 2
    lane = jnp.arange(head_dim, dtype=jnp.int32)
    freq = ROPE_BASE ** (-((lane % half).astype(F32) * (2.0 / rot)))
    angles = positions.astype(F32)[:, None] * freq
    cos_a, sin_a = jnp.cos(angles), jnp.sin(angles)
    c_tab = jnp.where(lane < rot, cos_a, 1.0)
    s_up = jnp.where((lane >= half) & (lane < rot), sin_a, 0.0)
    s_dn = jnp.where(lane < half, -sin_a, 0.0)
    return jnp.stack([c_tab, s_up, s_dn])


def attn_kernel(layer, dims, start_ref, q_ref, k_ref, v_ref, tab_ref, kc_hbm, vc_hbm, *rest):
    kv, group, toks, hd, s_len, ch, n_ch = dims
    if layer > 0:
        rest = rest[2:]
    ctx_ref, ko_hbm, vo_hbm, kbuf, vbuf, sbuf, ebuf, qbuf, mbuf, pbuf, lbuf, abuf, in_sem, out_sem = rest
    b = pl.program_id(0)
    nb = pl.num_programs(0)
    slot = lax.rem(b, 2)
    other = 1 - slot
    s_pad = kbuf.shape[2]
    win = toks + 16
    rows = group * toks
    coef = (hd ** -0.5) * math.log2(math.e)

    def load(bb, sl, go):
        for i, (src, dst) in enumerate(((kc_hbm, kbuf), (vc_hbm, vbuf))):
            copy = pltpu.make_async_copy(src.at[layer, bb], dst.at[sl, :, pl.ds(0, s_len), :], in_sem.at[sl, i])
            copy.start() if go else copy.wait()

    def save(bb, sl, go):
        for i, (src, dst) in enumerate(((kbuf, ko_hbm), (vbuf, vo_hbm))):
            copy = pltpu.make_async_copy(src.at[sl, :, pl.ds(0, s_len), :], dst.at[layer, bb], out_sem.at[sl, i])
            copy.start() if go else copy.wait()

    @pl.when(b == 0)
    def _():
        load(b, slot, True)
        if s_pad > s_len:
            for sl in range(2):
                kbuf[sl, :, s_len:, :] = jnp.zeros((kv, s_pad - s_len, hd), BF)
                vbuf[sl, :, s_len:, :] = jnp.zeros((kv, s_pad - s_len, hd), BF)

    @pl.when(b > 0)
    def _():
        save(b - 1, other, False)

    @pl.when(b + 1 < nb)
    def _():
        load(b + 1, other, True)

    c_tab, s_up, s_dn = tab_ref[0], tab_ref[1], tab_ref[2]
    half = hd // 4

    def rope(x):
        return x * c_tab + pltpu.roll(x, half, 1) * s_up + pltpu.roll(x, hd - half, 1) * s_dn

    for h in range(kv):
        for g in range(group):
            j = h * group + g
            qbuf[h, g * toks:(g + 1) * toks, :] = rope(q_ref[:, j * hd:(j + 1) * hd]).astype(BF)

    start = start_ref[b]
    base = jnp.minimum((start // 16) * 16, s_len - win)
    shift = start - base
    base = pl.multiple_of(base, 16)
    row_id = lax.broadcasted_iota(jnp.int32, (win, hd), 0)
    is_new = jnp.logical_and(row_id >= shift, row_id < shift + toks)

    load(b, slot, False)
    for h in range(kv):
        cols = slice(h * hd, (h + 1) * hd)
        for buf, fresh in ((kbuf, rope(k_ref[:, cols])), (vbuf, v_ref[:, cols])):
            fresh = fresh.astype(BF).astype(F32)
            fresh = jnp.concatenate([fresh, jnp.zeros((16, hd), F32)], axis=0)
            fresh = pltpu.roll(fresh, shift, 0)
            old = buf[slot, h, pl.ds(base, win), :].astype(F32)
            buf[slot, h, pl.ds(base, win), :] = jnp.where(is_new, fresh, old).astype(BF)
    save(b, slot, True)

    lbuf[...] = jnp.zeros(lbuf.shape, F32)
    abuf[...] = jnp.zeros(abuf.shape, F32)
    n_full = jnp.maximum(start // ch, 1)
    n_used = (start + toks + ch - 1) // ch
    step_rows = 64
    blocks = [slice(r, r + step_rows) for r in range(0, ch, step_rows)]
    ahead = lax.broadcasted_iota(jnp.int32, (step_rows, rows), 0) - lax.rem(lax.broadcasted_iota(jnp.int32, (step_rows, rows), 1), toks)

    def chunk(j):
        return pl.ds(pl.multiple_of(j * ch, ch), ch)

    def score(h, j):
        sbuf[h] = lax.dot_general(kbuf[slot, h, chunk(j), :], qbuf[h], (((1,), (1,)), ((), ())), preferred_element_type=F32)

    def scored(h, j, rb, masked):
        s = sbuf[h, rb]
        if masked:
            s = jnp.where(ahead <= start - j * ch - rb.start, s, NEG_BIG)
        return s.reshape(step_rows // 8, 8, rows)

    def peaks(h, j, masked):
        top = jnp.max(scored(h, j, blocks[0], masked), axis=0)
        for rb in blocks[1:]:
            top = jnp.maximum(top, jnp.max(scored(h, j, rb, masked), axis=0))
        peak = pbuf[h]
        mbuf[h] = peak
        pbuf[h] = jnp.maximum(peak, jnp.max(top, axis=0, keepdims=True))

    def weigh(h, j, masked):
        peak = pbuf[h]
        total = lbuf[h] * jnp.exp2((mbuf[h] - peak) * coef)
        for rb in blocks:
            e = jnp.exp2((scored(h, j, rb, masked) - peak) * coef)
            total = total + jnp.sum(e, axis=0)
            ebuf[h, rb] = e.reshape(step_rows, rows).astype(BF)
        lbuf[h] = total

    def mix(h, j, alpha):
        fresh = lax.dot_general(vbuf[slot, h, chunk(j), :], ebuf[h], (((0,), (0,)), ((), ())), preferred_element_type=F32)
        abuf[h] = (abuf[h].reshape(hd // 8, 8, rows) * alpha).reshape(hd, rows) + fresh

    def rescale(h):
        return jnp.exp2((mbuf[h] - pbuf[h]) * coef)

    def step(masked_now, masked_next, j, carry):
        for h in range(kv):
            alpha = rescale(h)
            weigh(h, j, masked_now)
            score(h, j + 1)
            mix(h, j, alpha)
        for h in range(kv):
            peaks(h, j + 1, masked_next)
        return carry

    pbuf[...] = jnp.full(pbuf.shape, NEG_BIG, F32)
    for h in range(kv):
        score(h, 0)
    for h in range(kv):
        peaks(h, 0, ch > MIN_START)
    last = n_used - 1
    lax.fori_loop(0, n_full - 1, functools.partial(step, ch > MIN_START, False), 0)
    lax.fori_loop(n_full - 1, last, functools.partial(step, True, True), 0)
    for h in range(kv):
        alpha = rescale(h)
        weigh(h, last, True)
        mix(h, last, alpha)
    for h in range(kv):
        ctx = (abuf[h] / jnp.sum(lbuf[h], axis=0, keepdims=True)).T.astype(BF)
        for g in range(group):
            j = h * group + g
            ctx_ref[:, j * hd:(j + 1) * hd] = ctx[g * toks:(g + 1) * toks, :]

    @pl.when(b == nb - 1)
    def _():
        save(b, slot, False)


def attend(layer, qkv, tabs, start_pos, k_cache, v_cache, prev):
    n_seq = start_pos.shape[0]
    _, _, kv, s_len, hd = k_cache.shape
    toks = qkv.shape[0] // n_seq
    kv_width = kv * hd
    q_width = qkv.shape[1] - 2 * kv_width
    group = q_width // kv_width
    n_ch = -(-s_len // 640)
    ch = 128 * -(-s_len // (128 * n_ch))
    rows = group * toks
    dims = (kv, group, toks, hd, s_len, ch, n_ch)
    any_spec = pl.BlockSpec(memory_space=pl.ANY)
    row_map = lambda b, *_: (b, 0)
    cache_shape = jax.ShapeDtypeStruct(k_cache.shape, BF)
    args = [start_pos, qkv, qkv, qkv, tabs, k_cache, v_cache] + list(prev)
    return pl.pallas_call(
        functools.partial(attn_kernel, layer, dims),
        grid_spec=pltpu.PrefetchScalarGridSpec(
            num_scalar_prefetch=1,
            grid=(n_seq,),
            in_specs=[
                pl.BlockSpec((toks, q_width), row_map),
                pl.BlockSpec((toks, kv_width), lambda b, *_: (b, group)),
                pl.BlockSpec((toks, kv_width), lambda b, *_: (b, group + 1)),
                pl.BlockSpec((3, toks, hd), lambda b, *_: (0, b, 0)),
            ] + [any_spec] * (2 + len(prev)),
            out_specs=[pl.BlockSpec((toks, q_width), row_map), any_spec, any_spec],
            scratch_shapes=[
                pltpu.VMEM((2, kv, ch * n_ch, hd), BF),
                pltpu.VMEM((2, kv, ch * n_ch, hd), BF),
                pltpu.VMEM((kv, ch, rows), F32),
                pltpu.VMEM((kv, ch, rows), BF),
                pltpu.VMEM((kv, rows, hd), BF),
                pltpu.VMEM((kv, 8, rows), F32),
                pltpu.VMEM((kv, 8, rows), F32),
                pltpu.VMEM((kv, 8, rows), F32),
                pltpu.VMEM((kv, hd, rows), F32),
                pltpu.SemaphoreType.DMA((2, 2)),
                pltpu.SemaphoreType.DMA((2, 2)),
            ],
        ),
        out_shape=[jax.ShapeDtypeStruct((n_seq * toks, q_width), BF), cache_shape, cache_shape],
        input_output_aliases={7: 1, 8: 2} if prev else {},
        compiler_params=pltpu.CompilerParams(vmem_limit_bytes=60 * 1024 * 1024, dimension_semantics=("arbitrary",)),
        cost_estimate=pl.CostEstimate(flops=8_000_000_000, bytes_accessed=80_000_000, transcendentals=15_000_000),
        name="attend",
    )(*args)


STEPS = 8
AHEAD = 3
EARLY = 2


def exchange_kernel(cfg, *args):
    refs = dict(zip(cfg['names'], args))
    layer, g_layer, ln_row = cfg['layer'], cfg['g_layer'], cfg['ln_row']
    scatter, gather = cfg['scatter'], cfg['gather']
    n_seq, toks, d_model = cfg['n_seq'], cfg['toks'], cfg['d_model']
    rows = n_seq * toks
    blk = d_model // STEPS
    me = lax.axis_index('tp')
    core = lax.rem(me, 2)
    partner = me + 1 - 2 * core
    counter = lax.rem(me + 2, 4)
    diag = lax.rem(partner + 2, 4)
    order = (me, partner, counter, diag)
    wbuf, xbuf = refs['wbuf'], refs['xbuf']

    barrier = pltpu.get_barrier_semaphore()
    for peer in (partner, counter):
        pl.semaphore_signal(barrier, inc=1, device_id={'tp': peer}, device_id_type=pl.DeviceIdType.MESH)

    def col(n, width=blk):
        return pl.ds(pl.multiple_of(n * width, width), width)

    x_copy = pltpu.make_async_copy(refs['x_hbm'], xbuf, refs['x_sem'])

    if scatter:
        depth = cfg['depth']
        abuf, w_s = refs['abuf'], refs['w_s']
        a_copies = [pltpu.make_async_copy(refs['a_hbm'].at[:, order[g]], abuf.at[g], refs['a_sem'].at[g]) for g in range(4)]

        def w_copy(n):
            return pltpu.make_async_copy(w_s.at[layer, :, col(n)], wbuf.at[pl.ds(0, depth), col(n)], refs['sw_sem'].at[n])

        for g in (2, 3):
            a_copies[g].start()
        w_copy(0).start()
        for g in (0, 1):
            a_copies[g].start()
        for n in range(1, AHEAD):
            w_copy(n).start()
    x_copy.start()

    g_copies = []
    if gather:
        if cfg['kind'] == 'up':
            cut = depth
            for i, (lo, hi) in enumerate(((cut, d_model), (0, cut))):
                span = pl.ds(lo, hi - lo)
                g_copies.append(pltpu.make_async_copy(refs['w_up'].at[g_layer, span, :], wbuf.at[span, :], refs['gw_sem'].at[i]))
        else:
            at = 0
            for i, name in enumerate(('w_q', 'w_k', 'w_v')):
                width = refs[name].shape[2]
                g_copies.append(pltpu.make_async_copy(refs[name].at[g_layer], wbuf.at[:, pl.ds(at, width)], refs['gw_sem'].at[i]))
                at += width

    def remote(src, dst, send, recv, peer):
        return pltpu.make_async_remote_copy(src_ref=src, dst_ref=dst, send_sem=send, recv_sem=recv, device_id={'tp': peer}, device_id_type=pl.DeviceIdType.MESH)

    if not scatter:
        x_copy.wait()
        for copy in g_copies:
            copy.start()
    pl.semaphore_wait(barrier, 2)

    if scatter:
        dsend, drecv, qsend, qrecv, own = refs['dsend'], refs['drecv'], refs['qsend'], refs['qrecv'], refs['own']
        part = refs['part']

        def d_copy(n, i):
            return remote(dsend.at[n, i], drecv.at[n, i], refs['ds_sem'].at[n, i], refs['dr_sem'].at[n, i], partner)

        def q_copy(n):
            return remote(qsend.at[n], qrecv.at[n], refs['qs_sem'].at[n], refs['qr_sem'].at[n], counter)

        for copy in a_copies:
            copy.wait()

        def s_step(n, carry):
            @pl.when(n + AHEAD < STEPS)
            def _():
                w_copy(n + AHEAD).start()

            w_copy(n).wait()
            far = jnp.dot(abuf[2:4].reshape(2 * rows, depth), wbuf[0:depth, col(n)], preferred_element_type=F32)
            dsend[n, 0] = far[rows:].astype(BF)
            d_copy(n, 0).start()
            part[...] = far[:rows]
            near = jnp.dot(abuf[0:2].reshape(2 * rows, depth), wbuf[0:depth, col(n)], preferred_element_type=F32)
            dsend[n, 1] = near[rows:].astype(BF)
            d_copy(n, 1).start()
            own[n] = near[:rows]
            d_copy(n, 0).wait_recv()
            qsend[n] = (part[...] + drecv[n, 0].astype(F32)).astype(BF)
            q_copy(n).start()
            return carry

        half = STEPS - AHEAD
        lax.fori_loop(0, half, s_step, 0)
        if gather:
            for copy in g_copies[:1] if cfg['kind'] == 'up' else g_copies:
                copy.start()
        lax.fori_loop(half, STEPS, s_step, 0)
        if gather and cfg['kind'] == 'up':
            g_copies[1].start()
        x_copy.wait()

    if gather:
        near_h, far_x, far_h, acc, stage, y_out = (refs[k] for k in ('near_h', 'far_x', 'far_h', 'acc', 'stage', 'y_out'))
        stat, far_stat = refs['stat'], refs['far_stat']
        n_out = acc.shape[1]

        def c_copy(k):
            return remote(xbuf.at[:, col(k)], far_x.at[pl.ds(0, rows), col(k)], refs['cs_sem'].at[k], refs['cr_sem'].at[k], counter)

        def f_copy(k):
            return remote(far_x.at[pl.ds(0, rows), col(k)], far_x.at[pl.ds(rows, rows), col(k)], refs['fs_sem'].at[k], refs['fr_sem'].at[k], partner)

        def p_copy(k):
            return remote(near_h.at[pl.ds(0, rows), col(k)], near_h.at[pl.ds(rows, rows), col(k)], refs['ps_sem'].at[k], refs['pr_sem'].at[k], partner)

        stat_copy = remote(stat, far_stat.at[0], refs['ts_sem'].at[0], refs['tr_sem'].at[0], counter)
        stat_pass = remote(far_stat.at[0], far_stat.at[1], refs['ts_sem'].at[1], refs['tr_sem'].at[1], partner)

    total = jnp.zeros((rows, 128), F32)
    for n in range(STEPS):
        cols = slice(n * blk, (n + 1) * blk)
        if scatter:
            d_copy(n, 1).wait_recv()
            q_copy(n).wait_recv()
            summed = own[n] + drecv[n, 1].astype(F32) + qrecv[n].astype(F32)
            fresh = (xbuf[:, cols].astype(F32) + summed.astype(BF).astype(F32)).astype(BF)
            xbuf[:, cols] = fresh
        else:
            fresh = xbuf[:, cols]
        if gather and 1 <= n <= EARLY:
            c_copy(n - 1).start()
        fresh = fresh.astype(F32)
        for j in range(blk // 128):
            total = total + fresh[:, j * 128:(j + 1) * 128]
    if scatter:
        out_copy = pltpu.make_async_copy(xbuf, refs['x_out'], refs['x_sem'])
        out_copy.start()

    if gather:
        mean = jnp.sum(total, axis=-1, keepdims=True) / d_model
        total = jnp.zeros((rows, 128), F32)
        for n in range(STEPS):
            diff = xbuf[:, n * blk:(n + 1) * blk].astype(F32) - mean
            diff = diff * diff
            for j in range(blk // 128):
                total = total + diff[:, j * 128:(j + 1) * 128]
        inv = lax.rsqrt(jnp.sum(total, axis=-1, keepdims=True) / d_model + LN_EPS)
        stat[...] = jnp.where(lax.broadcasted_iota(jnp.int32, (rows, 128), 1) < 64, mean, inv)

        def norm(values, mean, inv, cols):
            gain = refs['ln_gain'][ln_row // 2, ln_row % 2:ln_row % 2 + 1, cols].astype(F32)
            bias = refs['ln_bias'][ln_row // 2, ln_row % 2:ln_row % 2 + 1, cols].astype(F32)
            return ((values.astype(F32) - mean) * inv * (1.0 + gain) + bias).astype(BF)

        for k in range(STEPS):
            cols = slice(k * blk, (k + 1) * blk)
            near_h[0:rows, cols] = norm(xbuf[:, cols], mean, inv, cols)
            if k == 0:
                stat_copy.start()
                for n in range(EARLY, STEPS):
                    c_copy(n).start()
            else:
                p_copy(k - 1).start()
        acc[...] = jnp.zeros(acc.shape, F32)
        p_copy(STEPS - 1).start()

        for copy in g_copies:
            copy.wait()
        for k in range(STEPS):
            p_copy(k).wait_recv()

        def finish(value):
            if cfg['kind'] == 'up':
                value = jnp.square(jnp.maximum(value, 0.0)).astype(BF)
            return value.reshape(2, n_seq, toks, value.shape[-1])

        n_blk = n_out // STEPS

        def y_copy(g, n):
            return pltpu.make_async_copy(stage.at[g, :, :, col(n, n_blk)], y_out.at[:, order[g], :, col(n, n_blk)], refs['y_sem'].at[g, n])

        piece = min(1024, n_out)

        def far_norm(k):
            f_copy(k).wait_recv()
            for r in range(2):
                part_rows = slice(r * rows, (r + 1) * rows)
                far_h[part_rows] = norm(far_x[part_rows, col(k)], far_stat[r, :, 0:1], far_stat[r, :, 64:65], col(k))

        def far_dot(k, cols):
            return jnp.dot(far_h[...], wbuf[col(k), cols], preferred_element_type=F32)

        def near_step(i):
            near = jnp.dot(near_h[...], wbuf[:, col(i, n_blk)], preferred_element_type=F32)
            stage[0:2, :, :, col(i, n_blk)] = finish(near)
            y_copy(0, i).start()
            y_copy(1, i).start()
            c_copy(i).wait_recv()
            f_copy(i).start()

        def g_step(i, carry):
            near_step(i)
            far_norm(i - 1)
            for n in range(n_out // piece):
                cols = slice(n * piece, (n + 1) * piece)
                acc[:, cols] += far_dot(i - 1, cols)
            return carry

        near_step(0)
        stat_copy.wait_recv()
        stat_pass.start()
        stat_pass.wait_recv()
        lax.fori_loop(1, STEPS, g_step, 0)
        far_norm(STEPS - 1)
        for n in range(n_out // piece):
            cols = slice(n * piece, (n + 1) * piece)
            stage[2:4, :, :, cols] = finish(acc[:, cols] + far_dot(STEPS - 1, cols))
            for m in range(n * piece // n_blk, (n + 1) * piece // n_blk):
                y_copy(2, m).start()
                y_copy(3, m).start()
        stat_copy.wait_send()
        stat_pass.wait_send()
        for k in range(STEPS):
            c_copy(k).wait_send()
            p_copy(k).wait_send()
            f_copy(k).wait_send()
            for g in range(4):
                y_copy(g, k).wait()

    if scatter:
        for n in range(STEPS):
            d_copy(n, 0).wait_send()
            d_copy(n, 1).wait_send()
            q_copy(n).wait_send()
        out_copy.wait()


def exchange(cid, x, ln_gain, ln_bias, *, n_seq, layer=0, a=None, w_s=None, g_layer=0, ln_row=0, kind=None, weights=()):
    rows, d_model = x.shape
    toks = rows // n_seq
    blk = d_model // STEPS
    scatter, gather = a is not None, kind is not None
    any_spec, vmem = pl.BlockSpec(memory_space=pl.ANY), pl.BlockSpec(memory_space=pltpu.VMEM)
    dma = pltpu.SemaphoreType.DMA
    ins, outs, scr = [('x_hbm', x, any_spec)], [], []
    flops, moved = 0, 4_000_000
    scr += [('wbuf', None), ('xbuf', pltpu.VMEM((rows, d_model), BF)), ('x_sem', dma)]
    width = 0
    if scatter:
        depth = a.shape[3]
        ins += [('a_hbm', a, any_spec), ('w_s', w_s, any_spec)]
        outs += [('x_out', jax.ShapeDtypeStruct(x.shape, BF))]
        scr += [
            ('abuf', pltpu.VMEM((4, n_seq, toks, depth), BF)), ('a_sem', dma((4,))), ('sw_sem', dma((STEPS,))),
            ('dsend', pltpu.VMEM((STEPS, 2, rows, blk), BF)), ('drecv', pltpu.VMEM((STEPS, 2, rows, blk), BF)),
            ('qsend', pltpu.VMEM((STEPS, rows, blk), BF)), ('qrecv', pltpu.VMEM((STEPS, rows, blk), BF)),
            ('own', pltpu.VMEM((STEPS, rows, blk), F32)), ('part', pltpu.VMEM((rows, blk), F32)),
            ('ds_sem', dma((STEPS, 2))), ('dr_sem', dma((STEPS, 2))), ('qs_sem', dma((STEPS,))), ('qr_sem', dma((STEPS,))),
        ]
        width = d_model
        w_rows = depth
        flops += 2 * 4 * rows * depth * d_model
        moved += depth * d_model * 2
    if gather:
        names = ('w_up',) if kind == 'up' else ('w_q', 'w_k', 'w_v')
        ins += list(zip(names, weights, [any_spec] * len(names)))
        ins += [('ln_gain', ln_gain, vmem), ('ln_bias', ln_bias, vmem)]
        n_out = sum(w.shape[2] for w in weights)
        y_type = BF if kind == 'up' else F32
        outs += [('y_out', jax.ShapeDtypeStruct((n_seq, 4, toks, n_out), y_type))]
        scr += [
            ('near_h', pltpu.VMEM((2 * rows, d_model), BF)), ('far_x', pltpu.VMEM((2 * rows, d_model), BF)),
            ('far_h', pltpu.VMEM((2 * rows, blk), BF)), ('stat', pltpu.VMEM((rows, 128), F32)), ('far_stat', pltpu.VMEM((2, rows, 128), F32)),
            ('ts_sem', dma((2,))), ('tr_sem', dma((2,))),
            ('acc', pltpu.VMEM((2 * rows, n_out), F32)), ('stage', pltpu.VMEM((4, n_seq, toks, n_out), y_type)),
            ('gw_sem', dma((3,))), ('y_sem', dma((4, STEPS))),
        ] + [(s, dma((STEPS,))) for s in ('cs_sem', 'cr_sem', 'fs_sem', 'fr_sem', 'ps_sem', 'pr_sem')]
        width = max(width, n_out)
        w_rows = d_model
        flops += 2 * 4 * rows * n_out * d_model
        moved += n_out * d_model * 2
    scr[0] = ('wbuf', pltpu.VMEM((w_rows, width), BF))
    cfg = dict(
        names=[i[0] for i in ins] + [o[0] for o in outs] + [s[0] for s in scr], layer=layer, g_layer=g_layer, ln_row=ln_row,
        scatter=scatter, gather=gather, n_seq=n_seq, toks=toks, d_model=d_model, kind=kind, depth=depth if scatter else 0,
    )
    return pl.pallas_call(
        functools.partial(exchange_kernel, cfg),
        in_specs=[i[2] for i in ins],
        out_specs=[any_spec] * len(outs),
        out_shape=[o[1] for o in outs],
        scratch_shapes=[s[1] for s in scr],
        compiler_params=pltpu.CompilerParams(collective_id=cid, has_side_effects=True, vmem_limit_bytes=66_000_000),
        cost_estimate=pl.CostEstimate(flops=flops, bytes_accessed=moved, transcendentals=0),
        name=('scatter_' if scatter else '') + ('gather_' + kind if gather else 'end'),
    )(*[i[1] for i in ins])


def solution(mesh):
    tok_spec = P('dp', 'tp', None)
    cache_spec = P(None, 'dp', 'tp', None, None)
    col_spec = P(None, None, 'tp')
    row_spec = P(None, 'tp', None)

    def device_fn(x_loc, start_pos, k_cache, v_cache, w_q, w_k, w_v, w_o, w_up, w_down, ln_gain, ln_bias):
        n_layers = w_q.shape[0]
        n_seq, tok_loc, d_model = x_loc.shape
        new_len = tok_loc * 4
        rows = n_seq * new_len
        positions = (start_pos[:, None] + jnp.arange(new_len, dtype=jnp.int32)[None, :]).reshape(rows)
        tabs = rope_tables(positions, k_cache.shape[4])
        gain, bias = ln_gain, ln_bias
        hidden = x_loc.reshape(n_seq * tok_loc, d_model)
        prev = ()
        qkv, = exchange(0, hidden, gain, bias, n_seq=n_seq, kind='qkv', weights=(w_q, w_k, w_v))
        for layer in range(n_layers):
            context, *prev = attend(layer, qkv.reshape(rows, -1), tabs, start_pos, k_cache, v_cache, prev)
            context = context.reshape(n_seq, 4, tok_loc, -1)
            hidden, act = exchange(2 * layer + 1, hidden, gain, bias, n_seq=n_seq, layer=layer, a=context, w_s=w_o, g_layer=layer, ln_row=2 * layer + 1, kind='up', weights=(w_up,))
            if layer + 1 < n_layers:
                hidden, qkv = exchange(2 * layer + 2, hidden, gain, bias, n_seq=n_seq, layer=layer, a=act, w_s=w_down, g_layer=layer + 1, ln_row=2 * layer + 2, kind='qkv', weights=(w_q, w_k, w_v))
            else:
                hidden, = exchange(2 * layer + 2, hidden, gain, bias, n_seq=n_seq, layer=layer, a=act, w_s=w_down)
        return hidden.reshape(x_loc.shape), prev[0], prev[1]

    return jax.shard_map(device_fn, mesh=mesh, in_specs=(tok_spec, P('dp'), cache_spec, cache_spec, col_spec, col_spec, col_spec, row_spec, col_spec, row_spec, P(), P()), out_specs=(tok_spec, cache_spec, cache_spec), check_vma=False)
```

```python
import functools
import math

import jax
import jax.numpy as jnp
from jax import lax
from jax.experimental import pallas as pl
from jax.experimental.pallas import tpu as pltpu
from jax.sharding import PartitionSpec as P

LN_EPS = 1e-5
ROPE_BASE = 10000.0
NEG_BIG = -1e30
MIN_START = 768
BF = jnp.bfloat16
F32 = jnp.float32


def rope_tables(positions, head_dim):
    rot = head_dim // 2
    half = rot // 2
    lane = jnp.arange(head_dim, dtype=jnp.int32)
    freq = ROPE_BASE ** (-((lane % half).astype(F32) * (2.0 / rot)))
    angles = positions.astype(F32)[:, None] * freq
    cos_a, sin_a = jnp.cos(angles), jnp.sin(angles)
    c_tab = jnp.where(lane < rot, cos_a, 1.0)
    s_up = jnp.where((lane >= half) & (lane < rot), sin_a, 0.0)
    s_dn = jnp.where(lane < half, -sin_a, 0.0)
    return jnp.stack([c_tab, s_up, s_dn])


def attn_kernel(layer, dims, start_ref, q_ref, k_ref, v_ref, tab_ref, kc_hbm, vc_hbm, *rest):
    kv, group, toks, hd, s_len, ch, n_ch = dims
    if layer > 0:
        rest = rest[2:]
    ctx_ref, ko_hbm, vo_hbm, kbuf, vbuf, sbuf, ebuf, qbuf, mbuf, pbuf, lbuf, abuf, in_sem, out_sem = rest
    b = pl.program_id(0)
    nb = pl.num_programs(0)
    slot = lax.rem(b, 2)
    other = 1 - slot
    s_pad = kbuf.shape[2]
    win = toks + 16
    rows = group * toks
    coef = (hd ** -0.5) * math.log2(math.e)

    def load(bb, sl, go):
        for i, (src, dst) in enumerate(((kc_hbm, kbuf), (vc_hbm, vbuf))):
            copy = pltpu.make_async_copy(src.at[layer, bb], dst.at[sl, :, pl.ds(0, s_len), :], in_sem.at[sl, i])
            copy.start() if go else copy.wait()

    def save(bb, sl, go):
        for i, (src, dst) in enumerate(((kbuf, ko_hbm), (vbuf, vo_hbm))):
            copy = pltpu.make_async_copy(src.at[sl, :, pl.ds(0, s_len), :], dst.at[layer, bb], out_sem.at[sl, i])
            copy.start() if go else copy.wait()

    @pl.when(b == 0)
    def _():
        load(b, slot, True)
        if s_pad > s_len:
            for sl in range(2):
                kbuf[sl, :, s_len:, :] = jnp.zeros((kv, s_pad - s_len, hd), BF)
                vbuf[sl, :, s_len:, :] = jnp.zeros((kv, s_pad - s_len, hd), BF)

    @pl.when(b > 0)
    def _():
        save(b - 1, other, False)

    @pl.when(b + 1 < nb)
    def _():
        load(b + 1, other, True)

    c_tab, s_up, s_dn = tab_ref[0], tab_ref[1], tab_ref[2]
    half = hd // 4

    def rope(x):
        return x * c_tab + pltpu.roll(x, half, 1) * s_up + pltpu.roll(x, hd - half, 1) * s_dn

    for h in range(kv):
        for g in range(group):
            j = h * group + g
            qbuf[h, g * toks:(g + 1) * toks, :] = rope(q_ref[:, j * hd:(j + 1) * hd]).astype(BF)

    start = start_ref[b]
    base = jnp.minimum((start // 16) * 16, s_len - win)
    shift = start - base
    base = pl.multiple_of(base, 16)
    row_id = lax.broadcasted_iota(jnp.int32, (win, hd), 0)
    is_new = jnp.logical_and(row_id >= shift, row_id < shift + toks)

    load(b, slot, False)
    for h in range(kv):
        cols = slice(h * hd, (h + 1) * hd)
        for buf, fresh in ((kbuf, rope(k_ref[:, cols])), (vbuf, v_ref[:, cols])):
            fresh = fresh.astype(BF).astype(F32)
            fresh = jnp.concatenate([fresh, jnp.zeros((16, hd), F32)], axis=0)
            fresh = pltpu.roll(fresh, shift, 0)
            old = buf[slot, h, pl.ds(base, win), :].astype(F32)
            buf[slot, h, pl.ds(base, win), :] = jnp.where(is_new, fresh, old).astype(BF)
    save(b, slot, True)

    lbuf[...] = jnp.zeros(lbuf.shape, F32)
    abuf[...] = jnp.zeros(abuf.shape, F32)
    n_full = jnp.maximum(start // ch, 1)
    n_used = (start + toks + ch - 1) // ch
    step_rows = 64
    blocks = [slice(r, r + step_rows) for r in range(0, ch, step_rows)]
    ahead = lax.broadcasted_iota(jnp.int32, (step_rows, rows), 0) - lax.rem(lax.broadcasted_iota(jnp.int32, (step_rows, rows), 1), toks)

    def chunk(j):
        return pl.ds(pl.multiple_of(j * ch, ch), ch)

    def score(h, j):
        sbuf[h] = lax.dot_general(kbuf[slot, h, chunk(j), :], qbuf[h], (((1,), (1,)), ((), ())), preferred_element_type=F32)

    def scored(h, j, rb, masked):
        s = sbuf[h, rb]
        if masked:
            s = jnp.where(ahead <= start - j * ch - rb.start, s, NEG_BIG)
        return s.reshape(step_rows // 8, 8, rows)

    def peaks(h, j, masked):
        top = jnp.max(scored(h, j, blocks[0], masked), axis=0)
        for rb in blocks[1:]:
            top = jnp.maximum(top, jnp.max(scored(h, j, rb, masked), axis=0))
        peak = pbuf[h]
        mbuf[h] = peak
        pbuf[h] = jnp.maximum(peak, jnp.max(top, axis=0, keepdims=True))

    def weigh(h, j, masked):
        peak = pbuf[h]
        total = lbuf[h] * jnp.exp2((mbuf[h] - peak) * coef)
        for rb in blocks:
            e = jnp.exp2((scored(h, j, rb, masked) - peak) * coef)
            total = total + jnp.sum(e, axis=0)
            ebuf[h, rb] = e.reshape(step_rows, rows).astype(BF)
        lbuf[h] = total

    def mix(h, j, alpha):
        fresh = lax.dot_general(vbuf[slot, h, chunk(j), :], ebuf[h], (((0,), (0,)), ((), ())), preferred_element_type=F32)
        abuf[h] = (abuf[h].reshape(hd // 8, 8, rows) * alpha).reshape(hd, rows) + fresh

    def rescale(h):
        return jnp.exp2((mbuf[h] - pbuf[h]) * coef)

    def step(masked_now, masked_next, j, carry):
        for h in range(kv):
            alpha = rescale(h)
            weigh(h, j, masked_now)
            score(h, j + 1)
            mix(h, j, alpha)
        for h in range(kv):
            peaks(h, j + 1, masked_next)
        return carry

    pbuf[...] = jnp.full(pbuf.shape, NEG_BIG, F32)
    for h in range(kv):
        score(h, 0)
    for h in range(kv):
        peaks(h, 0, ch > MIN_START)
    last = n_used - 1
    lax.fori_loop(0, n_full - 1, functools.partial(step, ch > MIN_START, False), 0)
    lax.fori_loop(n_full - 1, last, functools.partial(step, True, True), 0)
    for h in range(kv):
        alpha = rescale(h)
        weigh(h, last, True)
        mix(h, last, alpha)
    for h in range(kv):
        ctx = (abuf[h] / jnp.sum(lbuf[h], axis=0, keepdims=True)).T.astype(BF)
        for g in range(group):
            j = h * group + g
            ctx_ref[:, j * hd:(j + 1) * hd] = ctx[g * toks:(g + 1) * toks, :]

    @pl.when(b == nb - 1)
    def _():
        save(b, slot, False)


def attend(layer, qkv, tabs, start_pos, k_cache, v_cache, prev):
    n_seq = start_pos.shape[0]
    _, _, kv, s_len, hd = k_cache.shape
    toks = qkv.shape[0] // n_seq
    kv_width = kv * hd
    q_width = qkv.shape[1] - 2 * kv_width
    group = q_width // kv_width
    n_ch = -(-s_len // 640)
    ch = 128 * -(-s_len // (128 * n_ch))
    rows = group * toks
    dims = (kv, group, toks, hd, s_len, ch, n_ch)
    any_spec = pl.BlockSpec(memory_space=pl.ANY)
    row_map = lambda b, *_: (b, 0)
    cache_shape = jax.ShapeDtypeStruct(k_cache.shape, BF)
    args = [start_pos, qkv, qkv, qkv, tabs, k_cache, v_cache] + list(prev)
    return pl.pallas_call(
        functools.partial(attn_kernel, layer, dims),
        grid_spec=pltpu.PrefetchScalarGridSpec(
            num_scalar_prefetch=1,
            grid=(n_seq,),
            in_specs=[
                pl.BlockSpec((toks, q_width), row_map),
                pl.BlockSpec((toks, kv_width), lambda b, *_: (b, group)),
                pl.BlockSpec((toks, kv_width), lambda b, *_: (b, group + 1)),
                pl.BlockSpec((3, toks, hd), lambda b, *_: (0, b, 0)),
            ] + [any_spec] * (2 + len(prev)),
            out_specs=[pl.BlockSpec((toks, q_width), row_map), any_spec, any_spec],
            scratch_shapes=[
                pltpu.VMEM((2, kv, ch * n_ch, hd), BF),
                pltpu.VMEM((2, kv, ch * n_ch, hd), BF),
                pltpu.VMEM((kv, ch, rows), F32),
                pltpu.VMEM((kv, ch, rows), BF),
                pltpu.VMEM((kv, rows, hd), BF),
                pltpu.VMEM((kv, 8, rows), F32),
                pltpu.VMEM((kv, 8, rows), F32),
                pltpu.VMEM((kv, 8, rows), F32),
                pltpu.VMEM((kv, hd, rows), F32),
                pltpu.SemaphoreType.DMA((2, 2)),
                pltpu.SemaphoreType.DMA((2, 2)),
            ],
        ),
        out_shape=[jax.ShapeDtypeStruct((n_seq * toks, q_width), BF), cache_shape, cache_shape],
        input_output_aliases={7: 1, 8: 2} if prev else {},
        compiler_params=pltpu.CompilerParams(vmem_limit_bytes=60 * 1024 * 1024, dimension_semantics=("arbitrary",)),
        cost_estimate=pl.CostEstimate(flops=8_000_000_000, bytes_accessed=80_000_000, transcendentals=15_000_000),
        name="attend",
    )(*args)


STEPS = 8
WIDE = STEPS + 2


def exchange_kernel(cfg, *args):
    refs = dict(zip(cfg['names'], args))
    n_seq, toks, d_model = cfg['n_seq'], cfg['toks'], cfg['d_model']
    rows = n_seq * toks
    blk = d_model // STEPS
    me = lax.axis_index('tp')
    core = lax.rem(me, 2)
    partner = me + 1 - 2 * core
    counter = lax.rem(me + 2, 4)
    diag = lax.rem(partner + 2, 4)
    order = (me, partner, counter, diag)
    wbuf, xbuf = refs['wbuf'], refs['xbuf']

    barrier = pltpu.get_barrier_semaphore()
    for peer in (partner, counter):
        pl.semaphore_signal(barrier, inc=1, device_id={'tp': peer}, device_id_type=pl.DeviceIdType.MESH)

    def col(n, width=blk):
        return pl.ds(pl.multiple_of(n * width, width), width)

    def remote(src, dst, send, recv, peer):
        return pltpu.make_async_remote_copy(src_ref=src, dst_ref=dst, send_sem=send, recv_sem=recv, device_id={'tp': peer}, device_id_type=pl.DeviceIdType.MESH)

    def fold(values, total):
        for j in range(blk // 128):
            total = total + values[:, j * 128:(j + 1) * 128]
        return total

    def scatter(tag, a_ref, w_copy, slot_of, depth, ahead, late):
        dsend, drecv, qsend, qrecv, own, part = (refs[k] for k in ('dsend', 'drecv', 'qsend', 'qrecv', 'own', 'part'))
        ds_sem, dr_sem, qs_sem, qr_sem = (refs[tag + k] for k in ('ds', 'dr', 'qs', 'qr'))

        def d_copy(n, i):
            return remote(dsend.at[n, i], drecv.at[n, i], ds_sem.at[n, i], dr_sem.at[n, i], partner)

        def q_copy(n):
            return remote(qsend.at[n], qrecv.at[n], qs_sem.at[n], qr_sem.at[n], counter)

        def step(n, carry):
            @pl.when(n + ahead < STEPS)
            def _():
                w_copy(n + ahead).start()

            w_copy(n).wait()
            cols = col(slot_of(n))
            far = jnp.dot(a_ref[2:4].reshape(2 * rows, depth), wbuf[0:depth, cols], preferred_element_type=F32)
            dsend[n, 0] = far[rows:].astype(BF)
            d_copy(n, 0).start()
            part[...] = far[:rows]
            near = jnp.dot(a_ref[0:2].reshape(2 * rows, depth), wbuf[0:depth, cols], preferred_element_type=F32)
            dsend[n, 1] = near[rows:].astype(BF)
            d_copy(n, 1).start()
            own[n] = near[:rows]
            d_copy(n, 0).wait_recv()
            qsend[n] = (part[...] + drecv[n, 0].astype(F32)).astype(BF)
            q_copy(n).start()
            return carry

        half = STEPS - 3
        lax.fori_loop(0, half, step, 0)
        late(0)
        lax.fori_loop(half, STEPS, step, 0)
        late(1)
        total = jnp.zeros((rows, 128), F32)
        for n in range(STEPS):
            cols = slice(n * blk, (n + 1) * blk)
            d_copy(n, 1).wait_recv()
            q_copy(n).wait_recv()
            summed = own[n] + drecv[n, 1].astype(F32) + qrecv[n].astype(F32)
            fresh = (xbuf[:, cols].astype(F32) + summed.astype(BF).astype(F32)).astype(BF)
            xbuf[:, cols] = fresh
            total = fold(fresh.astype(F32), total)
        for n in range(STEPS):
            d_copy(n, 0).wait_send()
            d_copy(n, 1).wait_send()
            q_copy(n).wait_send()
        return total

    def gather(tag, ln_row, total, w_at, n_out, ready, finish):
        near_h, far_h, acc = refs['near_h'], refs['far_h'], refs['acc']
        cs, cr, fs, fr, ps, pr = (refs[tag + k] for k in ('cs', 'cr', 'fs', 'fr', 'ps', 'pr'))
        mean = jnp.sum(total, axis=-1, keepdims=True) / d_model
        total = jnp.zeros((rows, 128), F32)
        for n in range(STEPS):
            diff = xbuf[:, n * blk:(n + 1) * blk].astype(F32) - mean
            total = fold(diff * diff, total)
        inv = lax.rsqrt(jnp.sum(total, axis=-1, keepdims=True) / d_model + LN_EPS)

        def c_copy(k):
            return remote(near_h.at[pl.ds(0, rows), col(k)], far_h.at[pl.ds(0, rows), col(k)], cs.at[k], cr.at[k], counter)

        def f_copy(k):
            return remote(far_h.at[pl.ds(0, rows), col(k)], far_h.at[pl.ds(rows, rows), col(k)], fs.at[k], fr.at[k], partner)

        def p_copy(k):
            return remote(near_h.at[pl.ds(0, rows), col(k)], near_h.at[pl.ds(rows, rows), col(k)], ps.at[k], pr.at[k], partner)

        for k in range(STEPS):
            cols = slice(k * blk, (k + 1) * blk)
            gain = refs['ln_gain'][ln_row // 2, ln_row % 2:ln_row % 2 + 1, cols].astype(F32)
            bias = refs['ln_bias'][ln_row // 2, ln_row % 2:ln_row % 2 + 1, cols].astype(F32)
            normed = (xbuf[:, cols].astype(F32) - mean) * inv
            near_h[0:rows, cols] = (normed * (1.0 + gain) + bias).astype(BF)
            if k:
                c_copy(k - 1).start()
                p_copy(k - 1).start()
        acc[:, 0:n_out] = jnp.zeros((2 * rows, n_out), F32)
        c_copy(STEPS - 1).start()
        p_copy(STEPS - 1).start()
        ready()
        for k in range(STEPS):
            p_copy(k).wait_recv()

        n_blk = n_out // STEPS
        piece = min(1024, n_out)

        def far_dot(k, cols):
            return jnp.dot(far_h[:, col(k)], wbuf[col(k), w_at + cols.start:w_at + cols.stop], preferred_element_type=F32)

        def near_step(i):
            at = pl.ds(pl.multiple_of(w_at + i * n_blk, n_blk), n_blk)
            finish(0, col(i, n_blk), jnp.dot(near_h[...], wbuf[:, at], preferred_element_type=F32), [i])
            c_copy(i).wait_recv()
            f_copy(i).start()

        def step(i, carry):
            near_step(i)
            f_copy(i - 1).wait_recv()
            for n in range(n_out // piece):
                cols = slice(n * piece, (n + 1) * piece)
                acc[:, cols] += far_dot(i - 1, cols)
            return carry

        near_step(0)
        lax.fori_loop(1, STEPS, step, 0)
        f_copy(STEPS - 1).wait_recv()
        for n in range(n_out // piece):
            cols = slice(n * piece, (n + 1) * piece)
            finish(2, cols, acc[:, cols] + far_dot(STEPS - 1, cols), range(n * piece // n_blk, (n + 1) * piece // n_blk))
        for k in range(STEPS):
            c_copy(k).wait_send()
            p_copy(k).wait_send()
            f_copy(k).wait_send()

    def split(value):
        return value.reshape(2, n_seq, toks, value.shape[-1])

    def gather_qkv(layer, total, w_at, start_now):
        stage, y_out = refs['stage'], refs['y_out']
        n_out = y_out.shape[3]
        n_blk = n_out // STEPS

        def y_copy(g, n):
            return pltpu.make_async_copy(stage.at[g, :, :, col(n, n_blk)], y_out.at[:, order[g], :, col(n, n_blk)], refs['y_sem'].at[g, n])

        def ready():
            for copy in qkv_copies(layer, w_at):
                copy.wait()

        def finish(g, cols, value, blocks):
            stage[g:g + 2, :, :, cols] = split(value)
            for n in blocks:
                y_copy(g, n).start()
                y_copy(g + 1, n).start()

        gather('g2', 2 * layer, total, w_at, n_out, ready, finish)
        for g in range(4):
            for n in range(STEPS):
                y_copy(g, n).wait()

    def qkv_copies(layer, w_at):
        copies = []
        for i, name in enumerate(('w_q', 'w_k', 'w_v')):
            width = refs[name].shape[2]
            copies.append(pltpu.make_async_copy(refs[name].at[layer], wbuf.at[:, pl.ds(w_at, width)], refs['gw_sem'].at[i]))
            w_at += width
        return copies

    x_copy = pltpu.make_async_copy(refs['x_hbm'], xbuf, refs['x_sem'])
    if cfg['first']:
        x_copy.start()
        x_copy.wait()
        for copy in qkv_copies(0, 0):
            copy.start()
        total = jnp.zeros((rows, 128), F32)
        for n in range(STEPS):
            total = fold(xbuf[:, n * blk:(n + 1) * blk].astype(F32), total)
        pl.semaphore_wait(barrier, 2)
        gather_qkv(0, total, 0, True)
        return

    layer = cfg['layer']
    abuf, act = refs['abuf'], refs['act']
    depth = abuf.shape[3]
    a_copies = [pltpu.make_async_copy(refs['a_hbm'].at[:, order[g]], abuf.at[g], refs['a_sem'].at[g]) for g in range(4)]

    def o_copy(n):
        return pltpu.make_async_copy(refs['w_o'].at[layer, :, col(n)], wbuf.at[pl.ds(0, depth), col(n)], refs['ow_sem'].at[n])

    def up_copy(i):
        span = pl.ds(0, depth) if i else pl.ds(depth, d_model - depth)
        return pltpu.make_async_copy(refs['w_up'].at[layer, span, :], wbuf.at[span, pl.ds(0, d_model)], refs['uw_sem'].at[i])

    def down_slot(n):
        return lax.rem(n + STEPS, WIDE)

    def down_copy(n):
        return pltpu.make_async_copy(refs['w_down'].at[layer, :, col(n)], wbuf.at[:, col(down_slot(n))], refs['dw_sem'].at[n])

    for g in (2, 3):
        a_copies[g].start()
    o_copy(0).start()
    for g in (0, 1):
        a_copies[g].start()
    o_copy(1).start()
    o_copy(2).start()
    x_copy.start()
    pl.semaphore_wait(barrier, 2)
    for copy in a_copies:
        copy.wait()

    def late_up(i):
        up_copy(i).start()
        if i:
            x_copy.wait()

    total = scatter('s1', abuf, o_copy, lambda n: n, depth, 3, late_up)

    def ready_up():
        for i in range(2):
            up_copy(i).wait()
        for n in range(WIDE - STEPS):
            down_copy(n).start()

    def finish_up(g, cols, value, blocks):
        act[g:g + 2, :, :, cols] = split(jnp.square(jnp.maximum(value, 0.0)).astype(BF))

    gather('g1', 2 * layer + 1, total, 0, d_model, ready_up, finish_up)

    w_at = (WIDE * blk) - (4 * blk)

    def late_qkv(i):
        if i == 0 and cfg['more']:
            for copy in qkv_copies(layer + 1, w_at):
                copy.start()

    total = scatter('s2', act, down_copy, down_slot, d_model, WIDE - STEPS, late_qkv)
    out_copy = pltpu.make_async_copy(xbuf, refs['x_out'], refs['x_sem'])
    out_copy.start()
    if cfg['more']:
        gather_qkv(layer + 1, total, w_at, False)
    out_copy.wait()


def exchange(cid, x, ln_gain, ln_bias, qkv_weights, *, n_seq, layer=-1, more=True, a=None, weights=()):
    rows, d_model = x.shape
    toks = rows // n_seq
    blk = d_model // STEPS
    first = a is None
    any_spec, vmem = pl.BlockSpec(memory_space=pl.ANY), pl.BlockSpec(memory_space=pltpu.VMEM)
    dma = pltpu.SemaphoreType.DMA
    ins = [('x_hbm', x, any_spec), ('ln_gain', ln_gain, vmem), ('ln_bias', ln_bias, vmem)]
    outs = []
    qkv_out = sum(w.shape[2] for w in qkv_weights)
    width = qkv_out if first else WIDE * blk
    scr = [('wbuf', pltpu.VMEM((d_model, width), BF)), ('xbuf', pltpu.VMEM((rows, d_model), BF)), ('x_sem', dma)]
    scr += [
        ('near_h', pltpu.VMEM((2 * rows, d_model), BF)), ('far_h', pltpu.VMEM((2 * rows, d_model), BF)),
        ('acc', pltpu.VMEM((2 * rows, qkv_out if first else d_model), F32)),
    ]
    gather_tags, flops, moved = [], 0, 4_000_000
    if not first:
        w_o, w_up, w_down = weights
        depth = a.shape[3]
        ins += [('a_hbm', a, any_spec), ('w_o', w_o, any_spec), ('w_up', w_up, any_spec), ('w_down', w_down, any_spec)]
        outs += [('x_out', jax.ShapeDtypeStruct(x.shape, BF))]
        scr += [
            ('abuf', pltpu.VMEM((4, n_seq, toks, depth), BF)), ('act', pltpu.VMEM((4, n_seq, toks, d_model), BF)),
            ('dsend', pltpu.VMEM((STEPS, 2, rows, blk), BF)), ('drecv', pltpu.VMEM((STEPS, 2, rows, blk), BF)),
            ('qsend', pltpu.VMEM((STEPS, rows, blk), BF)), ('qrecv', pltpu.VMEM((STEPS, rows, blk), BF)),
            ('own', pltpu.VMEM((STEPS, rows, blk), F32)), ('part', pltpu.VMEM((rows, blk), F32)),
            ('a_sem', dma((4,))), ('ow_sem', dma((STEPS,))), ('uw_sem', dma((2,))), ('dw_sem', dma((STEPS,))),
        ]
        for tag in ('s1', 's2'):
            scr += [(tag + k, dma((STEPS, 2))) for k in ('ds', 'dr')] + [(tag + k, dma((STEPS,))) for k in ('qs', 'qr')]
        gather_tags.append('g1')
        flops += 2 * 4 * rows * d_model * (depth + 2 * d_model)
        moved += 2 * d_model * (depth + 2 * d_model)
    if more:
        ins += list(zip(('w_q', 'w_k', 'w_v'), qkv_weights, [any_spec] * 3))
        outs += [('y_out', jax.ShapeDtypeStruct((n_seq, 4, toks, qkv_out), F32))]
        scr += [('stage', pltpu.VMEM((4, n_seq, toks, qkv_out), F32)), ('gw_sem', dma((3,))), ('y_sem', dma((4, STEPS)))]
        gather_tags.append('g2')
        flops += 2 * 4 * rows * d_model * qkv_out
        moved += 2 * d_model * qkv_out
    for tag in gather_tags:
        scr += [(tag + k, dma((STEPS,))) for k in ('cs', 'cr', 'fs', 'fr', 'ps', 'pr')]
    cfg = dict(names=[i[0] for i in ins] + [o[0] for o in outs] + [s[0] for s in scr], layer=layer, first=first, more=more, n_seq=n_seq, toks=toks, d_model=d_model)
    return pl.pallas_call(
        functools.partial(exchange_kernel, cfg),
        in_specs=[i[2] for i in ins],
        out_specs=[any_spec] * len(outs),
        out_shape=[o[1] for o in outs],
        scratch_shapes=[s[1] for s in scr],
        compiler_params=pltpu.CompilerParams(collective_id=cid, has_side_effects=True, vmem_limit_bytes=67_000_000),
        cost_estimate=pl.CostEstimate(flops=flops, bytes_accessed=moved, transcendentals=0),
        name='gather_first' if first else 'block' if more else 'block_last',
    )(*[i[1] for i in ins])


def solution(mesh):
    tok_spec = P('dp', 'tp', None)
    cache_spec = P(None, 'dp', 'tp', None, None)
    col_spec = P(None, None, 'tp')
    row_spec = P(None, 'tp', None)

    def device_fn(x_loc, start_pos, k_cache, v_cache, w_q, w_k, w_v, w_o, w_up, w_down, ln_gain, ln_bias):
        n_layers = w_q.shape[0]
        n_seq, tok_loc, d_model = x_loc.shape
        new_len = tok_loc * 4
        rows = n_seq * new_len
        positions = (start_pos[:, None] + jnp.arange(new_len, dtype=jnp.int32)[None, :]).reshape(rows)
        tabs = rope_tables(positions, k_cache.shape[4])
        hidden = x_loc.reshape(n_seq * tok_loc, d_model)
        prev = ()
        qkv_weights = (w_q, w_k, w_v)
        qkv, = exchange(0, hidden, ln_gain, ln_bias, qkv_weights, n_seq=n_seq)
        for layer in range(n_layers):
            context, *prev = attend(layer, qkv.reshape(rows, -1), tabs, start_pos, k_cache, v_cache, prev)
            context = context.reshape(n_seq, 4, tok_loc, -1)
            outs = exchange(layer + 1, hidden, ln_gain, ln_bias, qkv_weights, n_seq=n_seq, layer=layer, more=layer + 1 < n_layers, a=context, weights=(w_o, w_up, w_down))
            hidden, qkv = outs if layer + 1 < n_layers else (outs[0], None)
        return hidden.reshape(x_loc.shape), prev[0], prev[1]

    return jax.shard_map(device_fn, mesh=mesh, in_specs=(tok_spec, P('dp'), cache_spec, cache_spec, col_spec, col_spec, col_spec, row_spec, col_spec, row_spec, P(), P()), out_specs=(tok_spec, cache_spec, cache_spec), check_vma=False)
```

```python
import functools
import math

import jax
import jax.numpy as jnp
from jax import lax
from jax.experimental import pallas as pl
from jax.experimental.pallas import tpu as pltpu
from jax.sharding import PartitionSpec as P

LN_EPS = 1e-5
ROPE_BASE = 10000.0
NEG_BIG = -1e30
MIN_START = 768
BF = jnp.bfloat16
F32 = jnp.float32


def rope_tables(start_pos, toks, head_dim):
    rot = head_dim // 2
    half = rot // 2
    shape = (start_pos.shape[0], toks, head_dim)
    lane = lax.broadcasted_iota(jnp.int32, shape, 2)
    position = start_pos[:, None, None] + lax.broadcasted_iota(jnp.int32, shape, 1)
    angles = position.astype(F32) * ROPE_BASE ** (-((lane % half).astype(F32) * (2.0 / rot)))
    cos_a, sin_a = jnp.cos(angles), jnp.sin(angles)
    return [jnp.where(lane < rot, cos_a, 1.0), jnp.where((lane >= half) & (lane < rot), sin_a, 0.0), jnp.where(lane < half, -sin_a, 0.0)]


def attn_kernel(layer, dims, start_ref, q_ref, k_ref, v_ref, c_ref, up_ref, dn_ref, kc_hbm, vc_hbm, *rest):
    kv, group, toks, hd, s_len, ch = dims
    if layer > 0:
        rest = rest[2:]
    ctx_ref, ko_hbm, vo_hbm, kbuf, vbuf, sbuf, ebuf, qbuf, mbuf, pbuf, lbuf, abuf, in_sem, out_sem = rest
    b = pl.program_id(0)
    nb = pl.num_programs(0) - 1
    s_pad = kbuf.shape[2]
    win = toks + 16
    rows = group * toks
    coef = (hd ** -0.5) * math.log2(math.e)
    slot = lax.rem(b, 3)
    before = lax.rem(b + 2, 3)

    def load(bb):
        sl = lax.rem(bb, 3)
        return [pltpu.make_async_copy(src.at[layer, bb], dst.at[sl, :, pl.ds(0, s_len), :], in_sem.at[sl, i]) for i, (src, dst) in enumerate(((kc_hbm, kbuf), (vc_hbm, vbuf)))]

    def save(bb):
        sl = lax.rem(bb, 3)
        return [pltpu.make_async_copy(src.at[sl, :, pl.ds(0, s_len), :], dst.at[layer, bb], out_sem.at[sl, i]) for i, (src, dst) in enumerate(((kbuf, ko_hbm), (vbuf, vo_hbm)))]

    def run(copies, go):
        for copy in copies:
            copy.start() if go else copy.wait()

    @pl.when(b == 0)
    def _():
        run(load(b), True)
        if s_pad > s_len:
            for sl in range(3):
                kbuf[sl, :, s_len:, :] = jnp.zeros((kv, s_pad - s_len, hd), BF)
                vbuf[sl, :, s_len:, :] = jnp.zeros((kv, s_pad - s_len, hd), BF)

    @pl.when(b >= 2)
    def _():
        run(save(b - 2), False)

    @pl.when(b + 1 < nb)
    def _():
        run(load(b + 1), True)

    start = start_ref[jnp.minimum(b, nb - 1)]
    start_before = start_ref[jnp.maximum(b - 1, 0)]
    half = hd // 4

    def rope(x):
        return x * c_ref[0] + pltpu.roll(x, half, 1) * up_ref[0] + pltpu.roll(x, hd - half, 1) * dn_ref[0]

    def patch():
        base = jnp.minimum((start // 16) * 16, s_len - win)
        shift = start - base
        base = pl.multiple_of(base, 16)
        row_id = lax.broadcasted_iota(jnp.int32, (win, hd), 0)
        is_new = jnp.logical_and(row_id >= shift, row_id < shift + toks)
        run(load(b), False)
        for h in range(kv):
            cols = slice(h * hd, (h + 1) * hd)
            for buf, fresh in ((kbuf, rope(k_ref[:, cols])), (vbuf, v_ref[:, cols])):
                fresh = fresh.astype(BF).astype(F32)
                fresh = jnp.concatenate([fresh, jnp.zeros((16, hd), F32)], axis=0)
                fresh = pltpu.roll(fresh, shift, 0)
                old = buf[slot, h, pl.ds(base, win), :].astype(F32)
                buf[slot, h, pl.ds(base, win), :] = jnp.where(is_new, fresh, old).astype(BF)
        run(save(b), True)

    step_rows = 64
    blocks = [slice(r, r + step_rows) for r in range(0, ch, step_rows)]

    def chunk(j):
        return pl.ds(pl.multiple_of(j * ch, ch), ch)

    def score(h, j, masked):
        s = lax.dot_general(kbuf[slot, h, chunk(j), :], qbuf[h], (((1,), (1,)), ((), ())), preferred_element_type=F32)
        if masked:
            ahead = lax.broadcasted_iota(jnp.int32, (ch, rows), 0) - lax.rem(lax.broadcasted_iota(jnp.int32, (ch, rows), 1), toks)
            s = jnp.where(ahead <= start - j * ch, s, NEG_BIG)
        sbuf[h] = s

    def scored(h, rb):
        return sbuf[h, rb].reshape(step_rows // 8, 8, rows)

    def peaks(h, peak):
        top = jnp.max(scored(h, blocks[0]), axis=0)
        for rb in blocks[1:]:
            top = jnp.maximum(top, jnp.max(scored(h, rb), axis=0))
        mbuf[h] = peak
        pbuf[h] = jnp.maximum(peak, jnp.max(top, axis=0, keepdims=True))

    def weigh(h):
        peak = pbuf[h]
        alpha = jnp.exp2((mbuf[h] - peak) * coef)
        total = lbuf[h] * alpha
        for rb in blocks:
            e = jnp.exp2((scored(h, rb) - peak) * coef)
            total = total + jnp.sum(e, axis=0)
            ebuf[h, rb] = e.reshape(step_rows, rows).astype(BF)
        return alpha, total

    def mix(h, sl, j, alpha):
        fresh = lax.dot_general(vbuf[sl, h, chunk(j), :], ebuf[h], (((0,), (0,)), ((), ())), preferred_element_type=F32)
        return (abuf[h].reshape(hd // 8, 8, rows) * alpha).reshape(hd, rows) + fresh

    def step(masked_next, j, carry):
        for h in range(kv):
            alpha, lbuf[h] = weigh(h)
            score(h, j + 1, masked_next)
            abuf[h] = mix(h, slot, j, alpha)
        for h in range(kv):
            peaks(h, pbuf[h])
        return carry

    def last_of(bb_start):
        return (bb_start + toks + ch - 1) // ch - 1

    def turn(close, open_next):
        if open_next:
            patch()
            for h in range(kv):
                for g in range(group):
                    j = h * group + g
                    qbuf[h, g * toks:(g + 1) * toks, :] = rope(q_ref[:, j * hd:(j + 1) * hd]).astype(BF)
        for h in range(kv):
            if close:
                alpha, total = weigh(h)
            if open_next:
                score(h, 0, ch > MIN_START)
            if close:
                ctx = (mix(h, before, last_of(start_before), alpha) / jnp.sum(total, axis=0, keepdims=True)).T.astype(BF)
                for g in range(group):
                    j = h * group + g
                    ctx_ref[:, j * hd:(j + 1) * hd] = ctx[g * toks:(g + 1) * toks, :]
        if open_next:
            for h in range(kv):
                peaks(h, jnp.full((8, rows), NEG_BIG, F32))
                lbuf[h] = jnp.zeros((8, rows), F32)
                abuf[h] = jnp.zeros((hd, rows), F32)

    pl.when(b == 0)(functools.partial(turn, False, True))
    pl.when(jnp.logical_and(b > 0, b < nb))(functools.partial(turn, True, True))
    pl.when(b == nb)(functools.partial(turn, True, False))

    @pl.when(b < nb)
    def _():
        n_full = jnp.maximum(start // ch, 1)
        lax.fori_loop(0, n_full - 1, functools.partial(step, False), 0)
        lax.fori_loop(n_full - 1, last_of(start), functools.partial(step, True), 0)

    @pl.when(b == nb)
    def _():
        run(save(b - 1), False)


def attend(layer, qkv, tabs, start_pos, k_cache, v_cache, prev):
    n_seq = start_pos.shape[0]
    _, _, kv, s_len, hd = k_cache.shape
    toks = qkv.shape[0] // n_seq
    kv_width = kv * hd
    q_width = qkv.shape[1] - 2 * kv_width
    group = q_width // kv_width
    n_ch = -(-s_len // 640)
    ch = 128 * -(-s_len // (128 * n_ch))
    rows = group * toks
    dims = (kv, group, toks, hd, s_len, ch)
    any_spec = pl.BlockSpec(memory_space=pl.ANY)
    now = lambda b: jnp.minimum(b, n_seq - 1)
    tab_spec = pl.BlockSpec((1, toks, hd), lambda b, *_: (now(b), 0, 0))
    cache_shape = jax.ShapeDtypeStruct(k_cache.shape, BF)
    args = [start_pos, qkv, qkv, qkv, *tabs, k_cache, v_cache] + list(prev)
    return pl.pallas_call(
        functools.partial(attn_kernel, layer, dims),
        grid_spec=pltpu.PrefetchScalarGridSpec(
            num_scalar_prefetch=1,
            grid=(n_seq + 1,),
            in_specs=[
                pl.BlockSpec((toks, q_width), lambda b, *_: (now(b), 0)),
                pl.BlockSpec((toks, kv_width), lambda b, *_: (now(b), group)),
                pl.BlockSpec((toks, kv_width), lambda b, *_: (now(b), group + 1)),
                tab_spec, tab_spec, tab_spec,
            ] + [any_spec] * (2 + len(prev)),
            out_specs=[pl.BlockSpec((toks, q_width), lambda b, *_: (jnp.maximum(b - 1, 0), 0)), any_spec, any_spec],
            scratch_shapes=[
                pltpu.VMEM((3, kv, ch * n_ch, hd), BF),
                pltpu.VMEM((3, kv, ch * n_ch, hd), BF),
                pltpu.VMEM((kv, ch, rows), F32),
                pltpu.VMEM((kv, ch, rows), BF),
                pltpu.VMEM((kv, rows, hd), BF),
                pltpu.VMEM((kv, 8, rows), F32),
                pltpu.VMEM((kv, 8, rows), F32),
                pltpu.VMEM((kv, 8, rows), F32),
                pltpu.VMEM((kv, hd, rows), F32),
                pltpu.SemaphoreType.DMA((3, 2)),
                pltpu.SemaphoreType.DMA((3, 2)),
            ],
        ),
        out_shape=[jax.ShapeDtypeStruct((n_seq * toks, q_width), BF), cache_shape, cache_shape],
        input_output_aliases={9: 1, 10: 2} if prev else {},
        compiler_params=pltpu.CompilerParams(vmem_limit_bytes=60 * 1024 * 1024, dimension_semantics=("arbitrary",)),
        cost_estimate=pl.CostEstimate(flops=8_000_000_000, bytes_accessed=80_000_000, transcendentals=15_000_000),
        name="attend",
    )(*args)


STEPS = 8
WIDE = STEPS + 2


def exchange_kernel(cfg, *args):
    refs = dict(zip(cfg['names'], args))
    n_seq, toks, d_model = cfg['n_seq'], cfg['toks'], cfg['d_model']
    rows = n_seq * toks
    blk = d_model // STEPS
    me = lax.axis_index('tp')
    core = lax.rem(me, 2)
    partner = me + 1 - 2 * core
    counter = lax.rem(me + 2, 4)
    diag = lax.rem(partner + 2, 4)
    order = (me, partner, counter, diag)
    wbuf, xbuf = refs['wbuf'], refs['xbuf']

    barrier = pltpu.get_barrier_semaphore()
    for peer in (partner, counter):
        pl.semaphore_signal(barrier, inc=1, device_id={'tp': peer}, device_id_type=pl.DeviceIdType.MESH)

    def col(n, width=blk):
        return pl.ds(pl.multiple_of(n * width, width), width)

    def remote(src, dst, send, recv, peer):
        return pltpu.make_async_remote_copy(src_ref=src, dst_ref=dst, send_sem=send, recv_sem=recv, device_id={'tp': peer}, device_id_type=pl.DeviceIdType.MESH)

    def fold(values, total):
        for j in range(blk // 128):
            total = total + values[:, j * 128:(j + 1) * 128]
        return total

    def scatter(tag, a_ref, w_copy, slot_of, depth, ahead, late, add=True):
        dsend, drecv, qsend, qrecv, own, part = (refs[k] for k in ('dsend', 'drecv', 'qsend', 'qrecv', 'own', 'part'))
        ds_sem, dr_sem, qs_sem, qr_sem = (refs[tag + k] for k in ('ds', 'dr', 'qs', 'qr'))

        def d_copy(n, i):
            return remote(dsend.at[n, i], drecv.at[n, i], ds_sem.at[n, i], dr_sem.at[n, i], partner)

        def q_copy(n):
            return remote(qsend.at[n], qrecv.at[n], qs_sem.at[n], qr_sem.at[n], counter)

        def step(n, carry):
            @pl.when(n + ahead < STEPS)
            def _():
                w_copy(n + ahead).start()

            w_copy(n).wait()
            cols = col(slot_of(n))
            far = jnp.dot(a_ref[2:4].reshape(2 * rows, depth), wbuf[0:depth, cols], preferred_element_type=F32)
            dsend[n, 0] = far[rows:].astype(BF)
            d_copy(n, 0).start()
            part[...] = far[:rows]
            near = jnp.dot(a_ref[0:2].reshape(2 * rows, depth), wbuf[0:depth, cols], preferred_element_type=F32)
            dsend[n, 1] = near[rows:].astype(BF)
            d_copy(n, 1).start()
            own[n] = near[:rows]
            d_copy(n, 0).wait_recv()
            qsend[n] = (part[...] + drecv[n, 0].astype(F32)).astype(BF)
            q_copy(n).start()
            return carry

        half = STEPS - 3
        lax.fori_loop(0, half, step, 0)
        late(0)
        lax.fori_loop(half, STEPS, step, 0)
        late(1)
        total = jnp.zeros((rows, 128), F32)
        for n in range(STEPS):
            cols = slice(n * blk, (n + 1) * blk)
            d_copy(n, 1).wait_recv()
            q_copy(n).wait_recv()
            summed = own[n] + drecv[n, 1].astype(F32) + qrecv[n].astype(F32)
            if not add:
                xbuf[:, cols] = summed.astype(BF)
                continue
            fresh = (xbuf[:, cols].astype(F32) + summed.astype(BF).astype(F32)).astype(BF)
            xbuf[:, cols] = fresh
            total = fold(fresh.astype(F32), total)
        for n in range(STEPS):
            d_copy(n, 0).wait_send()
            d_copy(n, 1).wait_send()
            q_copy(n).wait_send()
        return total

    def gather(tag, ln_row, total, w_at, n_out, ready, finish):
        near_h, far_h, acc = refs['near_h'], refs['far_h'], refs['acc']
        cs, cr, fs, fr, ps, pr = (refs[tag + k] for k in ('cs', 'cr', 'fs', 'fr', 'ps', 'pr'))
        mean = jnp.sum(total, axis=-1, keepdims=True) / d_model
        total = jnp.zeros((rows, 128), F32)
        for n in range(STEPS):
            diff = xbuf[:, n * blk:(n + 1) * blk].astype(F32) - mean
            total = fold(diff * diff, total)
        inv = lax.rsqrt(jnp.sum(total, axis=-1, keepdims=True) / d_model + LN_EPS)

        def c_copy(k):
            return remote(near_h.at[pl.ds(0, rows), col(k)], far_h.at[pl.ds(0, rows), col(k)], cs.at[k], cr.at[k], counter)

        def f_copy(k):
            return remote(far_h.at[pl.ds(0, rows), col(k)], far_h.at[pl.ds(rows, rows), col(k)], fs.at[k], fr.at[k], partner)

        def p_copy(k):
            return remote(near_h.at[pl.ds(0, rows), col(k)], near_h.at[pl.ds(rows, rows), col(k)], ps.at[k], pr.at[k], partner)

        for k in range(STEPS):
            cols = slice(k * blk, (k + 1) * blk)
            gain = refs['ln_gain'][ln_row // 2, ln_row % 2:ln_row % 2 + 1, cols].astype(F32)
            bias = refs['ln_bias'][ln_row // 2, ln_row % 2:ln_row % 2 + 1, cols].astype(F32)
            normed = (xbuf[:, cols].astype(F32) - mean) * inv
            near_h[0:rows, cols] = (normed * (1.0 + gain) + bias).astype(BF)
            if k:
                c_copy(k - 1).start()
                p_copy(k - 1).start()
        acc[:, 0:n_out] = jnp.zeros((2 * rows, n_out), F32)
        c_copy(STEPS - 1).start()
        p_copy(STEPS - 1).start()
        ready()
        for k in range(STEPS):
            p_copy(k).wait_recv()

        n_blk = n_out // STEPS
        piece = min(1024, n_out)

        def far_dot(k, cols):
            return jnp.dot(far_h[:, col(k)], wbuf[col(k), w_at + cols.start:w_at + cols.stop], preferred_element_type=F32)

        def near_step(i):
            at = pl.ds(pl.multiple_of(w_at + i * n_blk, n_blk), n_blk)
            finish(0, col(i, n_blk), jnp.dot(near_h[...], wbuf[:, at], preferred_element_type=F32), [i])
            c_copy(i).wait_recv()
            f_copy(i).start()

        def step(i, carry):
            near_step(i)
            f_copy(i - 1).wait_recv()
            for n in range(n_out // piece):
                cols = slice(n * piece, (n + 1) * piece)
                acc[:, cols] += far_dot(i - 1, cols)
            return carry

        near_step(0)
        lax.fori_loop(1, STEPS, step, 0)
        f_copy(STEPS - 1).wait_recv()
        for n in range(n_out // piece):
            cols = slice(n * piece, (n + 1) * piece)
            finish(2, cols, acc[:, cols] + far_dot(STEPS - 1, cols), range(n * piece // n_blk, (n + 1) * piece // n_blk))
        for k in range(STEPS):
            c_copy(k).wait_send()
            p_copy(k).wait_send()
            f_copy(k).wait_send()

    def split(value):
        return value.reshape(2, n_seq, toks, value.shape[-1])

    def gather_qkv(layer, total, w_at, start_now):
        stage, y_out = refs['stage'], refs['y_out']
        n_out = y_out.shape[3]
        n_blk = n_out // STEPS

        def y_copy(g, n):
            return pltpu.make_async_copy(stage.at[g, :, :, col(n, n_blk)], y_out.at[:, order[g], :, col(n, n_blk)], refs['y_sem'].at[g, n])

        def ready():
            for copy in qkv_copies(layer, w_at):
                copy.wait()

        def finish(g, cols, value, blocks):
            stage[g:g + 2, :, :, cols] = split(value)
            for n in blocks:
                y_copy(g, n).start()
                y_copy(g + 1, n).start()

        gather('g2', 2 * layer, total, w_at, n_out, ready, finish)
        for g in range(4):
            for n in range(STEPS):
                y_copy(g, n).wait()

    def qkv_copies(layer, w_at):
        copies = []
        for i, name in enumerate(('w_q', 'w_k', 'w_v')):
            width = refs[name].shape[2]
            copies.append(pltpu.make_async_copy(refs[name].at[layer], wbuf.at[:, pl.ds(w_at, width)], refs['gw_sem'].at[i]))
            w_at += width
        return copies

    x_copy = pltpu.make_async_copy(refs['x_hbm'], xbuf, refs['x_sem'])
    if cfg['first']:
        x_copy.start()
        x_copy.wait()
        for copy in qkv_copies(0, 0):
            copy.start()
        total = jnp.zeros((rows, 128), F32)
        for n in range(STEPS):
            total = fold(xbuf[:, n * blk:(n + 1) * blk].astype(F32), total)
        pl.semaphore_wait(barrier, 2)
        gather_qkv(0, total, 0, True)
        return

    layer = cfg['layer']
    abuf, act = refs['abuf'], refs['act']
    depth = abuf.shape[3]
    a_copies = [pltpu.make_async_copy(refs['a_hbm'].at[:, order[g]], abuf.at[g], refs['a_sem'].at[g]) for g in range(4)]

    def o_copy(n):
        return pltpu.make_async_copy(refs['w_o'].at[layer, :, col(n)], wbuf.at[pl.ds(0, depth), col(n)], refs['ow_sem'].at[n])

    def up_copy(i):
        span = pl.ds(0, depth) if i else pl.ds(depth, d_model - depth)
        return pltpu.make_async_copy(refs['w_up'].at[layer, span, :], wbuf.at[span, pl.ds(0, d_model)], refs['uw_sem'].at[i])

    def down_slot(n):
        return lax.rem(n + STEPS, WIDE)

    def down_copy(n):
        return pltpu.make_async_copy(refs['w_down'].at[layer, :, col(n)], wbuf.at[:, col(down_slot(n))], refs['dw_sem'].at[n])

    for g in (2, 3):
        a_copies[g].start()
    o_copy(0).start()
    for g in (0, 1):
        a_copies[g].start()
    o_copy(1).start()
    o_copy(2).start()
    x_copy.start()
    pl.semaphore_wait(barrier, 2)
    for copy in a_copies:
        copy.wait()

    def late_up(i):
        up_copy(i).start()
        if i:
            x_copy.wait()

    total = scatter('s1', abuf, o_copy, lambda n: n, depth, 3, late_up)

    def ready_up():
        for i in range(2):
            up_copy(i).wait()
        for n in range(WIDE - STEPS):
            down_copy(n).start()

    def finish_up(g, cols, value, blocks):
        act[g:g + 2, :, :, cols] = split(jnp.square(jnp.maximum(value, 0.0)).astype(BF))

    if not cfg['more']:
        mid_copy = pltpu.make_async_copy(xbuf, refs['x_mid'], refs['x_sem'])
        mid_copy.start()
    gather('g1', 2 * layer + 1, total, 0, d_model, ready_up, finish_up)

    w_at = (WIDE * blk) - (4 * blk)

    def late_qkv(i):
        if i == 0 and cfg['more']:
            for copy in qkv_copies(layer + 1, w_at):
                copy.start()

    if not cfg['more']:
        mid_copy.wait()
    total = scatter('s2', act, down_copy, down_slot, d_model, WIDE - STEPS, late_qkv, cfg['more'])
    out_copy = pltpu.make_async_copy(xbuf, refs['x_out'], refs['x_sem'])
    out_copy.start()
    if cfg['more']:
        gather_qkv(layer + 1, total, w_at, False)
    out_copy.wait()


def exchange(cid, x, ln_gain, ln_bias, qkv_weights, *, n_seq, layer=-1, more=True, a=None, weights=()):
    rows, d_model = x.shape
    toks = rows // n_seq
    blk = d_model // STEPS
    first = a is None
    any_spec, vmem = pl.BlockSpec(memory_space=pl.ANY), pl.BlockSpec(memory_space=pltpu.VMEM)
    dma = pltpu.SemaphoreType.DMA
    ins = [('x_hbm', x, any_spec), ('ln_gain', ln_gain, vmem), ('ln_bias', ln_bias, vmem)]
    outs = []
    qkv_out = sum(w.shape[2] for w in qkv_weights)
    width = qkv_out if first else WIDE * blk
    scr = [('wbuf', pltpu.VMEM((d_model, width), BF)), ('xbuf', pltpu.VMEM((rows, d_model), BF)), ('x_sem', dma)]
    scr += [
        ('near_h', pltpu.VMEM((2 * rows, d_model), BF)), ('far_h', pltpu.VMEM((2 * rows, d_model), BF)),
        ('acc', pltpu.VMEM((2 * rows, qkv_out if first else d_model), F32)),
    ]
    gather_tags, flops, moved = [], 0, 4_000_000
    if not first:
        w_o, w_up, w_down = weights
        depth = a.shape[3]
        ins += [('a_hbm', a, any_spec), ('w_o', w_o, any_spec), ('w_up', w_up, any_spec), ('w_down', w_down, any_spec)]
        outs += [('x_out', jax.ShapeDtypeStruct(x.shape, BF))]
        scr += [
            ('abuf', pltpu.VMEM((4, n_seq, toks, depth), BF)), ('act', pltpu.VMEM((4, n_seq, toks, d_model), BF)),
            ('dsend', pltpu.VMEM((STEPS, 2, rows, blk), BF)), ('drecv', pltpu.VMEM((STEPS, 2, rows, blk), BF)),
            ('qsend', pltpu.VMEM((STEPS, rows, blk), BF)), ('qrecv', pltpu.VMEM((STEPS, rows, blk), BF)),
            ('own', pltpu.VMEM((STEPS, rows, blk), F32)), ('part', pltpu.VMEM((rows, blk), F32)),
            ('a_sem', dma((4,))), ('ow_sem', dma((STEPS,))), ('uw_sem', dma((2,))), ('dw_sem', dma((STEPS,))),
        ]
        for tag in ('s1', 's2'):
            scr += [(tag + k, dma((STEPS, 2))) for k in ('ds', 'dr')] + [(tag + k, dma((STEPS,))) for k in ('qs', 'qr')]
        if not more:
            outs += [('x_mid', jax.ShapeDtypeStruct(x.shape, BF))]
        gather_tags.append('g1')
        flops += 2 * 4 * rows * d_model * (depth + 2 * d_model)
        moved += 2 * d_model * (depth + 2 * d_model)
    if more:
        ins += list(zip(('w_q', 'w_k', 'w_v'), qkv_weights, [any_spec] * 3))
        outs += [('y_out', jax.ShapeDtypeStruct((n_seq, 4, toks, qkv_out), F32))]
        scr += [('stage', pltpu.VMEM((4, n_seq, toks, qkv_out), F32)), ('gw_sem', dma((3,))), ('y_sem', dma((4, STEPS)))]
        gather_tags.append('g2')
        flops += 2 * 4 * rows * d_model * qkv_out
        moved += 2 * d_model * qkv_out
    for tag in gather_tags:
        scr += [(tag + k, dma((STEPS,))) for k in ('cs', 'cr', 'fs', 'fr', 'ps', 'pr')]
    cfg = dict(names=[i[0] for i in ins] + [o[0] for o in outs] + [s[0] for s in scr], layer=layer, first=first, more=more, n_seq=n_seq, toks=toks, d_model=d_model)
    return pl.pallas_call(
        functools.partial(exchange_kernel, cfg),
        in_specs=[i[2] for i in ins],
        out_specs=[any_spec] * len(outs),
        out_shape=[o[1] for o in outs],
        scratch_shapes=[s[1] for s in scr],
        compiler_params=pltpu.CompilerParams(collective_id=cid, has_side_effects=True, vmem_limit_bytes=67_000_000),
        cost_estimate=pl.CostEstimate(flops=flops, bytes_accessed=moved, transcendentals=0),
        name='gather_first' if first else 'block' if more else 'block_last',
    )(*[i[1] for i in ins])


def solution(mesh):
    tok_spec = P('dp', 'tp', None)
    cache_spec = P(None, 'dp', 'tp', None, None)
    col_spec = P(None, None, 'tp')
    row_spec = P(None, 'tp', None)

    def device_fn(x_loc, start_pos, k_cache, v_cache, w_q, w_k, w_v, w_o, w_up, w_down, ln_gain, ln_bias):
        n_layers = w_q.shape[0]
        n_seq, tok_loc, d_model = x_loc.shape
        new_len = tok_loc * 4
        rows = n_seq * new_len
        tabs = rope_tables(start_pos, new_len, k_cache.shape[4])
        hidden = x_loc.reshape(n_seq * tok_loc, d_model)
        prev = ()
        qkv_weights = (w_q, w_k, w_v)
        qkv, = exchange(0, hidden, ln_gain, ln_bias, qkv_weights, n_seq=n_seq)
        for layer in range(n_layers):
            context, *prev = attend(layer, qkv.reshape(rows, -1), tabs, start_pos, k_cache, v_cache, prev)
            context = context.reshape(n_seq, 4, tok_loc, -1)
            outs = exchange(layer + 1, hidden, ln_gain, ln_bias, qkv_weights, n_seq=n_seq, layer=layer, more=layer + 1 < n_layers, a=context, weights=(w_o, w_up, w_down))
            if layer + 1 < n_layers:
                hidden, qkv = outs
            else:
                hidden = (outs[1].astype(F32) + outs[0].astype(F32)).astype(BF)
        return hidden.reshape(x_loc.shape), prev[0], prev[1]

    return jax.shard_map(device_fn, mesh=mesh, in_specs=(tok_spec, P('dp'), cache_spec, cache_spec, col_spec, col_spec, col_spec, row_spec, col_spec, row_spec, P(), P()), out_specs=(tok_spec, cache_spec, cache_spec), check_vma=False)
```

```python
import functools
import math

import jax
import jax.numpy as jnp
from jax import lax
from jax.experimental import pallas as pl
from jax.experimental.pallas import tpu as pltpu
from jax.sharding import PartitionSpec as P

LN_EPS = 1e-5
ROPE_BASE = 10000.0
NEG_BIG = -1e30
MIN_START = 768
SLOTS = 4
BF = jnp.bfloat16
F32 = jnp.float32


def rope_tables(start, toks, head_dim):
    rot = head_dim // 2
    half = rot // 2
    shape = (toks, head_dim)
    lane = lax.broadcasted_iota(jnp.int32, shape, 1)
    position = start + lax.broadcasted_iota(jnp.int32, shape, 0)
    power = lax.rem(lane, half).astype(F32) * (2.0 / rot)
    angles = position.astype(F32) * jnp.exp(power * -math.log(ROPE_BASE))
    cos_a, sin_a = jnp.cos(angles), jnp.sin(angles)
    upper = jnp.logical_and(lane >= half, lane < rot)
    return jnp.where(lane < rot, cos_a, 1.0), jnp.where(upper, sin_a, 0.0), jnp.where(lane < half, -sin_a, 0.0)


def attn_kernel(layer, dims, start_ref, q_ref, k_ref, v_ref, tab_ref, kc_hbm, vc_hbm, *rest):
    kv, group, toks, hd, s_len, ch = dims
    if layer > 0:
        rest = rest[2:]
    ctx_ref, ko_hbm, vo_hbm, kbuf, vbuf, sbuf, ebuf, qbuf, mbuf, pbuf, lbuf, abuf, in_sem, out_sem = rest
    b = pl.program_id(0)
    nb = pl.num_programs(0) - 1
    s_pad = kbuf.shape[2]
    win = toks + 16
    rows = group * toks
    coef = (hd ** -0.5) * math.log2(math.e)
    slot = lax.rem(b, SLOTS)
    before = lax.rem(b + SLOTS - 1, SLOTS)

    def load(bb):
        sl = lax.rem(bb, SLOTS)
        return [pltpu.make_async_copy(src.at[layer, bb], dst.at[sl, :, pl.ds(0, s_len), :], in_sem.at[sl, i]) for i, (src, dst) in enumerate(((kc_hbm, kbuf), (vc_hbm, vbuf)))]

    def save(bb):
        sl = lax.rem(bb, SLOTS)
        return [pltpu.make_async_copy(src.at[sl, :, pl.ds(0, s_len), :], dst.at[layer, bb], out_sem.at[sl, i]) for i, (src, dst) in enumerate(((kbuf, ko_hbm), (vbuf, vo_hbm)))]

    def run(copies, go):
        for copy in copies:
            copy.start() if go else copy.wait()

    @pl.when(b == 0)
    def _():
        run(load(b), True)
        if s_pad > s_len:
            for sl in range(SLOTS):
                kbuf[sl, :, s_len:, :] = jnp.zeros((kv, s_pad - s_len, hd), BF)
                vbuf[sl, :, s_len:, :] = jnp.zeros((kv, s_pad - s_len, hd), BF)

    @pl.when(b >= 2)
    def _():
        run(save(b - 2), False)

    @pl.when(jnp.logical_and(b > 0, b + 2 < nb))
    def _():
        run(load(b + 2), True)

    start = start_ref[jnp.minimum(b, nb - 1)]
    start_before = start_ref[jnp.maximum(b - 1, 0)]
    half = hd // 4

    def rope(x):
        return x * tab_ref[0, 0] + pltpu.roll(x, half, 1) * tab_ref[1, 0] + pltpu.roll(x, hd - half, 1) * tab_ref[2, 0]

    def patch():
        base = jnp.minimum((start // 16) * 16, s_len - win)
        shift = start - base
        base = pl.multiple_of(base, 16)
        row_id = lax.broadcasted_iota(jnp.int32, (win, hd), 0)
        is_new = jnp.logical_and(row_id >= shift, row_id < shift + toks)
        run(load(b), False)

        @pl.when(b == 0)
        def _():
            run(load(b + 1), True)
            run(load(b + 2), True)

        for h in range(kv):
            cols = slice(h * hd, (h + 1) * hd)
            for buf, fresh in ((kbuf, rope(k_ref[:, cols])), (vbuf, v_ref[:, cols])):
                fresh = fresh.astype(BF).astype(F32)
                fresh = jnp.concatenate([fresh, jnp.zeros((16, hd), F32)], axis=0)
                fresh = pltpu.roll(fresh, shift, 0)
                old = buf[slot, h, pl.ds(base, win), :].astype(F32)
                buf[slot, h, pl.ds(base, win), :] = jnp.where(is_new, fresh, old).astype(BF)
        run(save(b), True)

    step_rows = 64
    blocks = [slice(r, r + step_rows) for r in range(0, ch, step_rows)]

    def chunk(j):
        return pl.ds(pl.multiple_of(j * ch, ch), ch)

    def score(h, j, masked):
        s = lax.dot_general(kbuf[slot, h, chunk(j), :], qbuf[h], (((1,), (1,)), ((), ())), preferred_element_type=F32)
        if masked:
            ahead = lax.broadcasted_iota(jnp.int32, (ch, rows), 0) - lax.rem(lax.broadcasted_iota(jnp.int32, (ch, rows), 1), toks)
            s = jnp.where(ahead <= start - j * ch, s, NEG_BIG)
        sbuf[h] = s

    def scored(h, rb):
        return sbuf[h, rb].reshape(step_rows // 8, 8, rows)

    def peaks(h, peak):
        top = jnp.max(scored(h, blocks[0]), axis=0)
        for rb in blocks[1:]:
            top = jnp.maximum(top, jnp.max(scored(h, rb), axis=0))
        mbuf[h] = peak
        pbuf[h] = jnp.maximum(peak, jnp.max(top, axis=0, keepdims=True))

    def weigh(h):
        peak = pbuf[h]
        alpha = jnp.exp2((mbuf[h] - peak) * coef)
        total = lbuf[h] * alpha
        for rb in blocks:
            e = jnp.exp2((scored(h, rb) - peak) * coef)
            total = total + jnp.sum(e, axis=0)
            ebuf[h, rb] = e.reshape(step_rows, rows).astype(BF)
        return alpha, total

    def mix(h, sl, j, alpha):
        fresh = lax.dot_general(vbuf[sl, h, chunk(j), :], ebuf[h], (((0,), (0,)), ((), ())), preferred_element_type=F32)
        return (abuf[h].reshape(hd // 8, 8, rows) * alpha).reshape(hd, rows) + fresh

    def step(masked_next, j, carry):
        for h in range(kv):
            alpha, lbuf[h] = weigh(h)
            score(h, j + 1, masked_next)
            abuf[h] = mix(h, slot, j, alpha)
        for h in range(kv):
            peaks(h, pbuf[h])
        return carry

    def last_of(bb_start):
        return (bb_start + toks + ch - 1) // ch - 1

    def turn(close, open_next):
        if open_next:
            patch()
            for h in range(kv):
                for g in range(group):
                    j = h * group + g
                    qbuf[h, g * toks:(g + 1) * toks, :] = rope(q_ref[:, j * hd:(j + 1) * hd]).astype(BF)
        for h in range(kv):
            if close:
                alpha, total = weigh(h)
            if open_next:
                score(h, 0, ch > MIN_START)
            if close:
                ctx = (mix(h, before, last_of(start_before), alpha) / jnp.sum(total, axis=0, keepdims=True)).T.astype(BF)
                for g in range(group):
                    j = h * group + g
                    ctx_ref[:, j * hd:(j + 1) * hd] = ctx[g * toks:(g + 1) * toks, :]
        if open_next:
            for h in range(kv):
                peaks(h, jnp.full((8, rows), NEG_BIG, F32))
                lbuf[h] = jnp.zeros((8, rows), F32)
                abuf[h] = jnp.zeros((hd, rows), F32)

    pl.when(b == 0)(functools.partial(turn, False, True))
    pl.when(jnp.logical_and(b > 0, b < nb))(functools.partial(turn, True, True))
    pl.when(b == nb)(functools.partial(turn, True, False))

    @pl.when(b < nb)
    def _():
        n_full = jnp.maximum(start // ch, 1)
        lax.fori_loop(0, n_full - 1, functools.partial(step, False), 0)
        lax.fori_loop(n_full - 1, last_of(start), functools.partial(step, True), 0)

    @pl.when(b == nb)
    def _():
        run(save(b - 1), False)


def attend(layer, qkv, tabs, start_pos, k_cache, v_cache, prev):
    n_seq = start_pos.shape[0]
    _, _, kv, s_len, hd = k_cache.shape
    toks = qkv.shape[0] // n_seq
    kv_width = kv * hd
    q_width = qkv.shape[1] - 2 * kv_width
    group = q_width // kv_width
    n_ch = -(-s_len // 640)
    ch = 128 * -(-s_len // (128 * n_ch))
    rows = group * toks
    dims = (kv, group, toks, hd, s_len, ch)
    any_spec = pl.BlockSpec(memory_space=pl.ANY)
    now = lambda b: jnp.minimum(b, n_seq - 1)
    tab_spec = pl.BlockSpec((3, 1, toks, hd), lambda b, *_: (0, now(b), 0, 0))
    cache_shape = jax.ShapeDtypeStruct(k_cache.shape, BF)
    args = [start_pos, qkv, qkv, qkv, tabs, k_cache, v_cache] + list(prev)
    return pl.pallas_call(
        functools.partial(attn_kernel, layer, dims),
        grid_spec=pltpu.PrefetchScalarGridSpec(
            num_scalar_prefetch=1,
            grid=(n_seq + 1,),
            in_specs=[
                pl.BlockSpec((toks, q_width), lambda b, *_: (now(b), 0)),
                pl.BlockSpec((toks, kv_width), lambda b, *_: (now(b), group)),
                pl.BlockSpec((toks, kv_width), lambda b, *_: (now(b), group + 1)),
                tab_spec,
            ] + [any_spec] * (2 + len(prev)),
            out_specs=[pl.BlockSpec((toks, q_width), lambda b, *_: (jnp.maximum(b - 1, 0), 0)), any_spec, any_spec],
            scratch_shapes=[
                pltpu.VMEM((SLOTS, kv, ch * n_ch, hd), BF),
                pltpu.VMEM((SLOTS, kv, ch * n_ch, hd), BF),
                pltpu.VMEM((kv, ch, rows), F32),
                pltpu.VMEM((kv, ch, rows), BF),
                pltpu.VMEM((kv, rows, hd), BF),
                pltpu.VMEM((kv, 8, rows), F32),
                pltpu.VMEM((kv, 8, rows), F32),
                pltpu.VMEM((kv, 8, rows), F32),
                pltpu.VMEM((kv, hd, rows), F32),
                pltpu.SemaphoreType.DMA((SLOTS, 2)),
                pltpu.SemaphoreType.DMA((SLOTS, 2)),
            ],
        ),
        out_shape=[jax.ShapeDtypeStruct((n_seq * toks, q_width), BF), cache_shape, cache_shape],
        input_output_aliases={7: 1, 8: 2} if prev else {},
        compiler_params=pltpu.CompilerParams(vmem_limit_bytes=60 * 1024 * 1024, dimension_semantics=("arbitrary",)),
        cost_estimate=pl.CostEstimate(flops=8_000_000_000, bytes_accessed=80_000_000, transcendentals=15_000_000),
        name="attend",
    )(*args)


STEPS = 8
WIDE = STEPS + 2


def exchange_kernel(cfg, *args):
    refs = dict(zip(cfg['names'], args))
    n_seq, toks, d_model = cfg['n_seq'], cfg['toks'], cfg['d_model']
    rows = n_seq * toks
    blk = d_model // STEPS
    me = lax.axis_index('tp')
    core = lax.rem(me, 2)
    partner = me + 1 - 2 * core
    counter = lax.rem(me + 2, 4)
    diag = lax.rem(partner + 2, 4)
    order = (me, partner, counter, diag)
    wbuf, xbuf = refs['wbuf'], refs['xbuf']

    barrier = pltpu.get_barrier_semaphore()
    for peer in (partner, counter):
        pl.semaphore_signal(barrier, inc=1, device_id={'tp': peer}, device_id_type=pl.DeviceIdType.MESH)

    def col(n, width=blk):
        return pl.ds(pl.multiple_of(n * width, width), width)

    def remote(src, dst, send, recv, peer):
        return pltpu.make_async_remote_copy(src_ref=src, dst_ref=dst, send_sem=send, recv_sem=recv, device_id={'tp': peer}, device_id_type=pl.DeviceIdType.MESH)

    def fold(values, total):
        for j in range(blk // 128):
            total = total + values[:, j * 128:(j + 1) * 128]
        return total

    def scatter(tag, a_ref, w_copy, slot_of, depth, ahead, late):
        dsend, drecv, qsend, qrecv, own, part = (refs[k] for k in ('dsend', 'drecv', 'qsend', 'qrecv', 'own', 'part'))
        ds_sem, dr_sem, qs_sem, qr_sem = (refs[tag + k] for k in ('ds', 'dr', 'qs', 'qr'))

        def d_copy(n, i):
            return remote(dsend.at[n, i], drecv.at[n, i], ds_sem.at[n, i], dr_sem.at[n, i], partner)

        def q_copy(n):
            return remote(qsend.at[n], qrecv.at[n], qs_sem.at[n], qr_sem.at[n], counter)

        def step(n, carry):
            @pl.when(n + ahead < STEPS)
            def _():
                w_copy(n + ahead).start()

            w_copy(n).wait()
            cols = col(slot_of(n))
            far = jnp.dot(a_ref[2:4].reshape(2 * rows, depth), wbuf[0:depth, cols], preferred_element_type=F32)
            dsend[n, 0] = far[rows:].astype(BF)
            d_copy(n, 0).start()
            part[...] = far[:rows]
            near = jnp.dot(a_ref[0:2].reshape(2 * rows, depth), wbuf[0:depth, cols], preferred_element_type=F32)
            dsend[n, 1] = near[rows:].astype(BF)
            d_copy(n, 1).start()
            own[n] = near[:rows]
            d_copy(n, 0).wait_recv()
            qsend[n] = (part[...] + drecv[n, 0].astype(F32)).astype(BF)
            q_copy(n).start()
            return carry

        half = STEPS - 3
        lax.fori_loop(0, half, step, 0)
        late(0)
        lax.fori_loop(half, STEPS, step, 0)
        late(1)
        total = jnp.zeros((rows, 128), F32)
        for n in range(STEPS):
            cols = slice(n * blk, (n + 1) * blk)
            d_copy(n, 1).wait_recv()
            q_copy(n).wait_recv()
            summed = own[n] + drecv[n, 1].astype(F32) + qrecv[n].astype(F32)
            fresh = (xbuf[:, cols].astype(F32) + summed.astype(BF).astype(F32)).astype(BF)
            xbuf[:, cols] = fresh
            total = fold(fresh.astype(F32), total)
        for n in range(STEPS):
            d_copy(n, 0).wait_send()
            d_copy(n, 1).wait_send()
            q_copy(n).wait_send()
        return total

    def gather(tag, ln_row, total, w_at, n_out, ready, finish):
        near_h, far_h, acc = refs['near_h'], refs['far_h'], refs['acc']
        cs, cr, fs, fr, ps, pr = (refs[tag + k] for k in ('cs', 'cr', 'fs', 'fr', 'ps', 'pr'))
        mean = jnp.sum(total, axis=-1, keepdims=True) / d_model
        total = jnp.zeros((rows, 128), F32)
        for n in range(STEPS):
            diff = xbuf[:, n * blk:(n + 1) * blk].astype(F32) - mean
            total = fold(diff * diff, total)
        inv = lax.rsqrt(jnp.sum(total, axis=-1, keepdims=True) / d_model + LN_EPS)

        def c_copy(k):
            return remote(near_h.at[pl.ds(0, rows), col(k)], far_h.at[pl.ds(0, rows), col(k)], cs.at[k], cr.at[k], counter)

        def f_copy(k):
            return remote(far_h.at[pl.ds(0, rows), col(k)], far_h.at[pl.ds(rows, rows), col(k)], fs.at[k], fr.at[k], partner)

        def p_copy(k):
            return remote(near_h.at[pl.ds(0, rows), col(k)], near_h.at[pl.ds(rows, rows), col(k)], ps.at[k], pr.at[k], partner)

        for k in range(STEPS):
            cols = slice(k * blk, (k + 1) * blk)
            gain = refs['ln_gain'][ln_row // 2, ln_row % 2:ln_row % 2 + 1, cols].astype(F32)
            bias = refs['ln_bias'][ln_row // 2, ln_row % 2:ln_row % 2 + 1, cols].astype(F32)
            normed = (xbuf[:, cols].astype(F32) - mean) * inv
            near_h[0:rows, cols] = (normed * (1.0 + gain) + bias).astype(BF)
            if k:
                c_copy(k - 1).start()
                p_copy(k - 1).start()
        acc[:, 0:n_out] = jnp.zeros((2 * rows, n_out), F32)
        c_copy(STEPS - 1).start()
        p_copy(STEPS - 1).start()
        ready()
        for k in range(STEPS):
            p_copy(k).wait_recv()

        n_blk = n_out // STEPS
        piece = min(1024, n_out)

        def far_dot(k, cols):
            return jnp.dot(far_h[:, col(k)], wbuf[col(k), w_at + cols.start:w_at + cols.stop], preferred_element_type=F32)

        def near_step(i):
            at = pl.ds(pl.multiple_of(w_at + i * n_blk, n_blk), n_blk)
            finish(0, col(i, n_blk), jnp.dot(near_h[...], wbuf[:, at], preferred_element_type=F32), [i])
            c_copy(i).wait_recv()
            f_copy(i).start()

        def step(i, carry):
            near_step(i)
            f_copy(i - 1).wait_recv()
            for n in range(n_out // piece):
                cols = slice(n * piece, (n + 1) * piece)
                acc[:, cols] += far_dot(i - 1, cols)
            return carry

        near_step(0)
        lax.fori_loop(1, STEPS, step, 0)
        f_copy(STEPS - 1).wait_recv()
        for n in range(n_out // piece):
            cols = slice(n * piece, (n + 1) * piece)
            finish(2, cols, acc[:, cols] + far_dot(STEPS - 1, cols), range(n * piece // n_blk, (n + 1) * piece // n_blk))
        for k in range(STEPS):
            c_copy(k).wait_send()
            p_copy(k).wait_send()
            f_copy(k).wait_send()

    def split(value):
        return value.reshape(2, n_seq, toks, value.shape[-1])

    def gather_qkv(layer, total, w_at, start_now):
        stage, y_out = refs['stage'], refs['y_out']
        n_out = y_out.shape[3]
        n_blk = n_out // STEPS

        def y_copy(g, n):
            return pltpu.make_async_copy(stage.at[g, :, :, col(n, n_blk)], y_out.at[:, order[g], :, col(n, n_blk)], refs['y_sem'].at[g, n])

        def ready():
            if start_now:
                tabs = refs['tabs']

                def table(b, carry):
                    for i, part in enumerate(rope_tables(refs['start'][b], tabs.shape[2], tabs.shape[3])):
                        tabs[i, b] = part
                    return carry

                lax.fori_loop(0, n_seq, table, 0)
                tab_copy.start()
            for copy in qkv_copies(layer, w_at):
                copy.wait()

        def finish(g, cols, value, blocks):
            stage[g:g + 2, :, :, cols] = split(value)
            for n in blocks:
                y_copy(g, n).start()
                y_copy(g + 1, n).start()

        if start_now:
            tab_copy = pltpu.make_async_copy(refs['tabs'], refs['tab_out'], refs['tab_sem'])
        gather('g2', 2 * layer, total, w_at, n_out, ready, finish)
        if start_now:
            tab_copy.wait()
        for g in range(4):
            for n in range(STEPS):
                y_copy(g, n).wait()

    def qkv_copies(layer, w_at):
        copies = []
        for i, name in enumerate(('w_q', 'w_k', 'w_v')):
            width = refs[name].shape[2]
            copies.append(pltpu.make_async_copy(refs[name].at[layer], wbuf.at[:, pl.ds(w_at, width)], refs['gw_sem'].at[i]))
            w_at += width
        return copies

    x_copy = pltpu.make_async_copy(refs['x_hbm'], xbuf, refs['x_sem'])
    if cfg['first']:
        x_copy.start()
        x_copy.wait()
        for copy in qkv_copies(0, 0):
            copy.start()
        total = jnp.zeros((rows, 128), F32)
        for n in range(STEPS):
            total = fold(xbuf[:, n * blk:(n + 1) * blk].astype(F32), total)
        pl.semaphore_wait(barrier, 2)
        gather_qkv(0, total, 0, True)
        return

    layer = cfg['layer']
    abuf, act = refs['abuf'], refs['act']
    depth = abuf.shape[3]
    a_copies = [pltpu.make_async_copy(refs['a_hbm'].at[:, order[g]], abuf.at[g], refs['a_sem'].at[g]) for g in range(4)]

    def o_copy(n):
        return pltpu.make_async_copy(refs['w_o'].at[layer, :, col(n)], wbuf.at[pl.ds(0, depth), col(n)], refs['ow_sem'].at[n])

    def up_copy(i):
        span = pl.ds(0, depth) if i else pl.ds(depth, d_model - depth)
        return pltpu.make_async_copy(refs['w_up'].at[layer, span, :], wbuf.at[span, pl.ds(0, d_model)], refs['uw_sem'].at[i])

    def down_slot(n):
        return lax.rem(n + STEPS, WIDE)

    def down_copy(n):
        return pltpu.make_async_copy(refs['w_down'].at[layer, :, col(n)], wbuf.at[:, col(down_slot(n))], refs['dw_sem'].at[n])

    for g in (2, 3):
        a_copies[g].start()
    o_copy(0).start()
    for g in (0, 1):
        a_copies[g].start()
    o_copy(1).start()
    o_copy(2).start()
    x_copy.start()
    pl.semaphore_wait(barrier, 2)
    for copy in a_copies:
        copy.wait()

    def late_up(i):
        up_copy(i).start()
        if i:
            x_copy.wait()

    total = scatter('s1', abuf, o_copy, lambda n: n, depth, 3, late_up)

    def ready_up():
        for i in range(2):
            up_copy(i).wait()
        for n in range(WIDE - STEPS):
            down_copy(n).start()

    def finish_up(g, cols, value, blocks):
        act[g:g + 2, :, :, cols] = split(jnp.square(jnp.maximum(value, 0.0)).astype(BF))

    gather('g1', 2 * layer + 1, total, 0, d_model, ready_up, finish_up)

    w_at = (WIDE * blk) - (4 * blk)

    def late_qkv(i):
        if i == 0 and cfg['more']:
            for copy in qkv_copies(layer + 1, w_at):
                copy.start()

    total = scatter('s2', act, down_copy, down_slot, d_model, WIDE - STEPS, late_qkv)
    out_copy = pltpu.make_async_copy(xbuf, refs['x_out'], refs['x_sem'])
    out_copy.start()
    if cfg['more']:
        gather_qkv(layer + 1, total, w_at, False)
    out_copy.wait()


def exchange(cid, x, ln_gain, ln_bias, qkv_weights, *, n_seq, layer=-1, more=True, a=None, weights=(), start_pos=None, head_dim=0):
    rows, d_model = x.shape
    toks = rows // n_seq
    blk = d_model // STEPS
    first = a is None
    any_spec, vmem = pl.BlockSpec(memory_space=pl.ANY), pl.BlockSpec(memory_space=pltpu.VMEM)
    dma = pltpu.SemaphoreType.DMA
    ins = [('x_hbm', x, any_spec), ('ln_gain', ln_gain, vmem), ('ln_bias', ln_bias, vmem)]
    outs = []
    qkv_out = sum(w.shape[2] for w in qkv_weights)
    width = qkv_out if first else WIDE * blk
    scr = [('wbuf', pltpu.VMEM((d_model, width), BF)), ('xbuf', pltpu.VMEM((rows, d_model), BF)), ('x_sem', dma)]
    scr += [
        ('near_h', pltpu.VMEM((2 * rows, d_model), BF)), ('far_h', pltpu.VMEM((2 * rows, d_model), BF)),
        ('acc', pltpu.VMEM((2 * rows, qkv_out if first else d_model), F32)),
    ]
    gather_tags, flops, moved = [], 0, 4_000_000
    if not first:
        w_o, w_up, w_down = weights
        depth = a.shape[3]
        ins += [('a_hbm', a, any_spec), ('w_o', w_o, any_spec), ('w_up', w_up, any_spec), ('w_down', w_down, any_spec)]
        outs += [('x_out', jax.ShapeDtypeStruct(x.shape, BF))]
        scr += [
            ('abuf', pltpu.VMEM((4, n_seq, toks, depth), BF)), ('act', pltpu.VMEM((4, n_seq, toks, d_model), BF)),
            ('dsend', pltpu.VMEM((STEPS, 2, rows, blk), BF)), ('drecv', pltpu.VMEM((STEPS, 2, rows, blk), BF)),
            ('qsend', pltpu.VMEM((STEPS, rows, blk), BF)), ('qrecv', pltpu.VMEM((STEPS, rows, blk), BF)),
            ('own', pltpu.VMEM((STEPS, rows, blk), F32)), ('part', pltpu.VMEM((rows, blk), F32)),
            ('a_sem', dma((4,))), ('ow_sem', dma((STEPS,))), ('uw_sem', dma((2,))), ('dw_sem', dma((STEPS,))),
        ]
        for tag in ('s1', 's2'):
            scr += [(tag + k, dma((STEPS, 2))) for k in ('ds', 'dr')] + [(tag + k, dma((STEPS,))) for k in ('qs', 'qr')]
        gather_tags.append('g1')
        flops += 2 * 4 * rows * d_model * (depth + 2 * d_model)
        moved += 2 * d_model * (depth + 2 * d_model)
    if more:
        ins += list(zip(('w_q', 'w_k', 'w_v'), qkv_weights, [any_spec] * 3))
        outs += [('y_out', jax.ShapeDtypeStruct((n_seq, 4, toks, qkv_out), F32))]
        scr += [('stage', pltpu.VMEM((4, n_seq, toks, qkv_out), F32)), ('gw_sem', dma((3,))), ('y_sem', dma((4, STEPS)))]
        gather_tags.append('g2')
        flops += 2 * 4 * rows * d_model * qkv_out
        moved += 2 * d_model * qkv_out
    if first:
        tab_shape = (3, n_seq, 4 * toks, head_dim)
        ins += [('start', start_pos, pl.BlockSpec(memory_space=pltpu.SMEM))]
        outs += [('tab_out', jax.ShapeDtypeStruct(tab_shape, F32))]
        scr += [('tabs', pltpu.VMEM(tab_shape, F32)), ('tab_sem', dma)]
    for tag in gather_tags:
        scr += [(tag + k, dma((STEPS,))) for k in ('cs', 'cr', 'fs', 'fr', 'ps', 'pr')]
    cfg = dict(names=[i[0] for i in ins] + [o[0] for o in outs] + [s[0] for s in scr], layer=layer, first=first, more=more, n_seq=n_seq, toks=toks, d_model=d_model)
    return pl.pallas_call(
        functools.partial(exchange_kernel, cfg),
        in_specs=[i[2] for i in ins],
        out_specs=[any_spec] * len(outs),
        out_shape=[o[1] for o in outs],
        scratch_shapes=[s[1] for s in scr],
        compiler_params=pltpu.CompilerParams(collective_id=cid, has_side_effects=True, vmem_limit_bytes=67_000_000),
        cost_estimate=pl.CostEstimate(flops=flops, bytes_accessed=moved, transcendentals=0),
        name='gather_first' if first else 'block' if more else 'block_last',
    )(*[i[1] for i in ins])


def solution(mesh):
    tok_spec = P('dp', 'tp', None)
    cache_spec = P(None, 'dp', 'tp', None, None)
    col_spec = P(None, None, 'tp')
    row_spec = P(None, 'tp', None)

    def device_fn(x_loc, start_pos, k_cache, v_cache, w_q, w_k, w_v, w_o, w_up, w_down, ln_gain, ln_bias):
        n_layers = w_q.shape[0]
        n_seq, tok_loc, d_model = x_loc.shape
        new_len = tok_loc * 4
        rows = n_seq * new_len
        hidden = x_loc.reshape(n_seq * tok_loc, d_model)
        prev = ()
        qkv_weights = (w_q, w_k, w_v)
        qkv, tabs = exchange(0, hidden, ln_gain, ln_bias, qkv_weights, n_seq=n_seq, start_pos=start_pos, head_dim=k_cache.shape[4])
        for layer in range(n_layers):
            context, *prev = attend(layer, qkv.reshape(rows, -1), tabs, start_pos, k_cache, v_cache, prev)
            context = context.reshape(n_seq, 4, tok_loc, -1)
            outs = exchange(layer + 1, hidden, ln_gain, ln_bias, qkv_weights, n_seq=n_seq, layer=layer, more=layer + 1 < n_layers, a=context, weights=(w_o, w_up, w_down))
            hidden, qkv = outs if layer + 1 < n_layers else (outs[0], None)
        return hidden.reshape(x_loc.shape), prev[0], prev[1]

    return jax.shard_map(device_fn, mesh=mesh, in_specs=(tok_spec, P('dp'), cache_spec, cache_spec, col_spec, col_spec, col_spec, row_spec, col_spec, row_spec, P(), P()), out_specs=(tok_spec, cache_spec, cache_spec), check_vma=False)
```

```python
import functools
import math

import jax
import jax.numpy as jnp
from jax import lax
from jax.experimental import pallas as pl
from jax.experimental.pallas import tpu as pltpu
from jax.sharding import PartitionSpec as P

LN_EPS = 1e-5
ROPE_BASE = 10000.0
NEG_BIG = -1e30
MIN_START = 768
SLOTS = 4
BF = jnp.bfloat16
F32 = jnp.float32


def rope_tables(start, toks, head_dim):
    rot = head_dim // 2
    half = rot // 2
    shape = (toks, head_dim)
    lane = lax.broadcasted_iota(jnp.int32, shape, 1)
    position = start + lax.broadcasted_iota(jnp.int32, shape, 0)
    power = lax.rem(lane, half).astype(F32) * (2.0 / rot)
    angles = position.astype(F32) * jnp.exp(power * -math.log(ROPE_BASE))
    cos_a, sin_a = jnp.cos(angles), jnp.sin(angles)
    upper = jnp.logical_and(lane >= half, lane < rot)
    return jnp.where(lane < rot, cos_a, 1.0), jnp.where(upper, sin_a, 0.0), jnp.where(lane < half, -sin_a, 0.0)


def attn_kernel(layer, dims, start_ref, q_ref, k_ref, v_ref, tab_ref, kc_hbm, vc_hbm, *rest):
    kv, group, toks, hd, s_len, ch = dims
    if layer > 0:
        rest = rest[2:]
    ctx_ref, ko_hbm, vo_hbm, kbuf, vbuf, sbuf, ebuf, qbuf, mbuf, pbuf, lbuf, abuf, in_sem, out_sem = rest
    b = pl.program_id(0)
    nb = pl.num_programs(0) - 1
    s_pad = kbuf.shape[2]
    win = toks + 16
    rows = group * toks
    coef = (hd ** -0.5) * math.log2(math.e)
    slot = lax.rem(b, SLOTS)
    before = lax.rem(b + SLOTS - 1, SLOTS)

    def load(bb):
        sl = lax.rem(bb, SLOTS)
        return [pltpu.make_async_copy(src.at[layer, bb], dst.at[sl, :, pl.ds(0, s_len), :], in_sem.at[sl, i]) for i, (src, dst) in enumerate(((kc_hbm, kbuf), (vc_hbm, vbuf)))]

    def save(bb):
        sl = lax.rem(bb, SLOTS)
        return [pltpu.make_async_copy(src.at[sl, :, pl.ds(0, s_len), :], dst.at[layer, bb], out_sem.at[sl, i]) for i, (src, dst) in enumerate(((kbuf, ko_hbm), (vbuf, vo_hbm)))]

    def run(copies, go):
        for copy in copies:
            copy.start() if go else copy.wait()

    @pl.when(b == 0)
    def _():
        run(load(b), True)
        if s_pad > s_len:
            for sl in range(SLOTS):
                kbuf[sl, :, s_len:, :] = jnp.zeros((kv, s_pad - s_len, hd), BF)
                vbuf[sl, :, s_len:, :] = jnp.zeros((kv, s_pad - s_len, hd), BF)

    @pl.when(b >= 2)
    def _():
        run(save(b - 2), False)

    @pl.when(jnp.logical_and(b > 0, b + 2 < nb))
    def _():
        run(load(b + 2), True)

    start = start_ref[jnp.minimum(b, nb - 1)]
    start_before = start_ref[jnp.maximum(b - 1, 0)]
    half = hd // 4

    def rope(x):
        return x * tab_ref[0, 0] + pltpu.roll(x, half, 1) * tab_ref[1, 0] + pltpu.roll(x, hd - half, 1) * tab_ref[2, 0]

    def patch():
        base = jnp.minimum((start // 16) * 16, s_len - win)
        shift = start - base
        base = pl.multiple_of(base, 16)
        row_id = lax.broadcasted_iota(jnp.int32, (win, hd), 0)
        is_new = jnp.logical_and(row_id >= shift, row_id < shift + toks)
        run(load(b), False)

        @pl.when(b == 0)
        def _():
            run(load(b + 1), True)
            run(load(b + 2), True)

        for h in range(kv):
            cols = slice(h * hd, (h + 1) * hd)
            for buf, fresh in ((kbuf, rope(k_ref[:, cols])), (vbuf, v_ref[:, cols])):
                fresh = fresh.astype(BF).astype(F32)
                fresh = jnp.concatenate([fresh, jnp.zeros((16, hd), F32)], axis=0)
                fresh = pltpu.roll(fresh, shift, 0)
                old = buf[slot, h, pl.ds(base, win), :].astype(F32)
                buf[slot, h, pl.ds(base, win), :] = jnp.where(is_new, fresh, old).astype(BF)
        run(save(b), True)

    step_rows = 64
    blocks = [slice(r, r + step_rows) for r in range(0, ch, step_rows)]

    def chunk(j):
        return pl.ds(pl.multiple_of(j * ch, ch), ch)

    def score(h, j, masked):
        s = lax.dot_general(kbuf[slot, h, chunk(j), :], qbuf[h], (((1,), (1,)), ((), ())), preferred_element_type=F32)
        if masked:
            ahead = lax.broadcasted_iota(jnp.int32, (ch, rows), 0) - lax.rem(lax.broadcasted_iota(jnp.int32, (ch, rows), 1), toks)
            s = jnp.where(ahead <= start - j * ch, s, NEG_BIG)
        sbuf[h] = s

    def scored(h, rb):
        return sbuf[h, rb].reshape(step_rows // 8, 8, rows)

    def peaks(h, peak):
        top = jnp.max(scored(h, blocks[0]), axis=0)
        for rb in blocks[1:]:
            top = jnp.maximum(top, jnp.max(scored(h, rb), axis=0))
        mbuf[h] = peak
        pbuf[h] = jnp.maximum(peak, jnp.max(top, axis=0, keepdims=True))

    def weigh(h):
        peak = pbuf[h]
        alpha = jnp.exp2((mbuf[h] - peak) * coef)
        total = lbuf[h] * alpha
        for rb in blocks:
            e = jnp.exp2((scored(h, rb) - peak) * coef)
            total = total + jnp.sum(e, axis=0)
            ebuf[h, rb] = e.reshape(step_rows, rows).astype(BF)
        return alpha, total

    def mix(h, sl, j, alpha):
        fresh = lax.dot_general(vbuf[sl, h, chunk(j), :], ebuf[h], (((0,), (0,)), ((), ())), preferred_element_type=F32)
        return (abuf[h].reshape(hd // 8, 8, rows) * alpha).reshape(hd, rows) + fresh

    def step(masked_next, j, carry):
        for h in range(kv):
            alpha, lbuf[h] = weigh(h)
            score(h, j + 1, masked_next)
            abuf[h] = mix(h, slot, j, alpha)
        for h in range(kv):
            peaks(h, pbuf[h])
        return carry

    def last_of(bb_start):
        return (bb_start + toks + ch - 1) // ch - 1

    def turn(close, open_next):
        if open_next:
            for h in range(kv):
                for g in range(group):
                    j = h * group + g
                    qbuf[h, g * toks:(g + 1) * toks, :] = rope(q_ref[:, j * hd:(j + 1) * hd]).astype(BF)
            patch()
        for h in range(kv):
            if close:
                alpha, total = weigh(h)
            if open_next:
                score(h, 0, ch > MIN_START)
            if close:
                ctx = (mix(h, before, last_of(start_before), alpha) / jnp.sum(total, axis=0, keepdims=True)).T.astype(BF)
                for g in range(group):
                    j = h * group + g
                    ctx_ref[:, j * hd:(j + 1) * hd] = ctx[g * toks:(g + 1) * toks, :]
        if open_next:
            for h in range(kv):
                peaks(h, jnp.full((8, rows), NEG_BIG, F32))
                lbuf[h] = jnp.zeros((8, rows), F32)
                abuf[h] = jnp.zeros((hd, rows), F32)

    pl.when(b == 0)(functools.partial(turn, False, True))
    pl.when(jnp.logical_and(b > 0, b < nb))(functools.partial(turn, True, True))
    pl.when(b == nb)(functools.partial(turn, True, False))

    @pl.when(b < nb)
    def _():
        n_full = jnp.maximum(start // ch, 1)
        lax.fori_loop(0, n_full - 1, functools.partial(step, False), 0)
        lax.fori_loop(n_full - 1, last_of(start), functools.partial(step, True), 0)

    @pl.when(b == nb)
    def _():
        run(save(b - 1), False)


def attend(layer, qkv, tabs, start_pos, k_cache, v_cache, prev):
    n_seq = start_pos.shape[0]
    _, _, kv, s_len, hd = k_cache.shape
    toks = qkv.shape[0] // n_seq
    kv_width = kv * hd
    q_width = qkv.shape[1] - 2 * kv_width
    group = q_width // kv_width
    n_ch = -(-s_len // 640)
    ch = 128 * -(-s_len // (128 * n_ch))
    rows = group * toks
    dims = (kv, group, toks, hd, s_len, ch)
    any_spec = pl.BlockSpec(memory_space=pl.ANY)
    now = lambda b: jnp.minimum(b, n_seq - 1)
    tab_spec = pl.BlockSpec((3, 1, toks, hd), lambda b, *_: (0, now(b), 0, 0))
    cache_shape = jax.ShapeDtypeStruct(k_cache.shape, BF)
    args = [start_pos, qkv, qkv, qkv, tabs, k_cache, v_cache] + list(prev)
    return pl.pallas_call(
        functools.partial(attn_kernel, layer, dims),
        grid_spec=pltpu.PrefetchScalarGridSpec(
            num_scalar_prefetch=1,
            grid=(n_seq + 1,),
            in_specs=[
                pl.BlockSpec((toks, q_width), lambda b, *_: (now(b), 0)),
                pl.BlockSpec((toks, kv_width), lambda b, *_: (now(b), group)),
                pl.BlockSpec((toks, kv_width), lambda b, *_: (now(b), group + 1)),
                tab_spec,
            ] + [any_spec] * (2 + len(prev)),
            out_specs=[pl.BlockSpec((toks, q_width), lambda b, *_: (jnp.maximum(b - 1, 0), 0)), any_spec, any_spec],
            scratch_shapes=[
                pltpu.VMEM((SLOTS, kv, ch * n_ch, hd), BF),
                pltpu.VMEM((SLOTS, kv, ch * n_ch, hd), BF),
                pltpu.VMEM((kv, ch, rows), F32),
                pltpu.VMEM((kv, ch, rows), BF),
                pltpu.VMEM((kv, rows, hd), BF),
                pltpu.VMEM((kv, 8, rows), F32),
                pltpu.VMEM((kv, 8, rows), F32),
                pltpu.VMEM((kv, 8, rows), F32),
                pltpu.VMEM((kv, hd, rows), F32),
                pltpu.SemaphoreType.DMA((SLOTS, 2)),
                pltpu.SemaphoreType.DMA((SLOTS, 2)),
            ],
        ),
        out_shape=[jax.ShapeDtypeStruct((n_seq * toks, q_width), BF), cache_shape, cache_shape],
        input_output_aliases={7: 1, 8: 2} if prev else {},
        compiler_params=pltpu.CompilerParams(vmem_limit_bytes=60 * 1024 * 1024, dimension_semantics=("arbitrary",)),
        cost_estimate=pl.CostEstimate(flops=8_000_000_000, bytes_accessed=80_000_000, transcendentals=15_000_000),
        name="attend",
    )(*args)


STEPS = 8
WIDE = STEPS + 2


def exchange_kernel(cfg, *args):
    refs = dict(zip(cfg['names'], args))
    n_seq, toks, d_model = cfg['n_seq'], cfg['toks'], cfg['d_model']
    rows = n_seq * toks
    blk = d_model // STEPS
    me = lax.axis_index('tp')
    core = lax.rem(me, 2)
    partner = me + 1 - 2 * core
    counter = lax.rem(me + 2, 4)
    diag = lax.rem(partner + 2, 4)
    order = (me, partner, counter, diag)
    wbuf, xbuf = refs['wbuf'], refs['xbuf']

    barrier = pltpu.get_barrier_semaphore()
    for peer in (partner, counter):
        pl.semaphore_signal(barrier, inc=1, device_id={'tp': peer}, device_id_type=pl.DeviceIdType.MESH)

    def col(n, width=blk):
        return pl.ds(pl.multiple_of(n * width, width), width)

    def remote(src, dst, send, recv, peer):
        return pltpu.make_async_remote_copy(src_ref=src, dst_ref=dst, send_sem=send, recv_sem=recv, device_id={'tp': peer}, device_id_type=pl.DeviceIdType.MESH)

    def fold(values, total):
        for j in range(blk // 128):
            total = total + values[:, j * 128:(j + 1) * 128]
        return total

    def scatter(tag, a_ref, w_copy, slot_of, depth, ahead, late, near_ready=()):
        dsend, drecv, qsend, qrecv, own, part = (refs[k] for k in ('dsend', 'drecv', 'qsend', 'qrecv', 'own', 'part'))
        ds_sem, dr_sem, qs_sem, qr_sem = (refs[tag + k] for k in ('ds', 'dr', 'qs', 'qr'))

        def d_copy(n, i):
            return remote(dsend.at[n, i], drecv.at[n, i], ds_sem.at[n, i], dr_sem.at[n, i], partner)

        def q_copy(n):
            return remote(qsend.at[n], qrecv.at[n], qs_sem.at[n], qr_sem.at[n], counter)

        def step(n, carry):
            @pl.when(n + ahead < STEPS)
            def _():
                w_copy(n + ahead).start()

            w_copy(n).wait()
            cols = col(slot_of(n))
            far = jnp.dot(a_ref[2:4].reshape(2 * rows, depth), wbuf[0:depth, cols], preferred_element_type=F32)
            dsend[n, 0] = far[rows:].astype(BF)
            d_copy(n, 0).start()
            part[...] = far[:rows]
            if near_ready:
                @pl.when(n == 0)
                def _():
                    for copy in near_ready:
                        copy.wait()

            near = jnp.dot(a_ref[0:2].reshape(2 * rows, depth), wbuf[0:depth, cols], preferred_element_type=F32)
            dsend[n, 1] = near[rows:].astype(BF)
            d_copy(n, 1).start()
            own[n] = near[:rows]
            d_copy(n, 0).wait_recv()
            qsend[n] = (part[...] + drecv[n, 0].astype(F32)).astype(BF)
            q_copy(n).start()
            return carry

        half = STEPS - ahead
        lax.fori_loop(0, half, step, 0)
        late(0)
        lax.fori_loop(half, STEPS, step, 0)
        late(1)
        total = jnp.zeros((rows, 128), F32)
        for n in range(STEPS):
            cols = slice(n * blk, (n + 1) * blk)
            d_copy(n, 1).wait_recv()
            q_copy(n).wait_recv()
            summed = own[n] + drecv[n, 1].astype(F32) + qrecv[n].astype(F32)
            fresh = (xbuf[:, cols].astype(F32) + summed.astype(BF).astype(F32)).astype(BF)
            xbuf[:, cols] = fresh
            total = fold(fresh.astype(F32), total)
        for n in range(STEPS):
            d_copy(n, 0).wait_send()
            d_copy(n, 1).wait_send()
            q_copy(n).wait_send()
        return total

    def gather(tag, ln_row, total, w_at, n_out, ready, finish):
        near_h, far_h, acc = refs['near_h'], refs['far_h'], refs['acc']
        cs, cr, fs, fr, ps, pr = (refs[tag + k] for k in ('cs', 'cr', 'fs', 'fr', 'ps', 'pr'))
        mean = jnp.sum(total, axis=-1, keepdims=True) / d_model
        total = jnp.zeros((rows, 128), F32)
        for n in range(STEPS):
            diff = xbuf[:, n * blk:(n + 1) * blk].astype(F32) - mean
            total = fold(diff * diff, total)
        inv = lax.rsqrt(jnp.sum(total, axis=-1, keepdims=True) / d_model + LN_EPS)

        chunk = blk // 2

        def c_copy(k):
            return remote(near_h.at[pl.ds(0, rows), col(k, chunk)], far_h.at[pl.ds(0, rows), col(k, chunk)], cs.at[k], cr.at[k], counter)

        def f_copy(k):
            return remote(far_h.at[pl.ds(0, rows), col(k, chunk)], far_h.at[pl.ds(rows, rows), col(k, chunk)], fs.at[k], fr.at[k], partner)

        def p_copy(k):
            return remote(near_h.at[pl.ds(0, rows), col(k)], near_h.at[pl.ds(rows, rows), col(k)], ps.at[k], pr.at[k], partner)

        for k in range(STEPS):
            cols = slice(k * blk, (k + 1) * blk)
            gain = refs['ln_gain'][ln_row // 2, ln_row % 2:ln_row % 2 + 1, cols].astype(F32)
            bias = refs['ln_bias'][ln_row // 2, ln_row % 2:ln_row % 2 + 1, cols].astype(F32)
            normed = (xbuf[:, cols].astype(F32) - mean) * inv
            near_h[0:rows, cols] = (normed * (1.0 + gain) + bias).astype(BF)
            if k:
                c_copy(2 * k - 2).start()
                c_copy(2 * k - 1).start()
                p_copy(k - 1).start()
        acc[:, 0:n_out] = jnp.zeros((2 * rows, n_out), F32)
        c_copy(2 * STEPS - 2).start()
        c_copy(2 * STEPS - 1).start()
        p_copy(STEPS - 1).start()
        ready()
        for k in range(STEPS):
            p_copy(k).wait_recv()

        n_blk = n_out // STEPS
        piece = min(1024, n_out)

        def far_dot(k, width, cols):
            return jnp.dot(far_h[:, col(k, width)], wbuf[col(k, width), w_at + cols.start:w_at + cols.stop], preferred_element_type=F32)

        pieces = [slice(n, n + piece) for n in range(0, n_out, piece)]

        def far_step(k, width):
            for cols in pieces:
                acc[:, cols] += far_dot(k, width, cols)

        def pass_on(k):
            c_copy(k).wait_recv()
            f_copy(k).start()

        def near_step(i):
            at = pl.ds(pl.multiple_of(w_at + i * n_blk, n_blk), n_blk)
            finish(0, col(i, n_blk), jnp.dot(near_h[...], wbuf[:, at], preferred_element_type=F32), [i])
            pass_on(2 * i)

        def step(i, carry):
            near_step(i)
            f_copy(2 * i - 2).wait_recv()
            f_copy(2 * i - 1).wait_recv()
            far_step(i - 1, blk)
            pass_on(2 * i + 1)
            return carry

        near_step(0)
        pass_on(1)
        lax.fori_loop(1, STEPS, step, 0)
        f_copy(2 * STEPS - 2).wait_recv()
        far_step(2 * STEPS - 2, chunk)
        f_copy(2 * STEPS - 1).wait_recv()
        for cols in pieces:
            finish(2, cols, acc[:, cols] + far_dot(2 * STEPS - 1, chunk, cols), range(cols.start // n_blk, cols.stop // n_blk))
        for k in range(STEPS):
            p_copy(k).wait_send()
        for k in range(2 * STEPS):
            c_copy(k).wait_send()
            f_copy(k).wait_send()

    def split(value):
        return value.reshape(2, n_seq, toks, value.shape[-1])

    def gather_qkv(layer, total, w_at, start_now):
        stage, y_out = refs['stage'], refs['y_out']
        n_out = y_out.shape[3]
        n_blk = n_out // STEPS

        def y_copy(g, n):
            return pltpu.make_async_copy(stage.at[g, :, :, col(n, n_blk)], y_out.at[:, order[g], :, col(n, n_blk)], refs['y_sem'].at[g, n])

        def ready():
            if start_now:
                tabs = refs['tabs']

                def table(b, carry):
                    for i, part in enumerate(rope_tables(refs['start'][b], tabs.shape[2], tabs.shape[3])):
                        tabs[i, b] = part
                    return carry

                lax.fori_loop(0, n_seq, table, 0)
                tab_copy.start()
            for copy in qkv_copies(layer, w_at):
                copy.wait()

        def finish(g, cols, value, blocks):
            stage[g:g + 2, :, :, cols] = split(value)
            for n in blocks:
                y_copy(g, n).start()
                y_copy(g + 1, n).start()

        if start_now:
            tab_copy = pltpu.make_async_copy(refs['tabs'], refs['tab_out'], refs['tab_sem'])
        gather('g2', 2 * layer, total, w_at, n_out, ready, finish)
        if start_now:
            tab_copy.wait()
        for g in range(4):
            for n in range(STEPS):
                y_copy(g, n).wait()

    def qkv_copies(layer, w_at):
        copies = []
        for i, name in enumerate(('w_q', 'w_k', 'w_v')):
            width = refs[name].shape[2]
            copies.append(pltpu.make_async_copy(refs[name].at[layer], wbuf.at[:, pl.ds(w_at, width)], refs['gw_sem'].at[i]))
            w_at += width
        return copies

    x_copy = pltpu.make_async_copy(refs['x_hbm'], xbuf, refs['x_sem'])
    if cfg['first']:
        x_copy.start()
        x_copy.wait()
        for copy in qkv_copies(0, 0):
            copy.start()
        total = jnp.zeros((rows, 128), F32)
        for n in range(STEPS):
            total = fold(xbuf[:, n * blk:(n + 1) * blk].astype(F32), total)
        pl.semaphore_wait(barrier, 2)
        gather_qkv(0, total, 0, True)
        return

    layer = cfg['layer']
    abuf, act = refs['abuf'], refs['act']
    depth = abuf.shape[3]
    a_copies = [pltpu.make_async_copy(refs['a_hbm'].at[:, order[g]], abuf.at[g], refs['a_sem'].at[g]) for g in range(4)]

    def o_copy(n):
        return pltpu.make_async_copy(refs['w_o'].at[layer, :, col(n)], wbuf.at[pl.ds(0, depth), col(n)], refs['ow_sem'].at[n])

    def up_copy(i):
        span = pl.ds(0, depth) if i else pl.ds(depth, d_model - depth)
        return pltpu.make_async_copy(refs['w_up'].at[layer, span, :], wbuf.at[span, pl.ds(0, d_model)], refs['uw_sem'].at[i])

    def down_slot(n):
        return lax.rem(n + STEPS, WIDE)

    def down_copy(n):
        return pltpu.make_async_copy(refs['w_down'].at[layer, :, col(n)], wbuf.at[:, col(down_slot(n))], refs['dw_sem'].at[n])

    for g in (2, 3):
        a_copies[g].start()
    o_copy(0).start()
    for g in (0, 1):
        a_copies[g].start()
    o_copy(1).start()
    o_copy(2).start()
    x_copy.start()
    pl.semaphore_wait(barrier, 2)
    for copy in a_copies[2:]:
        copy.wait()

    def late_up(i):
        up_copy(i).start()
        if i:
            x_copy.wait()

    total = scatter('s1', abuf, o_copy, lambda n: n, depth, 3, late_up, a_copies[:2])

    def ready_up():
        for i in range(2):
            up_copy(i).wait()
        for n in range(WIDE - STEPS):
            down_copy(n).start()

    def finish_up(g, cols, value, blocks):
        act[g:g + 2, :, :, cols] = split(jnp.square(jnp.maximum(value, 0.0)).astype(BF))

    gather('g1', 2 * layer + 1, total, 0, d_model, ready_up, finish_up)

    w_at = (WIDE * blk) - (4 * blk)

    def late_qkv(i):
        if i == 0 and cfg['more']:
            for copy in qkv_copies(layer + 1, w_at):
                copy.start()

    total = scatter('s2', act, down_copy, down_slot, d_model, WIDE - STEPS, late_qkv)
    out_copy = pltpu.make_async_copy(xbuf, refs['x_out'], refs['x_sem'])
    out_copy.start()
    if cfg['more']:
        gather_qkv(layer + 1, total, w_at, False)
    out_copy.wait()


def exchange(cid, x, ln_gain, ln_bias, qkv_weights, *, n_seq, layer=-1, more=True, a=None, weights=(), start_pos=None, head_dim=0):
    rows, d_model = x.shape
    toks = rows // n_seq
    blk = d_model // STEPS
    first = a is None
    any_spec, vmem = pl.BlockSpec(memory_space=pl.ANY), pl.BlockSpec(memory_space=pltpu.VMEM)
    dma = pltpu.SemaphoreType.DMA
    ins = [('x_hbm', x, any_spec), ('ln_gain', ln_gain, vmem), ('ln_bias', ln_bias, vmem)]
    outs = []
    qkv_out = sum(w.shape[2] for w in qkv_weights)
    width = qkv_out if first else WIDE * blk
    scr = [('wbuf', pltpu.VMEM((d_model, width), BF)), ('xbuf', pltpu.VMEM((rows, d_model), BF)), ('x_sem', dma)]
    scr += [
        ('near_h', pltpu.VMEM((2 * rows, d_model), BF)), ('far_h', pltpu.VMEM((2 * rows, d_model), BF)),
        ('acc', pltpu.VMEM((2 * rows, qkv_out if first else d_model), F32)),
    ]
    gather_tags, flops, moved = [], 0, 4_000_000
    if not first:
        w_o, w_up, w_down = weights
        depth = a.shape[3]
        ins += [('a_hbm', a, any_spec), ('w_o', w_o, any_spec), ('w_up', w_up, any_spec), ('w_down', w_down, any_spec)]
        outs += [('x_out', jax.ShapeDtypeStruct(x.shape, BF))]
        scr += [
            ('abuf', pltpu.VMEM((4, n_seq, toks, depth), BF)), ('act', pltpu.VMEM((4, n_seq, toks, d_model), BF)),
            ('dsend', pltpu.VMEM((STEPS, 2, rows, blk), BF)), ('drecv', pltpu.VMEM((STEPS, 2, rows, blk), BF)),
            ('qsend', pltpu.VMEM((STEPS, rows, blk), BF)), ('qrecv', pltpu.VMEM((STEPS, rows, blk), BF)),
            ('own', pltpu.VMEM((STEPS, rows, blk), F32)), ('part', pltpu.VMEM((rows, blk), F32)),
            ('a_sem', dma((4,))), ('ow_sem', dma((STEPS,))), ('uw_sem', dma((2,))), ('dw_sem', dma((STEPS,))),
        ]
        for tag in ('s1', 's2'):
            scr += [(tag + k, dma((STEPS, 2))) for k in ('ds', 'dr')] + [(tag + k, dma((STEPS,))) for k in ('qs', 'qr')]
        gather_tags.append('g1')
        flops += 2 * 4 * rows * d_model * (depth + 2 * d_model)
        moved += 2 * d_model * (depth + 2 * d_model)
    if more:
        ins += list(zip(('w_q', 'w_k', 'w_v'), qkv_weights, [any_spec] * 3))
        outs += [('y_out', jax.ShapeDtypeStruct((n_seq, 4, toks, qkv_out), F32))]
        scr += [('stage', pltpu.VMEM((4, n_seq, toks, qkv_out), F32)), ('gw_sem', dma((3,))), ('y_sem', dma((4, STEPS)))]
        gather_tags.append('g2')
        flops += 2 * 4 * rows * d_model * qkv_out
        moved += 2 * d_model * qkv_out
    if first:
        tab_shape = (3, n_seq, 4 * toks, head_dim)
        ins += [('start', start_pos, pl.BlockSpec(memory_space=pltpu.SMEM))]
        outs += [('tab_out', jax.ShapeDtypeStruct(tab_shape, F32))]
        scr += [('tabs', pltpu.VMEM(tab_shape, F32)), ('tab_sem', dma)]
    for tag in gather_tags:
        scr += [(tag + k, dma((2 * STEPS,))) for k in ('cs', 'cr', 'fs', 'fr')] + [(tag + k, dma((STEPS,))) for k in ('ps', 'pr')]
    cfg = dict(names=[i[0] for i in ins] + [o[0] for o in outs] + [s[0] for s in scr], layer=layer, first=first, more=more, n_seq=n_seq, toks=toks, d_model=d_model)
    return pl.pallas_call(
        functools.partial(exchange_kernel, cfg),
        in_specs=[i[2] for i in ins],
        out_specs=[any_spec] * len(outs),
        out_shape=[o[1] for o in outs],
        scratch_shapes=[s[1] for s in scr],
        compiler_params=pltpu.CompilerParams(collective_id=cid, has_side_effects=True, vmem_limit_bytes=67_000_000),
        cost_estimate=pl.CostEstimate(flops=flops, bytes_accessed=moved, transcendentals=0),
        name='gather_first' if first else 'block' if more else 'block_last',
    )(*[i[1] for i in ins])


def solution(mesh):
    tok_spec = P('dp', 'tp', None)
    cache_spec = P(None, 'dp', 'tp', None, None)
    col_spec = P(None, None, 'tp')
    row_spec = P(None, 'tp', None)

    def device_fn(x_loc, start_pos, k_cache, v_cache, w_q, w_k, w_v, w_o, w_up, w_down, ln_gain, ln_bias):
        n_layers = w_q.shape[0]
        n_seq, tok_loc, d_model = x_loc.shape
        new_len = tok_loc * 4
        rows = n_seq * new_len
        hidden = x_loc.reshape(n_seq * tok_loc, d_model)
        prev = ()
        qkv_weights = (w_q, w_k, w_v)
        qkv, tabs = exchange(0, hidden, ln_gain, ln_bias, qkv_weights, n_seq=n_seq, start_pos=start_pos, head_dim=k_cache.shape[4])
        for layer in range(n_layers):
            context, *prev = attend(layer, qkv.reshape(rows, -1), tabs, start_pos, k_cache, v_cache, prev)
            context = context.reshape(n_seq, 4, tok_loc, -1)
            outs = exchange(layer + 1, hidden, ln_gain, ln_bias, qkv_weights, n_seq=n_seq, layer=layer, more=layer + 1 < n_layers, a=context, weights=(w_o, w_up, w_down))
            hidden, qkv = outs if layer + 1 < n_layers else (outs[0], None)
        return hidden.reshape(x_loc.shape), prev[0], prev[1]

    return jax.shard_map(device_fn, mesh=mesh, in_specs=(tok_spec, P('dp'), cache_spec, cache_spec, col_spec, col_spec, col_spec, row_spec, col_spec, row_spec, P(), P()), out_specs=(tok_spec, cache_spec, cache_spec), check_vma=False)
```

```python
import functools
import math

import jax
import jax.numpy as jnp
from jax import lax
from jax.experimental import pallas as pl
from jax.experimental.pallas import tpu as pltpu
from jax.sharding import PartitionSpec as P

LN_EPS = 1e-5
ROPE_BASE = 10000.0
NEG_BIG = -1e30
MIN_START = 768
SLOTS = 4
BF = jnp.bfloat16
F32 = jnp.float32


def rope_tables(start, toks, head_dim):
    rot = head_dim // 2
    half = rot // 2
    shape = (toks, head_dim)
    lane = lax.broadcasted_iota(jnp.int32, shape, 1)
    position = start + lax.broadcasted_iota(jnp.int32, shape, 0)
    power = lax.rem(lane, half).astype(F32) * (2.0 / rot)
    angles = position.astype(F32) * jnp.exp(power * -math.log(ROPE_BASE))
    cos_a, sin_a = jnp.cos(angles), jnp.sin(angles)
    upper = jnp.logical_and(lane >= half, lane < rot)
    return jnp.where(lane < rot, cos_a, 1.0), jnp.where(upper, sin_a, 0.0), jnp.where(lane < half, -sin_a, 0.0)


def attn_kernel(layer, dims, start_ref, q_ref, k_ref, v_ref, tab_ref, kc_hbm, vc_hbm, *rest):
    kv, group, toks, hd, s_len, ch = dims
    if layer > 0:
        rest = rest[2:]
    ctx_ref, ko_hbm, vo_hbm, kbuf, vbuf, sbuf, ebuf, qbuf, mbuf, pbuf, lbuf, abuf, in_sem, out_sem = rest
    b = pl.program_id(0)
    nb = pl.num_programs(0) - 1
    s_pad = kbuf.shape[2]
    win = toks + 16
    rows = group * toks
    coef = (hd ** -0.5) * math.log2(math.e)
    slot = lax.rem(b, SLOTS)
    before = lax.rem(b + SLOTS - 1, SLOTS)

    def load(bb):
        sl = lax.rem(bb, SLOTS)
        return [pltpu.make_async_copy(src.at[layer, bb], dst.at[sl, :, pl.ds(0, s_len), :], in_sem.at[sl, i]) for i, (src, dst) in enumerate(((kc_hbm, kbuf), (vc_hbm, vbuf)))]

    def save(bb):
        sl = lax.rem(bb, SLOTS)
        return [pltpu.make_async_copy(src.at[sl, :, pl.ds(0, s_len), :], dst.at[layer, bb], out_sem.at[sl, i]) for i, (src, dst) in enumerate(((kbuf, ko_hbm), (vbuf, vo_hbm)))]

    def run(copies, go):
        for copy in copies:
            copy.start() if go else copy.wait()

    @pl.when(b == 0)
    def _():
        run(load(b), True)
        if s_pad > s_len:
            for sl in range(SLOTS):
                kbuf[sl, :, s_len:, :] = jnp.zeros((kv, s_pad - s_len, hd), BF)
                vbuf[sl, :, s_len:, :] = jnp.zeros((kv, s_pad - s_len, hd), BF)

    @pl.when(b >= 2)
    def _():
        run(save(b - 2), False)

    @pl.when(b == 1)
    def _():
        run(load(b + 1), True)

    start = start_ref[jnp.minimum(b, nb - 1)]
    start_before = start_ref[jnp.maximum(b - 1, 0)]
    half = hd // 4

    def rope(x):
        return x * tab_ref[0, 0] + pltpu.roll(x, half, 1) * tab_ref[1, 0] + pltpu.roll(x, hd - half, 1) * tab_ref[2, 0]

    def patch():
        base = jnp.minimum((start // 16) * 16, s_len - win)
        shift = start - base
        base = pl.multiple_of(base, 16)
        row_id = lax.broadcasted_iota(jnp.int32, (win, hd), 0)
        is_new = jnp.logical_and(row_id >= shift, row_id < shift + toks)
        run(load(b), False)

        @pl.when(b == 0)
        def _():
            run(load(b + 1), True)

        @pl.when(jnp.logical_and(b > 0, b + 2 < nb))
        def _():
            run(load(b + 2), True)

        for h in range(kv):
            cols = slice(h * hd, (h + 1) * hd)
            for buf, fresh in ((kbuf, rope(k_ref[:, cols])), (vbuf, v_ref[:, cols])):
                fresh = fresh.astype(BF).astype(F32)
                fresh = jnp.concatenate([fresh, jnp.zeros((16, hd), F32)], axis=0)
                fresh = pltpu.roll(fresh, shift, 0)
                old = buf[slot, h, pl.ds(base, win), :].astype(F32)
                buf[slot, h, pl.ds(base, win), :] = jnp.where(is_new, fresh, old).astype(BF)
        run(save(b), True)

    step_rows = 64
    blocks = [slice(r, r + step_rows) for r in range(0, ch, step_rows)]

    def chunk(j):
        return pl.ds(pl.multiple_of(j * ch, ch), ch)

    def score(h, j, masked):
        s = lax.dot_general(kbuf[slot, h, chunk(j), :], qbuf[h], (((1,), (1,)), ((), ())), preferred_element_type=F32)
        if masked:
            ahead = lax.broadcasted_iota(jnp.int32, (ch, rows), 0) - lax.rem(lax.broadcasted_iota(jnp.int32, (ch, rows), 1), toks)
            s = jnp.where(ahead <= start - j * ch, s, NEG_BIG)
        sbuf[h] = s

    def scored(h, rb):
        return sbuf[h, rb].reshape(step_rows // 8, 8, rows)

    def peaks(h, peak):
        top = jnp.max(scored(h, blocks[0]), axis=0)
        for rb in blocks[1:]:
            top = jnp.maximum(top, jnp.max(scored(h, rb), axis=0))
        mbuf[h] = peak
        pbuf[h] = jnp.maximum(peak, jnp.max(top, axis=0, keepdims=True))

    def weigh(h):
        peak = pbuf[h]
        alpha = jnp.exp2((mbuf[h] - peak) * coef)
        total = lbuf[h] * alpha
        for rb in blocks:
            e = jnp.exp2((scored(h, rb) - peak) * coef)
            total = total + jnp.sum(e, axis=0)
            ebuf[h, rb] = e.reshape(step_rows, rows).astype(BF)
        return alpha, total

    def mix(h, sl, j, alpha):
        fresh = lax.dot_general(vbuf[sl, h, chunk(j), :], ebuf[h], (((0,), (0,)), ((), ())), preferred_element_type=F32)
        return (abuf[h].reshape(hd // 8, 8, rows) * alpha).reshape(hd, rows) + fresh

    def step(masked_next, j, carry):
        for h in range(kv):
            alpha, lbuf[h] = weigh(h)
            score(h, j + 1, masked_next)
            abuf[h] = mix(h, slot, j, alpha)
        for h in range(kv):
            peaks(h, pbuf[h])
        return carry

    def last_of(bb_start):
        return (bb_start + toks + ch - 1) // ch - 1

    def turn(close, open_next):
        if open_next:
            for h in range(kv):
                for g in range(group):
                    j = h * group + g
                    qbuf[h, g * toks:(g + 1) * toks, :] = rope(q_ref[:, j * hd:(j + 1) * hd]).astype(BF)
            patch()
        for h in range(kv):
            if close:
                alpha, total = weigh(h)
            if open_next:
                score(h, 0, ch > MIN_START)
            if close:
                ctx = (mix(h, before, last_of(start_before), alpha) / jnp.sum(total, axis=0, keepdims=True)).T.astype(BF)
                for g in range(group):
                    j = h * group + g
                    ctx_ref[:, j * hd:(j + 1) * hd] = ctx[g * toks:(g + 1) * toks, :]
        if open_next:
            for h in range(kv):
                peaks(h, jnp.full((8, rows), NEG_BIG, F32))
                lbuf[h] = jnp.zeros((8, rows), F32)
                abuf[h] = jnp.zeros((hd, rows), F32)

    pl.when(b == 0)(functools.partial(turn, False, True))
    pl.when(jnp.logical_and(b > 0, b < nb))(functools.partial(turn, True, True))
    pl.when(b == nb)(functools.partial(turn, True, False))

    @pl.when(b < nb)
    def _():
        n_full = jnp.maximum(start // ch, 1)
        lax.fori_loop(0, n_full - 1, functools.partial(step, False), 0)
        lax.fori_loop(n_full - 1, last_of(start), functools.partial(step, True), 0)

    @pl.when(b == nb)
    def _():
        run(save(b - 1), False)


def attend(layer, qkv, tabs, start_pos, k_cache, v_cache, prev):
    n_seq = start_pos.shape[0]
    _, _, kv, s_len, hd = k_cache.shape
    toks = qkv.shape[0] // n_seq
    kv_width = kv * hd
    q_width = qkv.shape[1] - 2 * kv_width
    group = q_width // kv_width
    n_ch = -(-s_len // 640)
    ch = 128 * -(-s_len // (128 * n_ch))
    rows = group * toks
    dims = (kv, group, toks, hd, s_len, ch)
    any_spec = pl.BlockSpec(memory_space=pl.ANY)
    now = lambda b: jnp.minimum(b, n_seq - 1)
    tab_spec = pl.BlockSpec((3, 1, toks, hd), lambda b, *_: (0, now(b), 0, 0))
    cache_shape = jax.ShapeDtypeStruct(k_cache.shape, BF)
    args = [start_pos, qkv, qkv, qkv, tabs, k_cache, v_cache] + list(prev)
    return pl.pallas_call(
        functools.partial(attn_kernel, layer, dims),
        grid_spec=pltpu.PrefetchScalarGridSpec(
            num_scalar_prefetch=1,
            grid=(n_seq + 1,),
            in_specs=[
                pl.BlockSpec((toks, q_width), lambda b, *_: (now(b), 0)),
                pl.BlockSpec((toks, kv_width), lambda b, *_: (now(b), group)),
                pl.BlockSpec((toks, kv_width), lambda b, *_: (now(b), group + 1)),
                tab_spec,
            ] + [any_spec] * (2 + len(prev)),
            out_specs=[pl.BlockSpec((toks, q_width), lambda b, *_: (jnp.maximum(b - 1, 0), 0)), any_spec, any_spec],
            scratch_shapes=[
                pltpu.VMEM((SLOTS, kv, ch * n_ch, hd), BF),
                pltpu.VMEM((SLOTS, kv, ch * n_ch, hd), BF),
                pltpu.VMEM((kv, ch, rows), F32),
                pltpu.VMEM((kv, ch, rows), BF),
                pltpu.VMEM((kv, rows, hd), BF),
                pltpu.VMEM((kv, 8, rows), F32),
                pltpu.VMEM((kv, 8, rows), F32),
                pltpu.VMEM((kv, 8, rows), F32),
                pltpu.VMEM((kv, hd, rows), F32),
                pltpu.SemaphoreType.DMA((SLOTS, 2)),
                pltpu.SemaphoreType.DMA((SLOTS, 2)),
            ],
        ),
        out_shape=[jax.ShapeDtypeStruct((n_seq * toks, q_width), BF), cache_shape, cache_shape],
        input_output_aliases={7: 1, 8: 2} if prev else {},
        compiler_params=pltpu.CompilerParams(vmem_limit_bytes=60 * 1024 * 1024, dimension_semantics=("arbitrary",)),
        cost_estimate=pl.CostEstimate(flops=8_000_000_000, bytes_accessed=80_000_000, transcendentals=15_000_000),
        name="attend",
    )(*args)


STEPS = 8
WIDE = STEPS + 2


def exchange_kernel(cfg, *args):
    refs = dict(zip(cfg['names'], args))
    n_seq, toks, d_model = cfg['n_seq'], cfg['toks'], cfg['d_model']
    rows = n_seq * toks
    blk = d_model // STEPS
    me = lax.axis_index('tp')
    core = lax.rem(me, 2)
    partner = me + 1 - 2 * core
    counter = lax.rem(me + 2, 4)
    diag = lax.rem(partner + 2, 4)
    order = (me, partner, counter, diag)
    wbuf, xbuf = refs['wbuf'], refs['xbuf']

    barrier = pltpu.get_barrier_semaphore()
    for peer in (partner, counter):
        pl.semaphore_signal(barrier, inc=1, device_id={'tp': peer}, device_id_type=pl.DeviceIdType.MESH)

    def col(n, width=blk):
        return pl.ds(pl.multiple_of(n * width, width), width)

    def remote(src, dst, send, recv, peer):
        return pltpu.make_async_remote_copy(src_ref=src, dst_ref=dst, send_sem=send, recv_sem=recv, device_id={'tp': peer}, device_id_type=pl.DeviceIdType.MESH)

    def fold(values, total):
        for j in range(blk // 128):
            total = total + values[:, j * 128:(j + 1) * 128]
        return total

    def moments(values, state):
        zero = jnp.zeros((rows, 128), F32)
        if state is None:
            state = (jnp.sum(fold(values, zero), axis=-1, keepdims=True) / blk, zero, zero)
        shift, first, second = state
        moved = values - shift
        return shift, fold(moved, first), fold(moved * moved, second)

    def scatter(tag, a_ref, w_copy, slot_of, depth, ahead, late, near_ready=()):
        dsend, drecv, qsend, qrecv, own, part = (refs[k] for k in ('dsend', 'drecv', 'qsend', 'qrecv', 'own', 'part'))
        ds_sem, dr_sem, qs_sem, qr_sem = (refs[tag + k] for k in ('ds', 'dr', 'qs', 'qr'))

        def d_copy(n, i):
            return remote(dsend.at[n, i], drecv.at[n, i], ds_sem.at[n, i], dr_sem.at[n, i], partner)

        def q_copy(n):
            return remote(qsend.at[n], qrecv.at[n], qs_sem.at[n], qr_sem.at[n], counter)

        def step(n, carry):
            @pl.when(n + ahead < STEPS)
            def _():
                w_copy(n + ahead).start()

            w_copy(n).wait()
            cols = col(slot_of(n))
            far = jnp.dot(a_ref[2:4].reshape(2 * rows, depth), wbuf[0:depth, cols], preferred_element_type=F32)
            dsend[n, 0] = far[rows:].astype(BF)
            d_copy(n, 0).start()
            part[...] = far[:rows]
            if near_ready:
                @pl.when(n == 0)
                def _():
                    for copy in near_ready:
                        copy.wait()

            near = jnp.dot(a_ref[0:2].reshape(2 * rows, depth), wbuf[0:depth, cols], preferred_element_type=F32)
            dsend[n, 1] = near[rows:].astype(BF)
            d_copy(n, 1).start()
            own[n] = near[:rows]
            d_copy(n, 0).wait_recv()
            qsend[n] = (part[...] + drecv[n, 0].astype(F32)).astype(BF)
            q_copy(n).start()
            return carry

        half = STEPS - ahead
        lax.fori_loop(0, half, step, 0)
        late(0)
        lax.fori_loop(half, STEPS, step, 0)
        late(1)
        total = None
        for n in range(STEPS):
            cols = slice(n * blk, (n + 1) * blk)
            d_copy(n, 1).wait_recv()
            q_copy(n).wait_recv()
            summed = own[n] + drecv[n, 1].astype(F32) + qrecv[n].astype(F32)
            fresh = (xbuf[:, cols].astype(F32) + summed.astype(BF).astype(F32)).astype(BF)
            xbuf[:, cols] = fresh
            total = moments(fresh.astype(F32), total)
        for n in range(STEPS):
            d_copy(n, 0).wait_send()
            d_copy(n, 1).wait_send()
            q_copy(n).wait_send()
        return total

    def gather(tag, ln_row, total, w_at, n_out, ready, finish):
        near_h, far_h, acc = refs['near_h'], refs['far_h'], refs['acc']
        cs, cr, fs, fr, ps, pr = (refs[tag + k] for k in ('cs', 'cr', 'fs', 'fr', 'ps', 'pr'))
        shift, first, second = total
        offset = jnp.sum(first, axis=-1, keepdims=True) / d_model
        mean = shift + offset
        variance = jnp.maximum(jnp.sum(second, axis=-1, keepdims=True) / d_model - offset * offset, 0.0)
        inv = lax.rsqrt(variance + LN_EPS)

        chunk = blk // 2

        def c_copy(k):
            return remote(near_h.at[pl.ds(0, rows), col(k, chunk)], far_h.at[pl.ds(0, rows), col(k, chunk)], cs.at[k], cr.at[k], counter)

        def f_copy(k):
            return remote(far_h.at[pl.ds(0, rows), col(k, chunk)], far_h.at[pl.ds(rows, rows), col(k, chunk)], fs.at[k], fr.at[k], partner)

        def p_copy(k):
            return remote(near_h.at[pl.ds(0, rows), col(k)], near_h.at[pl.ds(rows, rows), col(k)], ps.at[k], pr.at[k], partner)

        for k in range(STEPS):
            cols = slice(k * blk, (k + 1) * blk)
            gain = refs['ln_gain'][ln_row // 2, ln_row % 2:ln_row % 2 + 1, cols].astype(F32)
            bias = refs['ln_bias'][ln_row // 2, ln_row % 2:ln_row % 2 + 1, cols].astype(F32)
            normed = (xbuf[:, cols].astype(F32) - mean) * inv
            near_h[0:rows, cols] = (normed * (1.0 + gain) + bias).astype(BF)
            if k:
                c_copy(2 * k - 2).start()
                c_copy(2 * k - 1).start()
                p_copy(k - 1).start()
        acc[:, 0:n_out] = jnp.zeros((2 * rows, n_out), F32)
        c_copy(2 * STEPS - 2).start()
        c_copy(2 * STEPS - 1).start()
        p_copy(STEPS - 1).start()
        ready()
        for k in range(STEPS):
            p_copy(k).wait_recv()

        n_blk = n_out // STEPS
        piece = min(1024, n_out)

        def far_dot(k, width, cols):
            return jnp.dot(far_h[:, col(k, width)], wbuf[col(k, width), w_at + cols.start:w_at + cols.stop], preferred_element_type=F32)

        pieces = [slice(n, n + piece) for n in range(0, n_out, piece)]

        def far_step(k, width):
            for cols in pieces:
                acc[:, cols] += far_dot(k, width, cols)

        def pass_on(k):
            c_copy(k).wait_recv()
            f_copy(k).start()

        def near_step(i):
            at = pl.ds(pl.multiple_of(w_at + i * n_blk, n_blk), n_blk)
            finish(0, col(i, n_blk), jnp.dot(near_h[...], wbuf[:, at], preferred_element_type=F32), [i])
            pass_on(2 * i)

        def step(i, carry):
            near_step(i)
            f_copy(2 * i - 2).wait_recv()
            f_copy(2 * i - 1).wait_recv()
            far_step(i - 1, blk)
            pass_on(2 * i + 1)
            return carry

        near_step(0)
        pass_on(1)
        lax.fori_loop(1, STEPS, step, 0)
        f_copy(2 * STEPS - 2).wait_recv()
        far_step(2 * STEPS - 2, chunk)
        f_copy(2 * STEPS - 1).wait_recv()
        for cols in pieces:
            finish(2, cols, acc[:, cols] + far_dot(2 * STEPS - 1, chunk, cols), range(cols.start // n_blk, cols.stop // n_blk))
        for k in range(STEPS):
            p_copy(k).wait_send()
        for k in range(2 * STEPS):
            c_copy(k).wait_send()
            f_copy(k).wait_send()

    def split(value):
        return value.reshape(2, n_seq, toks, value.shape[-1])

    def gather_qkv(layer, total, w_at, start_now):
        stage, y_out = refs['stage'], refs['y_out']
        n_out = y_out.shape[3]
        n_blk = n_out // STEPS

        def y_copy(g, n):
            return pltpu.make_async_copy(stage.at[g, :, :, col(n, n_blk)], y_out.at[:, order[g], :, col(n, n_blk)], refs['y_sem'].at[g, n])

        def ready():
            if start_now:
                tabs = refs['tabs']

                def table(b, carry):
                    for i, part in enumerate(rope_tables(refs['start'][b], tabs.shape[2], tabs.shape[3])):
                        tabs[i, b] = part
                    return carry

                lax.fori_loop(0, n_seq, table, 0)
                tab_copy.start()
            for copy in qkv_copies(layer, w_at):
                copy.wait()

        def finish(g, cols, value, blocks):
            stage[g:g + 2, :, :, cols] = split(value)
            for n in blocks:
                y_copy(g, n).start()
                y_copy(g + 1, n).start()

        if start_now:
            tab_copy = pltpu.make_async_copy(refs['tabs'], refs['tab_out'], refs['tab_sem'])
        gather('g2', 2 * layer, total, w_at, n_out, ready, finish)
        if start_now:
            tab_copy.wait()
        for g in range(4):
            for n in range(STEPS):
                y_copy(g, n).wait()

    def qkv_copies(layer, w_at):
        copies = []
        for i, name in enumerate(('w_q', 'w_k', 'w_v')):
            width = refs[name].shape[2]
            copies.append(pltpu.make_async_copy(refs[name].at[layer], wbuf.at[:, pl.ds(w_at, width)], refs['gw_sem'].at[i]))
            w_at += width
        return copies

    x_copy = pltpu.make_async_copy(refs['x_hbm'], xbuf, refs['x_sem'])
    if cfg['first']:
        x_copy.start()
        x_copy.wait()
        for copy in qkv_copies(0, 0):
            copy.start()
        total = None
        for n in range(STEPS):
            total = moments(xbuf[:, n * blk:(n + 1) * blk].astype(F32), total)
        pl.semaphore_wait(barrier, 2)
        gather_qkv(0, total, 0, True)
        return

    layer = cfg['layer']
    abuf, act = refs['abuf'], refs['act']
    depth = abuf.shape[3]
    a_copies = [pltpu.make_async_copy(refs['a_hbm'].at[:, order[g]], abuf.at[g], refs['a_sem'].at[g]) for g in range(4)]

    def o_copy(n):
        return pltpu.make_async_copy(refs['w_o'].at[layer, :, col(n)], wbuf.at[pl.ds(0, depth), col(n)], refs['ow_sem'].at[n])

    def up_copy(i):
        span = pl.ds(0, depth) if i else pl.ds(depth, d_model - depth)
        return pltpu.make_async_copy(refs['w_up'].at[layer, span, :], wbuf.at[span, pl.ds(0, d_model)], refs['uw_sem'].at[i])

    def down_slot(n):
        return lax.rem(n + STEPS, WIDE)

    def down_copy(n):
        return pltpu.make_async_copy(refs['w_down'].at[layer, :, col(n)], wbuf.at[:, col(down_slot(n))], refs['dw_sem'].at[n])

    for g in (2, 3):
        a_copies[g].start()
    o_copy(0).start()
    for g in (0, 1):
        a_copies[g].start()
    o_copy(1).start()
    o_copy(2).start()
    x_copy.start()
    pl.semaphore_wait(barrier, 2)
    for copy in a_copies[2:]:
        copy.wait()

    def late_up(i):
        up_copy(i).start()
        if i:
            x_copy.wait()

    total = scatter('s1', abuf, o_copy, lambda n: n, depth, 3, late_up, a_copies[:2])

    def ready_up():
        for i in range(2):
            up_copy(i).wait()
        for n in range(WIDE - STEPS):
            down_copy(n).start()

    def finish_up(g, cols, value, blocks):
        act[g:g + 2, :, :, cols] = split(jnp.square(jnp.maximum(value, 0.0)).astype(BF))

    gather('g1', 2 * layer + 1, total, 0, d_model, ready_up, finish_up)

    w_at = (WIDE * blk) - (4 * blk)

    def late_qkv(i):
        if i == 0 and cfg['more']:
            for copy in qkv_copies(layer + 1, w_at):
                copy.start()

    total = scatter('s2', act, down_copy, down_slot, d_model, WIDE - STEPS, late_qkv)
    out_copy = pltpu.make_async_copy(xbuf, refs['x_out'], refs['x_sem'])
    out_copy.start()
    if cfg['more']:
        gather_qkv(layer + 1, total, w_at, False)
    out_copy.wait()


def exchange(cid, x, ln_gain, ln_bias, qkv_weights, *, n_seq, layer=-1, more=True, a=None, weights=(), start_pos=None, head_dim=0):
    rows, d_model = x.shape
    toks = rows // n_seq
    blk = d_model // STEPS
    first = a is None
    any_spec, vmem = pl.BlockSpec(memory_space=pl.ANY), pl.BlockSpec(memory_space=pltpu.VMEM)
    dma = pltpu.SemaphoreType.DMA
    ins = [('x_hbm', x, any_spec), ('ln_gain', ln_gain, vmem), ('ln_bias', ln_bias, vmem)]
    outs = []
    qkv_out = sum(w.shape[2] for w in qkv_weights)
    width = qkv_out if first else WIDE * blk
    scr = [('wbuf', pltpu.VMEM((d_model, width), BF)), ('xbuf', pltpu.VMEM((rows, d_model), BF)), ('x_sem', dma)]
    scr += [
        ('near_h', pltpu.VMEM((2 * rows, d_model), BF)), ('far_h', pltpu.VMEM((2 * rows, d_model), BF)),
        ('acc', pltpu.VMEM((2 * rows, qkv_out if first else d_model), F32)),
    ]
    gather_tags, flops, moved = [], 0, 4_000_000
    if not first:
        w_o, w_up, w_down = weights
        depth = a.shape[3]
        ins += [('a_hbm', a, any_spec), ('w_o', w_o, any_spec), ('w_up', w_up, any_spec), ('w_down', w_down, any_spec)]
        outs += [('x_out', jax.ShapeDtypeStruct(x.shape, BF))]
        scr += [
            ('abuf', pltpu.VMEM((4, n_seq, toks, depth), BF)), ('act', pltpu.VMEM((4, n_seq, toks, d_model), BF)),
            ('dsend', pltpu.VMEM((STEPS, 2, rows, blk), BF)), ('drecv', pltpu.VMEM((STEPS, 2, rows, blk), BF)),
            ('qsend', pltpu.VMEM((STEPS, rows, blk), BF)), ('qrecv', pltpu.VMEM((STEPS, rows, blk), BF)),
            ('own', pltpu.VMEM((STEPS, rows, blk), F32)), ('part', pltpu.VMEM((rows, blk), F32)),
            ('a_sem', dma((4,))), ('ow_sem', dma((STEPS,))), ('uw_sem', dma((2,))), ('dw_sem', dma((STEPS,))),
        ]
        for tag in ('s1', 's2'):
            scr += [(tag + k, dma((STEPS, 2))) for k in ('ds', 'dr')] + [(tag + k, dma((STEPS,))) for k in ('qs', 'qr')]
        gather_tags.append('g1')
        flops += 2 * 4 * rows * d_model * (depth + 2 * d_model)
        moved += 2 * d_model * (depth + 2 * d_model)
    if more:
        ins += list(zip(('w_q', 'w_k', 'w_v'), qkv_weights, [any_spec] * 3))
        outs += [('y_out', jax.ShapeDtypeStruct((n_seq, 4, toks, qkv_out), F32))]
        scr += [('stage', pltpu.VMEM((4, n_seq, toks, qkv_out), F32)), ('gw_sem', dma((3,))), ('y_sem', dma((4, STEPS)))]
        gather_tags.append('g2')
        flops += 2 * 4 * rows * d_model * qkv_out
        moved += 2 * d_model * qkv_out
    if first:
        tab_shape = (3, n_seq, 4 * toks, head_dim)
        ins += [('start', start_pos, pl.BlockSpec(memory_space=pltpu.SMEM))]
        outs += [('tab_out', jax.ShapeDtypeStruct(tab_shape, F32))]
        scr += [('tabs', pltpu.VMEM(tab_shape, F32)), ('tab_sem', dma)]
    for tag in gather_tags:
        scr += [(tag + k, dma((2 * STEPS,))) for k in ('cs', 'cr', 'fs', 'fr')] + [(tag + k, dma((STEPS,))) for k in ('ps', 'pr')]
    cfg = dict(names=[i[0] for i in ins] + [o[0] for o in outs] + [s[0] for s in scr], layer=layer, first=first, more=more, n_seq=n_seq, toks=toks, d_model=d_model)
    return pl.pallas_call(
        functools.partial(exchange_kernel, cfg),
        in_specs=[i[2] for i in ins],
        out_specs=[any_spec] * len(outs),
        out_shape=[o[1] for o in outs],
        scratch_shapes=[s[1] for s in scr],
        compiler_params=pltpu.CompilerParams(collective_id=cid, has_side_effects=True, vmem_limit_bytes=67_000_000),
        cost_estimate=pl.CostEstimate(flops=flops, bytes_accessed=moved, transcendentals=0),
        name='gather_first' if first else 'block' if more else 'block_last',
    )(*[i[1] for i in ins])


def solution(mesh):
    tok_spec = P('dp', 'tp', None)
    cache_spec = P(None, 'dp', 'tp', None, None)
    col_spec = P(None, None, 'tp')
    row_spec = P(None, 'tp', None)

    def device_fn(x_loc, start_pos, k_cache, v_cache, w_q, w_k, w_v, w_o, w_up, w_down, ln_gain, ln_bias):
        n_layers = w_q.shape[0]
        n_seq, tok_loc, d_model = x_loc.shape
        new_len = tok_loc * 4
        rows = n_seq * new_len
        hidden = x_loc.reshape(n_seq * tok_loc, d_model)
        prev = ()
        qkv_weights = (w_q, w_k, w_v)
        qkv, tabs = exchange(0, hidden, ln_gain, ln_bias, qkv_weights, n_seq=n_seq, start_pos=start_pos, head_dim=k_cache.shape[4])
        for layer in range(n_layers):
            context, *prev = attend(layer, qkv.reshape(rows, -1), tabs, start_pos, k_cache, v_cache, prev)
            context = context.reshape(n_seq, 4, tok_loc, -1)
            outs = exchange(layer + 1, hidden, ln_gain, ln_bias, qkv_weights, n_seq=n_seq, layer=layer, more=layer + 1 < n_layers, a=context, weights=(w_o, w_up, w_down))
            hidden, qkv = outs if layer + 1 < n_layers else (outs[0], None)
        return hidden.reshape(x_loc.shape), prev[0], prev[1]

    return jax.shard_map(device_fn, mesh=mesh, in_specs=(tok_spec, P('dp'), cache_spec, cache_spec, col_spec, col_spec, col_spec, row_spec, col_spec, row_spec, P(), P()), out_specs=(tok_spec, cache_spec, cache_spec), check_vma=False)
```

```python
import functools
import math

import jax
import jax.numpy as jnp
from jax import lax
from jax.experimental import pallas as pl
from jax.experimental.pallas import tpu as pltpu
from jax.sharding import PartitionSpec as P

LN_EPS = 1e-5
ROPE_BASE = 10000.0
NEG_BIG = -1e30
MIN_START = 768
SLOTS = 4
BF = jnp.bfloat16
F32 = jnp.float32


def rope_tables(start, toks, head_dim):
    rot = head_dim // 2
    half = rot // 2
    shape = (toks, head_dim)
    lane = lax.broadcasted_iota(jnp.int32, shape, 1)
    position = start + lax.broadcasted_iota(jnp.int32, shape, 0)
    power = lax.rem(lane, half).astype(F32) * (2.0 / rot)
    angles = position.astype(F32) * jnp.exp(power * -math.log(ROPE_BASE))
    cos_a, sin_a = jnp.cos(angles), jnp.sin(angles)
    upper = jnp.logical_and(lane >= half, lane < rot)
    return jnp.where(lane < rot, cos_a, 1.0), jnp.where(upper, sin_a, 0.0), jnp.where(lane < half, -sin_a, 0.0)


def attn_kernel(layer, dims, start_ref, q_ref, k_ref, v_ref, tab_ref, kc_hbm, vc_hbm, *rest):
    kv, group, toks, hd, s_len, ch = dims
    if layer > 0:
        rest = rest[2:]
    ctx_ref, ko_hbm, vo_hbm, kbuf, vbuf, sbuf, ebuf, qbuf, mbuf, pbuf, lbuf, abuf, in_sem, out_sem = rest
    b = pl.program_id(0)
    nb = pl.num_programs(0) - 1
    s_pad = kbuf.shape[2]
    win = toks + 16
    rows = group * toks
    coef = (hd ** -0.5) * math.log2(math.e)
    slot = lax.rem(b, SLOTS)
    before = lax.rem(b + SLOTS - 1, SLOTS)

    def load(bb):
        sl = lax.rem(bb, SLOTS)
        return [pltpu.make_async_copy(src.at[layer, bb], dst.at[sl, :, pl.ds(0, s_len), :], in_sem.at[sl, i]) for i, (src, dst) in enumerate(((kc_hbm, kbuf), (vc_hbm, vbuf)))]

    def save(bb):
        sl = lax.rem(bb, SLOTS)
        return [pltpu.make_async_copy(src.at[sl, :, pl.ds(0, s_len), :], dst.at[layer, bb], out_sem.at[sl, i]) for i, (src, dst) in enumerate(((kbuf, ko_hbm), (vbuf, vo_hbm)))]

    def run(copies, go):
        for copy in copies:
            copy.start() if go else copy.wait()

    @pl.when(b == 0)
    def _():
        run(load(b), True)
        if s_pad > s_len:
            for sl in range(SLOTS):
                kbuf[sl, :, s_len:, :] = jnp.zeros((kv, s_pad - s_len, hd), BF)
                vbuf[sl, :, s_len:, :] = jnp.zeros((kv, s_pad - s_len, hd), BF)

    @pl.when(b >= 2)
    def _():
        run(save(b - 2), False)

    @pl.when(jnp.logical_and(b > 0, b + 2 < nb))
    def _():
        run(load(b + 2), True)

    start = start_ref[jnp.minimum(b, nb - 1)]
    start_before = start_ref[jnp.maximum(b - 1, 0)]
    half = hd // 4

    def rope(x):
        return x * tab_ref[0, 0] + pltpu.roll(x, half, 1) * tab_ref[1, 0] + pltpu.roll(x, hd - half, 1) * tab_ref[2, 0]

    def patch():
        base = jnp.minimum((start // 16) * 16, s_len - win)
        shift = start - base
        base = pl.multiple_of(base, 16)
        row_id = lax.broadcasted_iota(jnp.int32, (win, hd), 0)
        is_new = jnp.logical_and(row_id >= shift, row_id < shift + toks)
        run(load(b), False)

        @pl.when(b == 0)
        def _():
            run(load(b + 1), True)
            run(load(b + 2), True)

        for h in range(kv):
            cols = slice(h * hd, (h + 1) * hd)
            for buf, fresh in ((kbuf, rope(k_ref[:, cols])), (vbuf, v_ref[:, cols])):
                fresh = fresh.astype(BF).astype(F32)
                fresh = jnp.concatenate([fresh, jnp.zeros((16, hd), F32)], axis=0)
                fresh = pltpu.roll(fresh, shift, 0)
                old = buf[slot, h, pl.ds(base, win), :].astype(F32)
                buf[slot, h, pl.ds(base, win), :] = jnp.where(is_new, fresh, old).astype(BF)
        run(save(b), True)

    step_rows = 64
    blocks = [slice(r, r + step_rows) for r in range(0, ch, step_rows)]

    def chunk(j):
        return pl.ds(pl.multiple_of(j * ch, ch), ch)

    def score(h, j, masked):
        s = lax.dot_general(kbuf[slot, h, chunk(j), :], qbuf[h], (((1,), (1,)), ((), ())), preferred_element_type=F32)
        if masked:
            ahead = lax.broadcasted_iota(jnp.int32, (ch, rows), 0) - lax.rem(lax.broadcasted_iota(jnp.int32, (ch, rows), 1), toks)
            s = jnp.where(ahead <= start - j * ch, s, NEG_BIG)
        sbuf[h] = s

    def scored(h, rb):
        return sbuf[h, rb].reshape(step_rows // 8, 8, rows)

    def peaks(h, peak):
        top = jnp.max(scored(h, blocks[0]), axis=0)
        for rb in blocks[1:]:
            top = jnp.maximum(top, jnp.max(scored(h, rb), axis=0))
        mbuf[h] = peak
        pbuf[h] = jnp.maximum(peak, jnp.max(top, axis=0, keepdims=True))

    def weigh(h):
        peak = pbuf[h]
        alpha = jnp.exp2((mbuf[h] - peak) * coef)
        total = lbuf[h] * alpha
        for rb in blocks:
            e = jnp.exp2((scored(h, rb) - peak) * coef)
            total = total + jnp.sum(e, axis=0)
            ebuf[h, rb] = e.reshape(step_rows, rows).astype(BF)
        return alpha, total

    def mix(h, sl, j, alpha):
        fresh = lax.dot_general(vbuf[sl, h, chunk(j), :], ebuf[h], (((0,), (0,)), ((), ())), preferred_element_type=F32)
        return (abuf[h].reshape(hd // 8, 8, rows) * alpha).reshape(hd, rows) + fresh

    def step(masked_next, j, carry):
        for h in range(kv):
            alpha, lbuf[h] = weigh(h)
            score(h, j + 1, masked_next)
            abuf[h] = mix(h, slot, j, alpha)
        for h in range(kv):
            peaks(h, pbuf[h])
        return carry

    def last_of(bb_start):
        return (bb_start + toks + ch - 1) // ch - 1

    def turn(close, open_next):
        if open_next:
            for h in range(kv):
                for g in range(group):
                    j = h * group + g
                    qbuf[h, g * toks:(g + 1) * toks, :] = rope(q_ref[:, j * hd:(j + 1) * hd]).astype(BF)
            patch()
        for h in range(kv):
            if close:
                alpha, total = weigh(h)
            if open_next:
                score(h, 0, ch > MIN_START)
            if close:
                ctx = (mix(h, before, last_of(start_before), alpha) / jnp.sum(total, axis=0, keepdims=True)).T.astype(BF)
                for g in range(group):
                    j = h * group + g
                    ctx_ref[:, j * hd:(j + 1) * hd] = ctx[g * toks:(g + 1) * toks, :]
        if open_next:
            for h in range(kv):
                peaks(h, jnp.full((8, rows), NEG_BIG, F32))
                lbuf[h] = jnp.zeros((8, rows), F32)
                abuf[h] = jnp.zeros((hd, rows), F32)

    pl.when(b == 0)(functools.partial(turn, False, True))
    pl.when(jnp.logical_and(b > 0, b < nb))(functools.partial(turn, True, True))
    pl.when(b == nb)(functools.partial(turn, True, False))

    @pl.when(b < nb)
    def _():
        n_full = jnp.maximum(start // ch, 1)
        lax.fori_loop(0, n_full - 1, functools.partial(step, False), 0)
        lax.fori_loop(n_full - 1, last_of(start), functools.partial(step, True), 0)

    @pl.when(b == nb)
    def _():
        run(save(b - 1), False)


def attend(layer, qkv, tabs, start_pos, k_cache, v_cache, prev):
    n_seq = start_pos.shape[0]
    _, _, kv, s_len, hd = k_cache.shape
    toks = qkv.shape[0] // n_seq
    kv_width = kv * hd
    q_width = qkv.shape[1] - 2 * kv_width
    group = q_width // kv_width
    n_ch = -(-s_len // 640)
    ch = 128 * -(-s_len // (128 * n_ch))
    rows = group * toks
    dims = (kv, group, toks, hd, s_len, ch)
    any_spec = pl.BlockSpec(memory_space=pl.ANY)
    now = lambda b: jnp.minimum(b, n_seq - 1)
    tab_spec = pl.BlockSpec((3, 1, toks, hd), lambda b, *_: (0, now(b), 0, 0))
    cache_shape = jax.ShapeDtypeStruct(k_cache.shape, BF)
    args = [start_pos, qkv, qkv, qkv, tabs, k_cache, v_cache] + list(prev)
    return pl.pallas_call(
        functools.partial(attn_kernel, layer, dims),
        grid_spec=pltpu.PrefetchScalarGridSpec(
            num_scalar_prefetch=1,
            grid=(n_seq + 1,),
            in_specs=[
                pl.BlockSpec((toks, q_width), lambda b, *_: (now(b), 0)),
                pl.BlockSpec((toks, kv_width), lambda b, *_: (now(b), group)),
                pl.BlockSpec((toks, kv_width), lambda b, *_: (now(b), group + 1)),
                tab_spec,
            ] + [any_spec] * (2 + len(prev)),
            out_specs=[pl.BlockSpec((toks, q_width), lambda b, *_: (jnp.maximum(b - 1, 0), 0)), any_spec, any_spec],
            scratch_shapes=[
                pltpu.VMEM((SLOTS, kv, ch * n_ch, hd), BF),
                pltpu.VMEM((SLOTS, kv, ch * n_ch, hd), BF),
                pltpu.VMEM((kv, ch, rows), F32),
                pltpu.VMEM((kv, ch, rows), BF),
                pltpu.VMEM((kv, rows, hd), BF),
                pltpu.VMEM((kv, 8, rows), F32),
                pltpu.VMEM((kv, 8, rows), F32),
                pltpu.VMEM((kv, 8, rows), F32),
                pltpu.VMEM((kv, hd, rows), F32),
                pltpu.SemaphoreType.DMA((SLOTS, 2)),
                pltpu.SemaphoreType.DMA((SLOTS, 2)),
            ],
        ),
        out_shape=[jax.ShapeDtypeStruct((n_seq * toks, q_width), BF), cache_shape, cache_shape],
        input_output_aliases={7: 1, 8: 2} if prev else {},
        compiler_params=pltpu.CompilerParams(vmem_limit_bytes=60 * 1024 * 1024, dimension_semantics=("arbitrary",)),
        cost_estimate=pl.CostEstimate(flops=8_000_000_000, bytes_accessed=80_000_000, transcendentals=15_000_000),
        name="attend",
    )(*args)


STEPS = 8
WIDE = STEPS + 2


def exchange_kernel(cfg, *args):
    refs = dict(zip(cfg['names'], args))
    n_seq, toks, d_model = cfg['n_seq'], cfg['toks'], cfg['d_model']
    rows = n_seq * toks
    blk = d_model // STEPS
    me = lax.axis_index('tp')
    core = lax.rem(me, 2)
    partner = me + 1 - 2 * core
    counter = lax.rem(me + 2, 4)
    diag = lax.rem(partner + 2, 4)
    order = (me, partner, counter, diag)
    wbuf, xbuf = refs['wbuf'], refs['xbuf']

    barrier = pltpu.get_barrier_semaphore()
    for peer in (partner, counter):
        pl.semaphore_signal(barrier, inc=1, device_id={'tp': peer}, device_id_type=pl.DeviceIdType.MESH)

    def col(n, width=blk):
        return pl.ds(pl.multiple_of(n * width, width), width)

    def remote(src, dst, send, recv, peer):
        return pltpu.make_async_remote_copy(src_ref=src, dst_ref=dst, send_sem=send, recv_sem=recv, device_id={'tp': peer}, device_id_type=pl.DeviceIdType.MESH)

    def fold(values, total):
        for j in range(blk // 128):
            total = total + values[:, j * 128:(j + 1) * 128]
        return total

    def moments(values, state):
        zero = jnp.zeros((rows, 128), F32)
        if state is None:
            state = (jnp.sum(fold(values, zero), axis=-1, keepdims=True) / blk, zero, zero)
        shift, first, second = state
        moved = values - shift
        return shift, fold(moved, first), fold(moved * moved, second)

    def scatter(tag, a_ref, w_copy, slot_of, depth, ahead, late, near_ready=()):
        dsend, drecv, qsend, qrecv, own, part = (refs[k] for k in ('dsend', 'drecv', 'qsend', 'qrecv', 'own', 'part'))
        ds_sem, dr_sem, qs_sem, qr_sem = (refs[tag + k] for k in ('ds', 'dr', 'qs', 'qr'))

        def d_copy(n, i):
            return remote(dsend.at[n, i], drecv.at[n, i], ds_sem.at[n, i], dr_sem.at[n, i], partner)

        def q_copy(n):
            return remote(qsend.at[n], qrecv.at[n], qs_sem.at[n], qr_sem.at[n], counter)

        def step(n, carry):
            @pl.when(n + ahead < STEPS)
            def _():
                w_copy(n + ahead).start()

            w_copy(n).wait()
            cols = col(slot_of(n))
            far = jnp.dot(a_ref[2:4].reshape(2 * rows, depth), wbuf[0:depth, cols], preferred_element_type=F32)
            dsend[n, 0] = far[rows:].astype(BF)
            d_copy(n, 0).start()
            part[...] = far[:rows]
            if near_ready:
                @pl.when(n == 0)
                def _():
                    for copy in near_ready:
                        copy.wait()

            near = jnp.dot(a_ref[0:2].reshape(2 * rows, depth), wbuf[0:depth, cols], preferred_element_type=F32)
            dsend[n, 1] = near[rows:].astype(BF)
            d_copy(n, 1).start()
            own[n] = near[:rows]
            d_copy(n, 0).wait_recv()
            qsend[n] = (part[...] + drecv[n, 0].astype(F32)).astype(BF)
            q_copy(n).start()
            return carry

        half = STEPS - ahead
        lax.fori_loop(0, half, step, 0)
        late(0)
        lax.fori_loop(half, STEPS, step, 0)
        late(1)
        total = None
        for n in range(STEPS):
            cols = slice(n * blk, (n + 1) * blk)
            d_copy(n, 1).wait_recv()
            q_copy(n).wait_recv()
            summed = own[n] + drecv[n, 1].astype(F32) + qrecv[n].astype(F32)
            fresh = (xbuf[:, cols].astype(F32) + summed.astype(BF).astype(F32)).astype(BF)
            xbuf[:, cols] = fresh
            total = moments(fresh.astype(F32), total)
        for n in range(STEPS):
            d_copy(n, 0).wait_send()
            d_copy(n, 1).wait_send()
            q_copy(n).wait_send()
        return total

    def gather(tag, ln_row, total, w_at, n_out, ready, finish):
        near_h, far_h, acc = refs['near_h'], refs['far_h'], refs['acc']
        cs, cr, fs, fr, ps, pr = (refs[tag + k] for k in ('cs', 'cr', 'fs', 'fr', 'ps', 'pr'))
        shift, first, second = total
        offset = jnp.sum(first, axis=-1, keepdims=True) / d_model
        mean = shift + offset
        variance = jnp.maximum(jnp.sum(second, axis=-1, keepdims=True) / d_model - offset * offset, 0.0)
        inv = lax.rsqrt(variance + LN_EPS)

        chunk = blk // 2

        def c_copy(k):
            return remote(near_h.at[pl.ds(0, rows), col(k, chunk)], far_h.at[pl.ds(0, rows), col(k, chunk)], cs.at[k], cr.at[k], counter)

        def f_copy(k):
            return remote(far_h.at[pl.ds(0, rows), col(k, chunk)], far_h.at[pl.ds(rows, rows), col(k, chunk)], fs.at[k], fr.at[k], partner)

        def p_copy(k):
            return remote(near_h.at[pl.ds(0, rows), col(k)], near_h.at[pl.ds(rows, rows), col(k)], ps.at[k], pr.at[k], partner)

        for k in range(STEPS):
            cols = slice(k * blk, (k + 1) * blk)
            gain = refs['ln_gain'][ln_row // 2, ln_row % 2:ln_row % 2 + 1, cols].astype(F32)
            bias = refs['ln_bias'][ln_row // 2, ln_row % 2:ln_row % 2 + 1, cols].astype(F32)
            normed = (xbuf[:, cols].astype(F32) - mean) * inv
            near_h[0:rows, cols] = (normed * (1.0 + gain) + bias).astype(BF)
            if k:
                c_copy(2 * k - 2).start()
                c_copy(2 * k - 1).start()
                p_copy(k - 1).start()
        acc[:, 0:n_out] = jnp.zeros((2 * rows, n_out), F32)
        c_copy(2 * STEPS - 2).start()
        c_copy(2 * STEPS - 1).start()
        p_copy(STEPS - 1).start()
        ready()
        for k in range(STEPS):
            p_copy(k).wait_recv()

        n_blk = n_out // STEPS
        piece = min(1024, n_out)

        def far_dot(k, width, cols):
            return jnp.dot(far_h[:, col(k, width)], wbuf[col(k, width), w_at + cols.start:w_at + cols.stop], preferred_element_type=F32)

        pieces = [slice(n, n + piece) for n in range(0, n_out, piece)]

        def far_step(k, width):
            for cols in pieces:
                acc[:, cols] += far_dot(k, width, cols)

        def pass_on(k):
            c_copy(k).wait_recv()
            f_copy(k).start()

        def near_step(i):
            at = pl.ds(pl.multiple_of(w_at + i * n_blk, n_blk), n_blk)
            finish(0, col(i, n_blk), jnp.dot(near_h[...], wbuf[:, at], preferred_element_type=F32), [i])
            pass_on(2 * i)

        def step(i, carry):
            near_step(i)
            f_copy(2 * i - 2).wait_recv()
            f_copy(2 * i - 1).wait_recv()
            far_step(i - 1, blk)
            pass_on(2 * i + 1)
            return carry

        near_step(0)
        pass_on(1)
        lax.fori_loop(1, STEPS, step, 0)
        f_copy(2 * STEPS - 2).wait_recv()
        far_step(2 * STEPS - 2, chunk)
        f_copy(2 * STEPS - 1).wait_recv()
        for cols in pieces:
            finish(2, cols, acc[:, cols] + far_dot(2 * STEPS - 1, chunk, cols), range(cols.start // n_blk, cols.stop // n_blk))
        for k in range(STEPS):
            p_copy(k).wait_send()
        for k in range(2 * STEPS):
            c_copy(k).wait_send()
            f_copy(k).wait_send()

    def split(value):
        return value.reshape(2, n_seq, toks, value.shape[-1])

    def gather_qkv(layer, total, w_at, start_now):
        stage, y_out = refs['stage'], refs['y_out']
        n_out = y_out.shape[3]
        n_blk = n_out // STEPS

        def y_copy(g, n):
            return pltpu.make_async_copy(stage.at[g, :, :, col(n, n_blk)], y_out.at[:, order[g], :, col(n, n_blk)], refs['y_sem'].at[g, n])

        def ready():
            if start_now:
                tabs = refs['tabs']

                def table(b, carry):
                    for i, part in enumerate(rope_tables(refs['start'][b], tabs.shape[2], tabs.shape[3])):
                        tabs[i, b] = part
                    return carry

                lax.fori_loop(0, n_seq, table, 0)
                tab_copy.start()
            for copy in qkv_copies(layer, w_at):
                copy.wait()

        def finish(g, cols, value, blocks):
            stage[g:g + 2, :, :, cols] = split(value)
            for n in blocks:
                y_copy(g, n).start()
                y_copy(g + 1, n).start()

        if start_now:
            tab_copy = pltpu.make_async_copy(refs['tabs'], refs['tab_out'], refs['tab_sem'])
        gather('g2', 2 * layer, total, w_at, n_out, ready, finish)
        if start_now:
            tab_copy.wait()
        for g in range(4):
            for n in range(STEPS):
                y_copy(g, n).wait()

    def qkv_copies(layer, w_at):
        copies = []
        for i, name in enumerate(('w_q', 'w_k', 'w_v')):
            width = refs[name].shape[2]
            copies.append(pltpu.make_async_copy(refs[name].at[layer], wbuf.at[:, pl.ds(w_at, width)], refs['gw_sem'].at[i]))
            w_at += width
        return copies

    x_copy = pltpu.make_async_copy(refs['x_hbm'], xbuf, refs['x_sem'])
    if cfg['first']:
        x_copy.start()
        x_copy.wait()
        for copy in qkv_copies(0, 0):
            copy.start()
        total = None
        for n in range(STEPS):
            total = moments(xbuf[:, n * blk:(n + 1) * blk].astype(F32), total)
        pl.semaphore_wait(barrier, 2)
        gather_qkv(0, total, 0, True)
        return

    layer = cfg['layer']
    abuf, act = refs['abuf'], refs['act']
    depth = abuf.shape[3]
    a_copies = [pltpu.make_async_copy(refs['a_hbm'].at[:, order[g]], abuf.at[g], refs['a_sem'].at[g]) for g in range(4)]

    def o_copy(n):
        return pltpu.make_async_copy(refs['w_o'].at[layer, :, col(n)], wbuf.at[pl.ds(0, depth), col(n)], refs['ow_sem'].at[n])

    def up_copy(i):
        span = pl.ds(0, depth) if i else pl.ds(depth, d_model - depth)
        return pltpu.make_async_copy(refs['w_up'].at[layer, span, :], wbuf.at[span, pl.ds(0, d_model)], refs['uw_sem'].at[i])

    def down_slot(n):
        return lax.rem(n + STEPS, WIDE)

    def down_copy(n):
        return pltpu.make_async_copy(refs['w_down'].at[layer, :, col(n)], wbuf.at[:, col(down_slot(n))], refs['dw_sem'].at[n])

    for g in (2, 3):
        a_copies[g].start()
    o_copy(0).start()
    for g in (0, 1):
        a_copies[g].start()
    o_copy(1).start()
    o_copy(2).start()
    x_copy.start()
    pl.semaphore_wait(barrier, 2)
    for copy in a_copies[2:]:
        copy.wait()

    def late_up(i):
        up_copy(i).start()
        if i:
            x_copy.wait()

    total = scatter('s1', abuf, o_copy, lambda n: n, depth, 3, late_up, a_copies[:2])

    def ready_up():
        for i in range(2):
            up_copy(i).wait()
        for n in range(WIDE - STEPS):
            down_copy(n).start()

    def finish_up(g, cols, value, blocks):
        act[g:g + 2, :, :, cols] = split(jnp.square(jnp.maximum(value, 0.0)).astype(BF))

    gather('g1', 2 * layer + 1, total, 0, d_model, ready_up, finish_up)

    w_at = (WIDE * blk) - (4 * blk)

    def late_qkv(i):
        if i == 0 and cfg['more']:
            for copy in qkv_copies(layer + 1, w_at):
                copy.start()

    total = scatter('s2', act, down_copy, down_slot, d_model, WIDE - STEPS, late_qkv)
    out_copy = pltpu.make_async_copy(xbuf, refs['x_out'], refs['x_sem'])
    out_copy.start()
    if cfg['more']:
        gather_qkv(layer + 1, total, w_at, False)
    out_copy.wait()


def exchange(cid, x, ln_gain, ln_bias, qkv_weights, *, n_seq, layer=-1, more=True, a=None, weights=(), start_pos=None, head_dim=0):
    rows, d_model = x.shape
    toks = rows // n_seq
    blk = d_model // STEPS
    first = a is None
    any_spec, vmem = pl.BlockSpec(memory_space=pl.ANY), pl.BlockSpec(memory_space=pltpu.VMEM)
    dma = pltpu.SemaphoreType.DMA
    ins = [('x_hbm', x, any_spec), ('ln_gain', ln_gain, vmem), ('ln_bias', ln_bias, vmem)]
    outs = []
    qkv_out = sum(w.shape[2] for w in qkv_weights)
    width = qkv_out if first else WIDE * blk
    scr = [('wbuf', pltpu.VMEM((d_model, width), BF)), ('xbuf', pltpu.VMEM((rows, d_model), BF)), ('x_sem', dma)]
    scr += [
        ('near_h', pltpu.VMEM((2 * rows, d_model), BF)), ('far_h', pltpu.VMEM((2 * rows, d_model), BF)),
        ('acc', pltpu.VMEM((2 * rows, qkv_out if first else d_model), F32)),
    ]
    gather_tags, flops, moved = [], 0, 4_000_000
    if not first:
        w_o, w_up, w_down = weights
        depth = a.shape[3]
        ins += [('a_hbm', a, any_spec), ('w_o', w_o, any_spec), ('w_up', w_up, any_spec), ('w_down', w_down, any_spec)]
        outs += [('x_out', jax.ShapeDtypeStruct(x.shape, BF))]
        scr += [
            ('abuf', pltpu.VMEM((4, n_seq, toks, depth), BF)), ('act', pltpu.VMEM((4, n_seq, toks, d_model), BF)),
            ('dsend', pltpu.VMEM((STEPS, 2, rows, blk), BF)), ('drecv', pltpu.VMEM((STEPS, 2, rows, blk), BF)),
            ('qsend', pltpu.VMEM((STEPS, rows, blk), BF)), ('qrecv', pltpu.VMEM((STEPS, rows, blk), BF)),
            ('own', pltpu.VMEM((STEPS, rows, blk), F32)), ('part', pltpu.VMEM((rows, blk), F32)),
            ('a_sem', dma((4,))), ('ow_sem', dma((STEPS,))), ('uw_sem', dma((2,))), ('dw_sem', dma((STEPS,))),
        ]
        for tag in ('s1', 's2'):
            scr += [(tag + k, dma((STEPS, 2))) for k in ('ds', 'dr')] + [(tag + k, dma((STEPS,))) for k in ('qs', 'qr')]
        gather_tags.append('g1')
        flops += 2 * 4 * rows * d_model * (depth + 2 * d_model)
        moved += 2 * d_model * (depth + 2 * d_model)
    if more:
        ins += list(zip(('w_q', 'w_k', 'w_v'), qkv_weights, [any_spec] * 3))
        outs += [('y_out', jax.ShapeDtypeStruct((n_seq, 4, toks, qkv_out), F32))]
        scr += [('stage', pltpu.VMEM((4, n_seq, toks, qkv_out), F32)), ('gw_sem', dma((3,))), ('y_sem', dma((4, STEPS)))]
        gather_tags.append('g2')
        flops += 2 * 4 * rows * d_model * qkv_out
        moved += 2 * d_model * qkv_out
    if first:
        tab_shape = (3, n_seq, 4 * toks, head_dim)
        ins += [('start', start_pos, pl.BlockSpec(memory_space=pltpu.SMEM))]
        outs += [('tab_out', jax.ShapeDtypeStruct(tab_shape, F32))]
        scr += [('tabs', pltpu.VMEM(tab_shape, F32)), ('tab_sem', dma)]
    for tag in gather_tags:
        scr += [(tag + k, dma((2 * STEPS,))) for k in ('cs', 'cr', 'fs', 'fr')] + [(tag + k, dma((STEPS,))) for k in ('ps', 'pr')]
    cfg = dict(names=[i[0] for i in ins] + [o[0] for o in outs] + [s[0] for s in scr], layer=layer, first=first, more=more, n_seq=n_seq, toks=toks, d_model=d_model)
    return pl.pallas_call(
        functools.partial(exchange_kernel, cfg),
        in_specs=[i[2] for i in ins],
        out_specs=[any_spec] * len(outs),
        out_shape=[o[1] for o in outs],
        scratch_shapes=[s[1] for s in scr],
        compiler_params=pltpu.CompilerParams(collective_id=cid, has_side_effects=True, vmem_limit_bytes=67_000_000),
        cost_estimate=pl.CostEstimate(flops=flops, bytes_accessed=moved, transcendentals=0),
        name='gather_first' if first else 'block' if more else 'block_last',
    )(*[i[1] for i in ins])


def solution(mesh):
    tok_spec = P('dp', 'tp', None)
    cache_spec = P(None, 'dp', 'tp', None, None)
    col_spec = P(None, None, 'tp')
    row_spec = P(None, 'tp', None)

    def device_fn(x_loc, start_pos, k_cache, v_cache, w_q, w_k, w_v, w_o, w_up, w_down, ln_gain, ln_bias):
        n_layers = w_q.shape[0]
        n_seq, tok_loc, d_model = x_loc.shape
        new_len = tok_loc * 4
        rows = n_seq * new_len
        hidden = x_loc.reshape(n_seq * tok_loc, d_model)
        prev = ()
        qkv_weights = (w_q, w_k, w_v)
        qkv, tabs = exchange(0, hidden, ln_gain, ln_bias, qkv_weights, n_seq=n_seq, start_pos=start_pos, head_dim=k_cache.shape[4])
        for layer in range(n_layers):
            context, *prev = attend(layer, qkv.reshape(rows, -1), tabs, start_pos, k_cache, v_cache, prev)
            context = context.reshape(n_seq, 4, tok_loc, -1)
            outs = exchange(layer + 1, hidden, ln_gain, ln_bias, qkv_weights, n_seq=n_seq, layer=layer, more=layer + 1 < n_layers, a=context, weights=(w_o, w_up, w_down))
            hidden, qkv = outs if layer + 1 < n_layers else (outs[0], None)
        return hidden.reshape(x_loc.shape), prev[0], prev[1]

    return jax.shard_map(device_fn, mesh=mesh, in_specs=(tok_spec, P('dp'), cache_spec, cache_spec, col_spec, col_spec, col_spec, row_spec, col_spec, row_spec, P(), P()), out_specs=(tok_spec, cache_spec, cache_spec), check_vma=False)
```

```python
import functools
import math

import jax
import jax.numpy as jnp
from jax import lax
from jax.experimental import pallas as pl
from jax.experimental.pallas import tpu as pltpu
from jax.sharding import PartitionSpec as P

LN_EPS = 1e-5
ROPE_BASE = 10000.0
NEG_BIG = -1e30
MIN_START = 768
SLOTS = 4
BF = jnp.bfloat16
F32 = jnp.float32


def rope_tables(start, toks, head_dim):
    rot = head_dim // 2
    half = rot // 2
    shape = (toks, head_dim)
    lane = lax.broadcasted_iota(jnp.int32, shape, 1)
    position = start + lax.broadcasted_iota(jnp.int32, shape, 0)
    power = lax.rem(lane, half).astype(F32) * (2.0 / rot)
    angles = position.astype(F32) * jnp.exp(power * -math.log(ROPE_BASE))
    cos_a, sin_a = jnp.cos(angles), jnp.sin(angles)
    upper = jnp.logical_and(lane >= half, lane < rot)
    return jnp.where(lane < rot, cos_a, 1.0), jnp.where(upper, sin_a, 0.0), jnp.where(lane < half, -sin_a, 0.0)


def attn_kernel(layer, dims, start_ref, q_ref, k_ref, v_ref, tab_ref, kc_hbm, vc_hbm, *rest):
    kv, group, toks, hd, s_len, ch = dims
    if layer > 0:
        rest = rest[2:]
    ctx_ref, ko_hbm, vo_hbm, kbuf, vbuf, sbuf, ebuf, qbuf, mbuf, pbuf, lbuf, abuf, in_sem, out_sem = rest
    b = pl.program_id(0)
    nb = pl.num_programs(0) - 1
    s_pad = kbuf.shape[2]
    win = toks + 16
    rows = group * toks
    coef = (hd ** -0.5) * math.log2(math.e)
    slot = lax.rem(b, SLOTS)
    before = lax.rem(b + SLOTS - 1, SLOTS)

    def load(bb):
        sl = lax.rem(bb, SLOTS)
        return [pltpu.make_async_copy(src.at[layer, bb], dst.at[sl, :, pl.ds(0, s_len), :], in_sem.at[sl, i]) for i, (src, dst) in enumerate(((kc_hbm, kbuf), (vc_hbm, vbuf)))]

    def save(bb):
        sl = lax.rem(bb, SLOTS)
        return [pltpu.make_async_copy(src.at[sl, :, pl.ds(0, s_len), :], dst.at[layer, bb], out_sem.at[sl, i]) for i, (src, dst) in enumerate(((kbuf, ko_hbm), (vbuf, vo_hbm)))]

    def run(copies, go):
        for copy in copies:
            copy.start() if go else copy.wait()

    @pl.when(b == 0)
    def _():
        run(load(b), True)
        if s_pad > s_len:
            for sl in range(SLOTS):
                kbuf[sl, :, s_len:, :] = jnp.zeros((kv, s_pad - s_len, hd), BF)
                vbuf[sl, :, s_len:, :] = jnp.zeros((kv, s_pad - s_len, hd), BF)

    @pl.when(b >= 2)
    def _():
        run(save(b - 2), False)

    @pl.when(jnp.logical_and(b > 0, b + 2 < nb))
    def _():
        run(load(b + 2), True)

    start = start_ref[jnp.minimum(b, nb - 1)]
    start_before = start_ref[jnp.maximum(b - 1, 0)]
    half = hd // 4

    def rope(x):
        return x * tab_ref[0, 0] + pltpu.roll(x, half, 1) * tab_ref[1, 0] + pltpu.roll(x, hd - half, 1) * tab_ref[2, 0]

    def patch():
        base = jnp.minimum((start // 16) * 16, s_len - win)
        shift = start - base
        base = pl.multiple_of(base, 16)
        row_id = lax.broadcasted_iota(jnp.int32, (win, hd), 0)
        is_new = jnp.logical_and(row_id >= shift, row_id < shift + toks)
        run(load(b), False)

        @pl.when(b == 0)
        def _():
            run(load(b + 1), True)
            run(load(b + 2), True)

        for h in range(kv):
            cols = slice(h * hd, (h + 1) * hd)
            for buf, fresh in ((kbuf, rope(k_ref[:, cols])), (vbuf, v_ref[:, cols])):
                fresh = fresh.astype(BF).astype(F32)
                fresh = jnp.concatenate([fresh, jnp.zeros((16, hd), F32)], axis=0)
                fresh = pltpu.roll(fresh, shift, 0)
                old = buf[slot, h, pl.ds(base, win), :].astype(F32)
                buf[slot, h, pl.ds(base, win), :] = jnp.where(is_new, fresh, old).astype(BF)
        run(save(b), True)

    step_rows = 64
    blocks = [slice(r, r + step_rows) for r in range(0, ch, step_rows)]

    def chunk(j):
        return pl.ds(pl.multiple_of(j * ch, ch), ch)

    def score(h, j, masked):
        s = lax.dot_general(kbuf[slot, h, chunk(j), :], qbuf[h], (((1,), (1,)), ((), ())), preferred_element_type=F32)
        if masked:
            ahead = lax.broadcasted_iota(jnp.int32, (ch, rows), 0) - lax.rem(lax.broadcasted_iota(jnp.int32, (ch, rows), 1), toks)
            s = jnp.where(ahead <= start - j * ch, s, NEG_BIG)
        sbuf[h] = s

    def scored(h, rb):
        return sbuf[h, rb].reshape(step_rows // 8, 8, rows)

    def peaks(h, peak):
        top = jnp.max(scored(h, blocks[0]), axis=0)
        for rb in blocks[1:]:
            top = jnp.maximum(top, jnp.max(scored(h, rb), axis=0))
        mbuf[h] = peak
        pbuf[h] = jnp.maximum(peak, jnp.max(top, axis=0, keepdims=True))

    def weigh(h):
        peak = pbuf[h]
        alpha = jnp.exp2((mbuf[h] - peak) * coef)
        total = lbuf[h] * alpha
        for rb in blocks:
            e = jnp.exp2((scored(h, rb) - peak) * coef)
            total = total + jnp.sum(e, axis=0)
            ebuf[h, rb] = e.reshape(step_rows, rows).astype(BF)
        return alpha, total

    def mix(h, sl, j, alpha):
        fresh = lax.dot_general(vbuf[sl, h, chunk(j), :], ebuf[h], (((0,), (0,)), ((), ())), preferred_element_type=F32)
        return (abuf[h].reshape(hd // 8, 8, rows) * alpha).reshape(hd, rows) + fresh

    def step(masked_next, j, carry):
        for h in range(kv):
            alpha, lbuf[h] = weigh(h)
            score(h, j + 1, masked_next)
            abuf[h] = mix(h, slot, j, alpha)
        for h in range(kv):
            peaks(h, pbuf[h])
        return carry

    def last_of(bb_start):
        return (bb_start + toks + ch - 1) // ch - 1

    def turn(close, open_next):
        if open_next:
            for h in range(kv):
                for g in range(group):
                    j = h * group + g
                    qbuf[h, g * toks:(g + 1) * toks, :] = rope(q_ref[:, j * hd:(j + 1) * hd]).astype(BF)
            patch()
        for h in range(kv):
            if close:
                alpha, total = weigh(h)
            if open_next:
                score(h, 0, ch > MIN_START)
            if close:
                ctx = (mix(h, before, last_of(start_before), alpha) / jnp.sum(total, axis=0, keepdims=True)).T.astype(BF)
                for g in range(group):
                    j = h * group + g
                    ctx_ref[:, j * hd:(j + 1) * hd] = ctx[g * toks:(g + 1) * toks, :]
        if open_next:
            for h in range(kv):
                peaks(h, jnp.full((8, rows), NEG_BIG, F32))
                lbuf[h] = jnp.zeros((8, rows), F32)
                abuf[h] = jnp.zeros((hd, rows), F32)

    pl.when(b == 0)(functools.partial(turn, False, True))
    pl.when(jnp.logical_and(b > 0, b < nb))(functools.partial(turn, True, True))
    pl.when(b == nb)(functools.partial(turn, True, False))

    @pl.when(b < nb)
    def _():
        n_full = jnp.maximum(start // ch, 1)
        lax.fori_loop(0, n_full - 1, functools.partial(step, False), 0)
        lax.fori_loop(n_full - 1, last_of(start), functools.partial(step, True), 0)

    @pl.when(b == nb)
    def _():
        run(save(b - 1), False)


def attend(layer, qkv, tabs, start_pos, k_cache, v_cache, prev):
    n_seq = start_pos.shape[0]
    _, _, kv, s_len, hd = k_cache.shape
    toks = qkv.shape[0] // n_seq
    kv_width = kv * hd
    q_width = qkv.shape[1] - 2 * kv_width
    group = q_width // kv_width
    n_ch = -(-s_len // 640)
    ch = 128 * -(-s_len // (128 * n_ch))
    rows = group * toks
    dims = (kv, group, toks, hd, s_len, ch)
    any_spec = pl.BlockSpec(memory_space=pl.ANY)
    now = lambda b: jnp.minimum(b, n_seq - 1)
    tab_spec = pl.BlockSpec((3, 1, toks, hd), lambda b, *_: (0, now(b), 0, 0))
    cache_shape = jax.ShapeDtypeStruct(k_cache.shape, BF)
    args = [start_pos, qkv, qkv, qkv, tabs, k_cache, v_cache] + list(prev)
    return pl.pallas_call(
        functools.partial(attn_kernel, layer, dims),
        grid_spec=pltpu.PrefetchScalarGridSpec(
            num_scalar_prefetch=1,
            grid=(n_seq + 1,),
            in_specs=[
                pl.BlockSpec((toks, q_width), lambda b, *_: (now(b), 0)),
                pl.BlockSpec((toks, kv_width), lambda b, *_: (now(b), group)),
                pl.BlockSpec((toks, kv_width), lambda b, *_: (now(b), group + 1)),
                tab_spec,
            ] + [any_spec] * (2 + len(prev)),
            out_specs=[pl.BlockSpec((toks, q_width), lambda b, *_: (jnp.maximum(b - 1, 0), 0)), any_spec, any_spec],
            scratch_shapes=[
                pltpu.VMEM((SLOTS, kv, ch * n_ch, hd), BF),
                pltpu.VMEM((SLOTS, kv, ch * n_ch, hd), BF),
                pltpu.VMEM((kv, ch, rows), F32),
                pltpu.VMEM((kv, ch, rows), BF),
                pltpu.VMEM((kv, rows, hd), BF),
                pltpu.VMEM((kv, 8, rows), F32),
                pltpu.VMEM((kv, 8, rows), F32),
                pltpu.VMEM((kv, 8, rows), F32),
                pltpu.VMEM((kv, hd, rows), F32),
                pltpu.SemaphoreType.DMA((SLOTS, 2)),
                pltpu.SemaphoreType.DMA((SLOTS, 2)),
            ],
        ),
        out_shape=[jax.ShapeDtypeStruct((n_seq * toks, q_width), BF), cache_shape, cache_shape],
        input_output_aliases={7: 1, 8: 2} if prev else {},
        compiler_params=pltpu.CompilerParams(vmem_limit_bytes=60 * 1024 * 1024, dimension_semantics=("arbitrary",)),
        cost_estimate=pl.CostEstimate(flops=8_000_000_000, bytes_accessed=80_000_000, transcendentals=15_000_000),
        name="attend",
    )(*args)


STEPS = 8
WIDE = STEPS + 2


def exchange_kernel(cfg, *args):
    refs = dict(zip(cfg['names'], args))
    n_seq, toks, d_model = cfg['n_seq'], cfg['toks'], cfg['d_model']
    rows = n_seq * toks
    blk = d_model // STEPS
    me = lax.axis_index('tp')
    core = lax.rem(me, 2)
    partner = me + 1 - 2 * core
    counter = lax.rem(me + 2, 4)
    diag = lax.rem(partner + 2, 4)
    order = (me, partner, counter, diag)
    wbuf, xbuf = refs['wbuf'], refs['xbuf']

    barrier = pltpu.get_barrier_semaphore()
    for peer in (partner, counter):
        pl.semaphore_signal(barrier, inc=1, device_id={'tp': peer}, device_id_type=pl.DeviceIdType.MESH)

    def col(n, width=blk):
        return pl.ds(pl.multiple_of(n * width, width), width)

    def remote(src, dst, send, recv, peer):
        return pltpu.make_async_remote_copy(src_ref=src, dst_ref=dst, send_sem=send, recv_sem=recv, device_id={'tp': peer}, device_id_type=pl.DeviceIdType.MESH)

    def fold(values, total):
        for j in range(blk // 128):
            total = total + values[:, j * 128:(j + 1) * 128]
        return total

    def moments(values, state):
        zero = jnp.zeros((rows, 128), F32)
        if state is None:
            state = (jnp.sum(fold(values, zero), axis=-1, keepdims=True) / blk, zero, zero)
        shift, first, second = state
        moved = values - shift
        return shift, fold(moved, first), fold(moved * moved, second)

    def scatter(tag, a_ref, w_copy, slot_of, depth, ahead, late, near_ready=()):
        dsend, drecv, qsend, qrecv, own, part = (refs[k] for k in ('dsend', 'drecv', 'qsend', 'qrecv', 'own', 'part'))
        ds_sem, dr_sem, qs_sem, qr_sem = (refs[tag + k] for k in ('ds', 'dr', 'qs', 'qr'))

        def d_copy(n, i):
            return remote(dsend.at[n, i], drecv.at[n, i], ds_sem.at[n, i], dr_sem.at[n, i], partner)

        def q_copy(n):
            return remote(qsend.at[n], qrecv.at[n], qs_sem.at[n], qr_sem.at[n], counter)

        def step(n, carry):
            @pl.when(n + ahead < STEPS)
            def _():
                w_copy(n + ahead).start()

            w_copy(n).wait()
            cols = col(slot_of(n))
            far = jnp.dot(a_ref[2:4].reshape(2 * rows, depth), wbuf[0:depth, cols], preferred_element_type=F32)
            dsend[n, 0] = far[rows:].astype(BF)
            d_copy(n, 0).start()
            part[...] = far[:rows]
            if near_ready:
                @pl.when(n == 0)
                def _():
                    for copy in near_ready:
                        copy.wait()

            near = jnp.dot(a_ref[0:2].reshape(2 * rows, depth), wbuf[0:depth, cols], preferred_element_type=F32)
            dsend[n, 1] = near[rows:].astype(BF)
            d_copy(n, 1).start()
            own[n] = near[:rows]
            d_copy(n, 0).wait_recv()
            qsend[n] = (part[...] + drecv[n, 0].astype(F32)).astype(BF)
            q_copy(n).start()
            return carry

        half = STEPS - ahead
        lax.fori_loop(0, half, step, 0)
        late(0)
        lax.fori_loop(half, STEPS, step, 0)
        late(1)
        total = None
        for n in range(STEPS):
            cols = slice(n * blk, (n + 1) * blk)
            d_copy(n, 1).wait_recv()
            q_copy(n).wait_recv()
            summed = own[n] + drecv[n, 1].astype(F32) + qrecv[n].astype(F32)
            fresh = (xbuf[:, cols].astype(F32) + summed.astype(BF).astype(F32)).astype(BF)
            xbuf[:, cols] = fresh
            total = moments(fresh.astype(F32), total)
        for n in range(STEPS):
            d_copy(n, 0).wait_send()
            d_copy(n, 1).wait_send()
            q_copy(n).wait_send()
        return total

    def gather(tag, ln_row, total, w_at, n_out, ready, finish):
        near_h, far_h, acc = refs['near_h'], refs['far_h'], refs['acc']
        cs, cr, fs, fr, ps, pr = (refs[tag + k] for k in ('cs', 'cr', 'fs', 'fr', 'ps', 'pr'))
        shift, first, second = total
        offset = jnp.sum(first, axis=-1, keepdims=True) / d_model
        mean = shift + offset
        variance = jnp.maximum(jnp.sum(second, axis=-1, keepdims=True) / d_model - offset * offset, 0.0)
        inv = lax.rsqrt(variance + LN_EPS)

        chunk = blk // 2

        def c_copy(k):
            return remote(near_h.at[pl.ds(0, rows), col(k, chunk)], far_h.at[pl.ds(0, rows), col(k, chunk)], cs.at[k], cr.at[k], counter)

        def f_copy(k):
            return remote(far_h.at[pl.ds(0, rows), col(k, chunk)], far_h.at[pl.ds(rows, rows), col(k, chunk)], fs.at[k], fr.at[k], partner)

        def p_copy(k):
            return remote(near_h.at[pl.ds(0, rows), col(k)], near_h.at[pl.ds(rows, rows), col(k)], ps.at[k], pr.at[k], partner)

        for k in range(STEPS):
            cols = slice(k * blk, (k + 1) * blk)
            gain = refs['ln_gain'][ln_row // 2, ln_row % 2:ln_row % 2 + 1, cols].astype(F32)
            bias = refs['ln_bias'][ln_row // 2, ln_row % 2:ln_row % 2 + 1, cols].astype(F32)
            normed = (xbuf[:, cols].astype(F32) - mean) * inv
            near_h[0:rows, cols] = (normed * (1.0 + gain) + bias).astype(BF)
            if k:
                c_copy(2 * k - 2).start()
                c_copy(2 * k - 1).start()
                p_copy(k - 1).start()
        acc[:, 0:n_out] = jnp.zeros((2 * rows, n_out), F32)
        c_copy(2 * STEPS - 2).start()
        c_copy(2 * STEPS - 1).start()
        p_copy(STEPS - 1).start()
        ready()
        for k in range(STEPS):
            p_copy(k).wait_recv()

        n_blk = n_out // STEPS
        piece = min(1024, n_out)

        def far_dot(k, width, cols):
            return jnp.dot(far_h[:, col(k, width)], wbuf[col(k, width), w_at + cols.start:w_at + cols.stop], preferred_element_type=F32)

        pieces = [slice(n, n + piece) for n in range(0, n_out, piece)]

        def far_step(k, width):
            for cols in pieces:
                acc[:, cols] += far_dot(k, width, cols)

        def pass_on(k):
            c_copy(k).wait_recv()
            f_copy(k).start()

        def near_step(i):
            at = pl.ds(pl.multiple_of(w_at + i * n_blk, n_blk), n_blk)
            finish(0, col(i, n_blk), jnp.dot(near_h[...], wbuf[:, at], preferred_element_type=F32), [i])
            pass_on(2 * i)

        def step(i, carry):
            near_step(i)
            f_copy(2 * i - 2).wait_recv()
            f_copy(2 * i - 1).wait_recv()
            far_step(i - 1, blk)
            pass_on(2 * i + 1)
            return carry

        near_step(0)
        pass_on(1)
        lax.fori_loop(1, STEPS, step, 0)
        f_copy(2 * STEPS - 2).wait_recv()
        far_step(2 * STEPS - 2, chunk)
        f_copy(2 * STEPS - 1).wait_recv()
        for cols in pieces:
            finish(2, cols, acc[:, cols] + far_dot(2 * STEPS - 1, chunk, cols), range(cols.start // n_blk, cols.stop // n_blk))
        for k in range(STEPS):
            p_copy(k).wait_send()
        for k in range(2 * STEPS):
            c_copy(k).wait_send()
            f_copy(k).wait_send()

    def split(value):
        return value.reshape(2, n_seq, toks, value.shape[-1])

    def gather_qkv(layer, total, w_at, start_now):
        stage, y_out = refs['stage'], refs['y_out']
        n_out = y_out.shape[3]
        n_blk = n_out // STEPS

        def y_copy(g, n):
            return pltpu.make_async_copy(stage.at[g, :, :, col(n, n_blk)], y_out.at[:, order[g], :, col(n, n_blk)], refs['y_sem'].at[g, n])

        def ready():
            if start_now:
                tabs = refs['tabs']

                def table(b, carry):
                    for i, part in enumerate(rope_tables(refs['start'][b], tabs.shape[2], tabs.shape[3])):
                        tabs[i, b] = part
                    return carry

                lax.fori_loop(0, n_seq, table, 0)
                tab_copy.start()
            for copy in qkv_copies(layer, w_at):
                copy.wait()

        def finish(g, cols, value, blocks):
            stage[g:g + 2, :, :, cols] = split(value)
            for n in blocks:
                y_copy(g, n).start()
                y_copy(g + 1, n).start()

        if start_now:
            tab_copy = pltpu.make_async_copy(refs['tabs'], refs['tab_out'], refs['tab_sem'])
        gather('g2', 2 * layer, total, w_at, n_out, ready, finish)
        if start_now:
            tab_copy.wait()
        for g in range(4):
            for n in range(STEPS):
                y_copy(g, n).wait()

    def qkv_copies(layer, w_at):
        copies = []
        for i, name in enumerate(('w_q', 'w_k', 'w_v')):
            width = refs[name].shape[2]
            copies.append(pltpu.make_async_copy(refs[name].at[layer], wbuf.at[:, pl.ds(w_at, width)], refs['gw_sem'].at[i]))
            w_at += width
        return copies

    x_copy = pltpu.make_async_copy(refs['x_hbm'], xbuf, refs['x_sem'])
    if cfg['first']:
        x_copy.start()
        x_copy.wait()
        for copy in qkv_copies(0, 0):
            copy.start()
        total = None
        for n in range(STEPS):
            total = moments(xbuf[:, n * blk:(n + 1) * blk].astype(F32), total)
        pl.semaphore_wait(barrier, 2)
        gather_qkv(0, total, 0, True)
        return

    layer = cfg['layer']
    abuf, act = refs['abuf'], refs['act']
    depth = abuf.shape[3]
    a_copies = [pltpu.make_async_copy(refs['a_hbm'].at[:, order[g]], abuf.at[g], refs['a_sem'].at[g]) for g in range(4)]

    def o_copy(n):
        return pltpu.make_async_copy(refs['w_o'].at[layer, :, col(n)], wbuf.at[pl.ds(0, depth), col(n)], refs['ow_sem'].at[n])

    def up_copy(i):
        span = pl.ds(0, depth) if i else pl.ds(depth, d_model - depth)
        return pltpu.make_async_copy(refs['w_up'].at[layer, span, :], wbuf.at[span, pl.ds(0, d_model)], refs['uw_sem'].at[i])

    def down_slot(n):
        return lax.rem(n + STEPS, WIDE)

    def down_copy(n):
        return pltpu.make_async_copy(refs['w_down'].at[layer, :, col(n)], wbuf.at[:, col(down_slot(n))], refs['dw_sem'].at[n])

    for g in (2, 3):
        a_copies[g].start()
    o_copy(0).start()
    for g in (0, 1):
        a_copies[g].start()
    pl.semaphore_wait(barrier, 2)
    for copy in a_copies[2:]:
        copy.wait()
    o_copy(1).start()
    o_copy(2).start()
    x_copy.start()

    def late_up(i):
        up_copy(i).start()
        if i:
            x_copy.wait()

    total = scatter('s1', abuf, o_copy, lambda n: n, depth, 3, late_up, a_copies[:2])

    def ready_up():
        for i in range(2):
            up_copy(i).wait()
        for n in range(WIDE - STEPS):
            down_copy(n).start()

    def finish_up(g, cols, value, blocks):
        act[g:g + 2, :, :, cols] = split(jnp.square(jnp.maximum(value, 0.0)).astype(BF))

    gather('g1', 2 * layer + 1, total, 0, d_model, ready_up, finish_up)

    w_at = (WIDE * blk) - (4 * blk)

    def late_qkv(i):
        if i == 0 and cfg['more']:
            for copy in qkv_copies(layer + 1, w_at):
                copy.start()

    total = scatter('s2', act, down_copy, down_slot, d_model, WIDE - STEPS, late_qkv)
    out_copy = pltpu.make_async_copy(xbuf, refs['x_out'], refs['x_sem'])
    out_copy.start()
    if cfg['more']:
        gather_qkv(layer + 1, total, w_at, False)
    out_copy.wait()


def exchange(cid, x, ln_gain, ln_bias, qkv_weights, *, n_seq, layer=-1, more=True, a=None, weights=(), start_pos=None, head_dim=0):
    rows, d_model = x.shape
    toks = rows // n_seq
    blk = d_model // STEPS
    first = a is None
    any_spec, vmem = pl.BlockSpec(memory_space=pl.ANY), pl.BlockSpec(memory_space=pltpu.VMEM)
    dma = pltpu.SemaphoreType.DMA
    ins = [('x_hbm', x, any_spec), ('ln_gain', ln_gain, vmem), ('ln_bias', ln_bias, vmem)]
    outs = []
    qkv_out = sum(w.shape[2] for w in qkv_weights)
    width = qkv_out if first else WIDE * blk
    scr = [('wbuf', pltpu.VMEM((d_model, width), BF)), ('xbuf', pltpu.VMEM((rows, d_model), BF)), ('x_sem', dma)]
    scr += [
        ('near_h', pltpu.VMEM((2 * rows, d_model), BF)), ('far_h', pltpu.VMEM((2 * rows, d_model), BF)),
        ('acc', pltpu.VMEM((2 * rows, qkv_out if first else d_model), F32)),
    ]
    gather_tags, flops, moved = [], 0, 4_000_000
    if not first:
        w_o, w_up, w_down = weights
        depth = a.shape[3]
        ins += [('a_hbm', a, any_spec), ('w_o', w_o, any_spec), ('w_up', w_up, any_spec), ('w_down', w_down, any_spec)]
        outs += [('x_out', jax.ShapeDtypeStruct(x.shape, BF))]
        scr += [
            ('abuf', pltpu.VMEM((4, n_seq, toks, depth), BF)), ('act', pltpu.VMEM((4, n_seq, toks, d_model), BF)),
            ('dsend', pltpu.VMEM((STEPS, 2, rows, blk), BF)), ('drecv', pltpu.VMEM((STEPS, 2, rows, blk), BF)),
            ('qsend', pltpu.VMEM((STEPS, rows, blk), BF)), ('qrecv', pltpu.VMEM((STEPS, rows, blk), BF)),
            ('own', pltpu.VMEM((STEPS, rows, blk), F32)), ('part', pltpu.VMEM((rows, blk), F32)),
            ('a_sem', dma((4,))), ('ow_sem', dma((STEPS,))), ('uw_sem', dma((2,))), ('dw_sem', dma((STEPS,))),
        ]
        for tag in ('s1', 's2'):
            scr += [(tag + k, dma((STEPS, 2))) for k in ('ds', 'dr')] + [(tag + k, dma((STEPS,))) for k in ('qs', 'qr')]
        gather_tags.append('g1')
        flops += 2 * 4 * rows * d_model * (depth + 2 * d_model)
        moved += 2 * d_model * (depth + 2 * d_model)
    if more:
        ins += list(zip(('w_q', 'w_k', 'w_v'), qkv_weights, [any_spec] * 3))
        outs += [('y_out', jax.ShapeDtypeStruct((n_seq, 4, toks, qkv_out), F32))]
        scr += [('stage', pltpu.VMEM((4, n_seq, toks, qkv_out), F32)), ('gw_sem', dma((3,))), ('y_sem', dma((4, STEPS)))]
        gather_tags.append('g2')
        flops += 2 * 4 * rows * d_model * qkv_out
        moved += 2 * d_model * qkv_out
    if first:
        tab_shape = (3, n_seq, 4 * toks, head_dim)
        ins += [('start', start_pos, pl.BlockSpec(memory_space=pltpu.SMEM))]
        outs += [('tab_out', jax.ShapeDtypeStruct(tab_shape, F32))]
        scr += [('tabs', pltpu.VMEM(tab_shape, F32)), ('tab_sem', dma)]
    for tag in gather_tags:
        scr += [(tag + k, dma((2 * STEPS,))) for k in ('cs', 'cr', 'fs', 'fr')] + [(tag + k, dma((STEPS,))) for k in ('ps', 'pr')]
    cfg = dict(names=[i[0] for i in ins] + [o[0] for o in outs] + [s[0] for s in scr], layer=layer, first=first, more=more, n_seq=n_seq, toks=toks, d_model=d_model)
    return pl.pallas_call(
        functools.partial(exchange_kernel, cfg),
        in_specs=[i[2] for i in ins],
        out_specs=[any_spec] * len(outs),
        out_shape=[o[1] for o in outs],
        scratch_shapes=[s[1] for s in scr],
        compiler_params=pltpu.CompilerParams(collective_id=cid, has_side_effects=True, vmem_limit_bytes=67_000_000),
        cost_estimate=pl.CostEstimate(flops=flops, bytes_accessed=moved, transcendentals=0),
        name='gather_first' if first else 'block' if more else 'block_last',
    )(*[i[1] for i in ins])


def solution(mesh):
    tok_spec = P('dp', 'tp', None)
    cache_spec = P(None, 'dp', 'tp', None, None)
    col_spec = P(None, None, 'tp')
    row_spec = P(None, 'tp', None)

    def device_fn(x_loc, start_pos, k_cache, v_cache, w_q, w_k, w_v, w_o, w_up, w_down, ln_gain, ln_bias):
        n_layers = w_q.shape[0]
        n_seq, tok_loc, d_model = x_loc.shape
        new_len = tok_loc * 4
        rows = n_seq * new_len
        hidden = x_loc.reshape(n_seq * tok_loc, d_model)
        prev = ()
        qkv_weights = (w_q, w_k, w_v)
        qkv, tabs = exchange(0, hidden, ln_gain, ln_bias, qkv_weights, n_seq=n_seq, start_pos=start_pos, head_dim=k_cache.shape[4])
        for layer in range(n_layers):
            context, *prev = attend(layer, qkv.reshape(rows, -1), tabs, start_pos, k_cache, v_cache, prev)
            context = context.reshape(n_seq, 4, tok_loc, -1)
            outs = exchange(layer + 1, hidden, ln_gain, ln_bias, qkv_weights, n_seq=n_seq, layer=layer, more=layer + 1 < n_layers, a=context, weights=(w_o, w_up, w_down))
            hidden, qkv = outs if layer + 1 < n_layers else (outs[0], None)
        return hidden.reshape(x_loc.shape), prev[0], prev[1]

    return jax.shard_map(device_fn, mesh=mesh, in_specs=(tok_spec, P('dp'), cache_spec, cache_spec, col_spec, col_spec, col_spec, row_spec, col_spec, row_spec, P(), P()), out_specs=(tok_spec, cache_spec, cache_spec), check_vma=False)
```
